32 devices in a mesh: gx: 2 (over y), gy: 4 (over z), gz: 4 (over x, core).
Axes of the slice: x: 2, y: 2, z: 4, core: 2. Of those that a mesh axis runs over, the one named last changes fastest.
Arguments:
- conserved: float32 [5, 16, 32, 512], P(None, 'gx', 'gy', 'gz'), may hold values from -3 to 4, as said below
- sigma_guess: float32 [16, 32, 512], P('gx', 'gy', 'gz'), may hold values from -30 to 30
Outputs:
- advanced: float32 [5, 16, 32, 512], P(None, 'gx', 'gy', 'gz')
- sigma_field: float32 [16, 32, 512], P('gx', 'gy', 'gz')
The draws below stay inside these ranges and needn't reach their ends.
Inputs may be any that keep to these rules, and one draw needn't show every extreme that they name: `conserved`: component 0 (density) lies between 0.5 and 2, components 1 to 3 (momenta) between -3 and 3, component 4 (energy) between 1 and 4.
All inputs are finite; a program needn't handle non-finite values.
Results may differ from the reference program's by a relative error of at most 0.00002.
Values sent between devices are 32-bit elements; how exact they have to be, the bound alone decides.
A program may use at most 64 MiB of HBM per device.

```python
import jax
import jax.numpy as jnp

SWEEPS = 4
NX = 16
NY = 32
NZ = 512


def draw_conserved(key, part):
    key_rho = jax.random.fold_in(key, 11)
    key_mom = jax.random.fold_in(key, 12)
    key_energy = jax.random.fold_in(key, 13)
    grid_shape = (NX, NY, NZ)
    density = jax.random.uniform(key_rho, grid_shape, jnp.float32, 0.5, 2.0)
    momentum = jnp.clip(0.6 * jax.random.normal(key_mom, (3,) + grid_shape, jnp.float32), -3.0, 3.0)
    energy = jax.random.uniform(key_energy, grid_shape, jnp.float32, 1.0, 2.5)
    return jnp.concatenate([density[None], momentum, energy[None]], axis=0)


def draw_sigma_guess(key, part):
    key_sign = jax.random.fold_in(key, 21)
    key_size = jax.random.fold_in(key, 22)
    grid_shape = (NX, NY, NZ)
    sign_part = (2 * jax.random.randint(key_sign, grid_shape, 0, 2) - 1).astype(jnp.float32)
    magnitude = jax.random.uniform(key_size, grid_shape, jnp.float32, 24.0, 30.0)
    return sign_part * magnitude


def setup_inputs(seed: int = 0) -> dict:
    key_of = jax.random.split(jax.random.key(seed), 3)
    conserved = draw_conserved(jax.random.fold_in(key_of[2], 71), 0)
    sigma_guess = draw_sigma_guess(jax.random.fold_in(key_of[2], 71), 0)
    return dict(conserved=conserved, sigma_guess=sigma_guess)


ALPHA = 10.0
GAMMA = 1.4
LAMBDA = 3.0
STEP_DT = 0.4


def central(field, direction):
    return 0.5 * (jnp.roll(field, -1, direction) - jnp.roll(field, 1, direction))


def source_term(velocity):
    gradient = [[central(velocity[member], across) for across in range(3)] for member in range(3)]
    trace_sq = jnp.zeros_like(velocity[0])
    for member in range(3):
        for across in range(3):
            trace_sq = trace_sq + gradient[member][across] * gradient[across][member]
    divergence = gradient[0][0] + gradient[1][1] + gradient[2][2]
    return trace_sq + divergence * divergence


def jacobi_sweep(sigma_now, inv_density, source):
    acc_num = jnp.zeros_like(sigma_now)
    acc_den = jnp.zeros_like(sigma_now)
    for direction in range(3):
        for offset in (1, -1):
            weight_face = 0.5 * (inv_density + jnp.roll(inv_density, offset, direction))
            acc_num = acc_num + weight_face * jnp.roll(sigma_now, offset, direction)
            acc_den = acc_den + weight_face
    return (ALPHA * source + ALPHA * acc_num) / (inv_density + ALPHA * acc_den)


def physical(states, sigma_face, direction):
    density = states[0]
    normal_speed = states[1 + direction] / density
    kinetic = 0.5 * (states[1] * states[1] + states[2] * states[2] + states[3] * states[3]) / density
    pressure = (GAMMA - 1.0) * (states[4] - kinetic) + sigma_face
    flux_rows = [states[1 + direction]]
    for member in range(3):
        flux_term = states[1 + member] * normal_speed
        if member == direction:
            flux_term = flux_term + pressure
        flux_rows.append(flux_term)
    flux_rows.append((states[4] + pressure) * normal_speed)
    return jnp.stack(flux_rows)


def flux_change(conserved, sigma_field, direction):
    axis_q = direction + 1
    left_state = (5.0 * conserved + 2.0 * jnp.roll(conserved, -1, axis_q) - jnp.roll(conserved, 1, axis_q)) / 6.0
    right_state = (2.0 * conserved + 5.0 * jnp.roll(conserved, -1, axis_q) - jnp.roll(conserved, -2, axis_q)) / 6.0
    left_sigma = (5.0 * sigma_field + 2.0 * jnp.roll(sigma_field, -1, direction) - jnp.roll(sigma_field, 1, direction)) / 6.0
    right_sigma = (2.0 * sigma_field + 5.0 * jnp.roll(sigma_field, -1, direction) - jnp.roll(sigma_field, -2, direction)) / 6.0
    face_flux = 0.5 * (physical(left_state, left_sigma, direction) + physical(right_state, right_sigma, direction)) - 0.5 * LAMBDA * (right_state - left_state)
    return face_flux - jnp.roll(face_flux, 1, axis_q)


def reference(conserved, sigma_guess):
    inv_density = 1.0 / conserved[0]
    velocity = conserved[1:4] / conserved[0]
    source = source_term(velocity)
    sigma_now = sigma_guess
    for sweep_no in range(SWEEPS):
        sigma_now = jacobi_sweep(sigma_now, inv_density, source)
    tendency = jnp.zeros_like(conserved)
    for direction in range(3):
        tendency = tendency - flux_change(conserved, sigma_now, direction)
    advanced = conserved + STEP_DT * tendency
    return advanced, sigma_now
```

```python
import functools
import itertools

import jax
import jax.numpy as jnp
from jax import lax
from jax.experimental import pallas as pl
from jax.experimental.pallas import tpu as pltpu
from jax.sharding import PartitionSpec as P

SWEEPS = 4
ALPHA = 10.0
GAMMA = 1.4
LAMBDA = 3.0
STEP_DT = 0.4
DEPTH = SWEEPS
MESH = pl.DeviceIdType.MESH
AXES = ("gx", "gy", "gz")

OFFSETS = [o for o in itertools.product((-1, 0, 1), repeat=3) if any(o)]
NEAR = [o for o in OFFSETS if sum(abs(v) for v in o) == 1]
XY_MOVES = [o for o in OFFSETS if o[0] != 0 and o[1] != 0 and o[2] == 0]
Z_NEAR = [(0, 0, 1), (0, 0, -1)]
Z_VERTEX = [o for o in OFFSETS if all(o)]
Z_EDGE = [o for o in OFFSETS if o[2] != 0 and o not in Z_NEAR and o not in Z_VERTEX]


def iota(shape, dim):
    return lax.broadcasted_iota(jnp.int32, shape, dim)


def roll(value, shift, axis):
    size = value.shape[axis]
    shift = shift % size
    return value if shift == 0 else pltpu.roll(value, shift, axis)


def ring(core, ghost, step, axis):
    size = core.shape[axis]
    a, b = roll(core, -step, axis), roll(ghost, -step, axis)
    edge = iota(core.shape, axis) == (size - 1 if step == 1 else 0)
    return jnp.where(edge, b, a), jnp.where(edge, a, b)


def distinct(moves, sizes):
    first = {}
    return {o: first.setdefault(tuple(v % s for v, s in zip(o, sizes)), o) for o in moves}


def landing(X, R, sizes):
    count = lambda moves: len(set(distinct(moves, sizes).values()))
    A, B, H = X // R, 2 * X // R, X // 2
    return [
        2 * (5 * A + 5 + 2),
        2 * (H + A + 4 * B + 5 + 1 + DEPTH - 1),
        count(Z_NEAR),
        2 * len(XY_MOVES) + count(Z_EDGE) + count(Z_VERTEX),
        2 * len(XY_MOVES) + count(Z_NEAR) + count(Z_EDGE) + count(Z_VERTEX) + 2 * 2 * H + 2 * 2 * DEPTH,
    ]


def kernel(sizes, cons_hbm, sig_hbm, adv_ref, out_sig_ref, cons, sig, g0, g1, g2, g3, g4,
           yas, zas, ybs, yrs, zrs, drs, x2s, y2s, z2s, d2s, in_sem, ready, send_sem, recv_sem):
    X, R, L = sig.shape
    H, D, DZ = R // 2, DEPTH, L // (4 * X)
    me = [lax.axis_index(a) for a in AXES]

    def device(offset):
        return {a: lax.rem(me[i] + offset[i] + sizes[i], sizes[i]) for i, a in enumerate(AXES)}

    load_c = pltpu.make_async_copy(cons_hbm, cons, in_sem.at[0])
    load_s = pltpu.make_async_copy(sig_hbm, sig, in_sem.at[1])
    load_c.start()
    load_s.start()
    barrier = pltpu.get_barrier_semaphore()
    for o in NEAR:
        pl.semaphore_signal(barrier, inc=1, device_id=device(o), device_id_type=MESH)

    class Group:
        def __init__(self, n, buf):
            self.n, self.buf, self.used = n, buf, 0

        def copy(self, src, dst, offset):
            return pltpu.make_async_remote_copy(
                src_ref=src, dst_ref=dst, send_sem=send_sem.at[self.n], recv_sem=recv_sem.at[self.n],
                device_id=device(offset), device_id_type=MESH)

        def send(self, src, offset):
            at = self.used
            if len(src.shape) == 2:
                self.used += 1
                self.copy(src, self.buf.at[at], offset).start()
            else:
                self.used += src.shape[0]
                self.copy(src, self.buf.at[at:self.used], offset).start()
            return at

        def arrived(self):
            assert self.used == self.buf.shape[0]
            self.copy(self.buf, self.buf, NEAR[0]).wait_recv()

        def left(self):
            self.copy(self.buf, self.buf, NEAR[0]).wait_send()

    groups = [Group(n, buf) for n, buf in enumerate((g0, g1, g2, g3, g4))]
    first, late, side, late_rho, second = groups

    rows = lambda shape: iota(shape, len(shape) - 2)
    lanes = lambda shape: iota(shape, len(shape) - 1)

    def pack_rows(field, first, n):
        size = X * n // R
        out = field[0:size]
        r = rows(out.shape)
        for g in range(1, R // n):
            part = roll(field[g * size:(g + 1) * size], n * g, 1)
            out = jnp.where((r + (2 * R - first - n * g)) % R < n, part, out)
        return out

    def unpack_rows(after, before, n, reach=0):
        low = rows(after.shape) < H
        return jnp.concatenate(
            [jnp.where(low, roll(after, -n * g - reach, 1), roll(before, reach - n * g, 1)) for g in range(R // n)],
            axis=0)

    lane2, row2 = lanes((R, L)), rows((R, L))
    low2 = row2 < H

    def pack_lanes(fields, width):
        out = jnp.zeros((R, L), jnp.float32)
        for k, tile in enumerate(f[p] for f in fields for p in range(X)):
            out = jnp.where(((lane2 + width // 2) % L) // width == k, roll(tile, width * k, 1), out)
        return out

    def merge_lanes(after, before, width):
        return jnp.where(lanes(after.shape) % width < width // 2, after, before)

    def unpack_lanes(packed, ks, width):
        return [roll(packed, -width * k, 1)[None] for k in ks]

    def pack_corner(f, s, o):
        a1, a2, a3, a4 = (f[X - a if o[0] == 1 else a - 1] for a in range(1, 5))
        if o[1] == 1:
            one = jnp.where(row2 >= H, a1, jnp.where(row2 >= 1, roll(a2, -H, 0), roll(a4, 1, 0)))
            two = roll(a3, 2, 0)
        else:
            one = jnp.where(row2 < H, a1, jnp.where(row2 < R - 1, roll(a2, H, 0), roll(a4, -1, 0)))
            two = roll(a3, -2, 0)
        if s is not None:
            s1, s2, s3 = (s[X - a if o[0] == 1 else a - 1] for a in range(1, 4))
            if o[1] == 1:
                two = jnp.where(row2 > H, s1, jnp.where(row2 == H, roll(s3, 1 - H, 0),
                                                        jnp.where(row2 >= 2, roll(s2, -H, 0), two)))
            else:
                two = jnp.where(row2 < H - 1, s1, jnp.where(row2 == H - 1, roll(s3, H - 1, 0),
                                                            jnp.where(row2 < R - 2, roll(s2, H, 0), two)))
        return one, two

    def unpack_corner(buf, slots, dx, source):
        after, before = slots[(-dx, -1, 0)], slots[(-dx, 1, 0)]
        fa, fb, sa, sb = buf[after], buf[before], buf[after + 1], buf[before + 1]
        if source:
            out = [jnp.where(low2, sa, sb), roll(jnp.where(low2, sb, sa), H, 0),
                   jnp.where(low2, roll(sa, 1 - H, 0), roll(sb, H - 1, 0))]
        else:
            out = [jnp.where(low2, fa, fb), roll(jnp.where(low2, fb, fa), H, 0),
                   jnp.where(low2, roll(sa, 2, 0), roll(sb, -2, 0)),
                   jnp.where(low2, roll(fa, 1, 0), roll(fb, -1, 0))]
        out = [v[None] for v in out]
        return out if dx == 1 else out[::-1]

    def cat(*parts):
        return jnp.concatenate(parts, axis=0)

    ups = ((0, 1), (1, -1))

    def plane(d, back=0):
        return X - 1 - back if d == 1 else back

    def planes(d, count, back=0):
        return slice(X - count - back, X - back) if d == 1 else slice(back, back + count)

    def send_z(group, src_ref, moves, slots):
        for o, same in distinct(moves, sizes).items():
            slots[o] = group.send(src_ref, o) if o == same else slots[same]

    def z_tiles(buf, slots, e, ew, width, f=0):
        def of(dx, dy):
            return merge_lanes(buf[slots[(-dx, -dy, -1)]], buf[slots[(-dx, -dy, 1)]], width)

        def diag(dx):
            return jnp.where(low2, of(dx, 1), of(dx, -1))

        k = f * X
        spread = lambda t, e: cat(*unpack_lanes(t(-1), range(k + X - e, k + X), width),
                                  *unpack_lanes(t(0), range(k, k + X), width),
                                  *unpack_lanes(t(1), range(k, k + e), width))
        return spread(lambda dx: of(dx, 0), e), spread(diag, ew)

    load_c.wait()
    load_s.wait()
    pl.semaphore_wait(barrier, len(NEAR))
    state = [cons[f] for f in range(4)] + [sig[...]]
    A, B = X // R, 2 * X // R
    for f in range(5):
        yas[0, f * A:(f + 1) * A] = pack_rows(state[f], R - 1, 1)
        yas[1, f * A:(f + 1) * A] = pack_rows(state[f], 0, 1)
    ya = [first.send(yas.at[j], (0, d, 0)) for j, d in ups]
    xa = []
    for j, d in ups:
        xa.append(first.send(cons.at[0:4, plane(d)], (d, 0, 0)))
        first.send(sig.at[plane(d)], (d, 0, 0))
    energy = cons[4]
    zas[0] = pack_lanes(state[0:4], 4)
    zas[1] = pack_lanes([state[4], energy], 4)
    za = [first.send(zas, (0, 0, d)) for j, d in ups]
    for o in NEAR:
        pl.semaphore_signal(ready, inc=1, device_id=device(o), device_id_type=MESH)

    for f in range(4):
        field = state[1 + f] if f < 3 else energy
        ybs[0, f * B:(f + 1) * B] = pack_rows(field, R - 2, 2)
        ybs[1, f * B:(f + 1) * B] = pack_rows(field, 0, 2)
    for j, start, beyond in ((0, H, H - 1), (1, 0, H)):
        yrs[j, 0:X // 2] = pack_rows(state[0], start, H)
        yrs[j, X // 2:X // 2 + A] = pack_rows(state[0], beyond, 1)
    yr, yb, xb, xe, xt = [], [], [], [], []
    for j, d in ups:
        yr.append(late.send(yrs.at[j], (0, d, 0)))
        yb.append(late.send(ybs.at[j], (0, d, 0)))
        xb.append(late.send(cons.at[0:5, plane(d, 1)], (d, 0, 0)))
        xe.append(late.send(cons.at[4, plane(d)], (d, 0, 0)))
        xt.append(late.send(cons.at[0, planes(d, D - 1, 2)], (d, 0, 0)))
    zrs[...] = pack_lanes([state[0]], 4 * DZ)
    for n, o in enumerate(XY_MOVES):
        drs[n, 0], drs[n, 1] = pack_corner(state[0], None, o)

    pl.semaphore_wait(ready, len(NEAR))
    zr, dr = {}, {}
    send_z(side, zrs, Z_NEAR, zr)
    side_slots = dict(zr)
    for n, o in enumerate(XY_MOVES):
        dr[o] = late_rho.send(drs.at[n], o)
    zr_far = {}
    send_z(late_rho, zrs, Z_EDGE, zr_far)
    side.arrived()
    send_z(late_rho, zrs, Z_VERTEX, zr_far)

    first.arrived()
    zmerged = [merge_lanes(g0[za[1] + v], g0[za[0] + v], 4) for v in range(2)]

    def near(f):
        y = unpack_rows(g0[ya[1] + f * A:ya[1] + (f + 1) * A], g0[ya[0] + f * A:ya[0] + (f + 1) * A], 1)
        z = cat(*unpack_lanes(zmerged[f // 4], [(f % 4) * X + p for p in range(X)], 4))
        return cat(g0[xa[0] + f][None], state[f], g0[xa[1] + f][None]), y, z

    def neighbours(field):
        c, y, z = field
        m = c[1:X + 1]
        return [(c[2:X + 2], c[0:X]),
                (ring(m, y, 1, 1)[0], ring(m, y, -1, 1)[0]),
                (ring(m, z, 1, 2)[0], ring(m, z, -1, 2)[0])]

    def coefficients(inv_m, inv_n):
        ws = [[0.5 * (inv_m + inv_n[d][s]) for s in range(2)] for d in range(3)]
        return ws, ALPHA / (inv_m + ALPHA * sum(w for pair in ws for w in pair))

    def update(source, ws, scale, nbr):
        acc = source
        for d in range(3):
            for s in range(2):
                acc = acc + ws[d][s] * nbr[d][s]
        return acc * scale

    ext = [near(f) for f in range(5)]
    inv = tuple(1.0 / v for v in ext[0])
    g = []
    for k in (1, 2, 3):
        n = neighbours(tuple(m * r for m, r in zip(ext[k], inv)))
        g.append([0.5 * (n[d][0] - n[d][1]) for d in range(3)])
    div = g[0][0] + g[1][1] + g[2][2]
    source = (g[0][0] * g[0][0] + g[1][1] * g[1][1] + g[2][2] * g[2][2]
              + 2.0 * (g[0][1] * g[1][0] + g[0][2] * g[2][0] + g[1][2] * g[2][1]) + div * div)
    near_w, near_scale = coefficients(inv[0][1:X + 1], neighbours(inv))
    sigma1 = update(source, near_w, near_scale, neighbours(ext[4]))

    z_fold = jnp.where(lanes(source.shape) == DZ - 1, near_w[2][0] * roll(sigma1, -1, 2),
                       jnp.where(lanes(source.shape) == L - DZ, near_w[2][1] * roll(sigma1, 1, 2), 0.0))
    z2s[...] = pack_lanes([sigma1, source + z_fold], 2 * DZ)
    z2, d2 = {}, {}
    send_z(second, z2s, Z_VERTEX, z2)
    for n, o in enumerate(XY_MOVES):
        d2s[n, 0], d2s[n, 1] = pack_corner(sigma1, source, o)
        d2[o] = second.send(d2s.at[n], o)
    send_z(second, z2s, Z_EDGE, z2)
    y_fold = jnp.where(rows(source.shape) == H - 1, near_w[1][0] * roll(sigma1, -1, 1),
                       jnp.where(rows(source.shape) == H, near_w[1][1] * roll(sigma1, 1, 1), 0.0))
    for j, start in ((0, H), (1, 0)):
        y2s[j, 0:X // 2] = pack_rows(sigma1, start, H)
        y2s[j, X // 2:X] = pack_rows(source + y_fold, start, H)
    y2 = [second.send(y2s.at[j], (0, d, 0)) for j, d in ups]
    for j, d in ups:
        x2s[j, 0:D] = sigma1[planes(d, D)]
        x2s[j, D:2 * D] = source[planes(d, D)]
    x2s[0, D] = source[X - D] + near_w[0][1][X - D] * sigma1[X - D - 1]
    x2s[1, 2 * D - 1] = source[D - 1] + near_w[0][0][D - 1] * sigma1[D]
    x2 = [second.send(x2s.at[j], (d, 0, 0)) for j, d in ups]
    send_z(second, z2s, Z_NEAR, z2)

    late.arrived()
    core = state[0:4] + [energy]
    rho_y = unpack_rows(g1[yr[1]:yr[1] + X // 2], g1[yr[0]:yr[0] + X // 2], H)
    rho_yy = unpack_rows(g1[yr[1] + X // 2:yr[1] + X // 2 + A], g1[yr[0] + X // 2:yr[0] + X // 2 + A], 1, 1)
    xn = [[g0[xa[j] + f][None] for f in range(4)] + [g1[xe[j]][None]] for j in range(2)]
    xc = [cat(g1[xb[0] + f][None], xn[0][f], core[f], xn[1][f], g1[xb[1] + f][None]) for f in range(5)]
    yc = [rho_y] + [unpack_rows(g1[yb[1] + f * B:yb[1] + (f + 1) * B], g1[yb[0] + f * B:yb[0] + (f + 1) * B], 2)
                    for f in range(4)]
    zc = [ext[f][2] for f in range(4)] + [cat(*unpack_lanes(zmerged[1], range(X, 2 * X), 4))]

    def x_stencil(c):
        return c[0:X + 1], c[1:X + 2], c[2:X + 3], c[3:X + 4]

    def ring_stencil(c, gh, axis):
        m, p = ring(c, gh, -1, axis), ring(c, gh, 1, axis)
        return cat(*m), cat(c, gh), cat(*p), cat(*ring(p[0], p[1], 1, axis))

    def faces(st):
        m, q, p, pp = st
        sixth = 1.0 / 6.0
        return (5.0 * q + 2.0 * p - m) * sixth, (2.0 * q + 5.0 * p - pp) * sixth

    def plain_flux(s, d):
        r = 1.0 / s[0]
        v = s[1 + d] * r
        pressure = (GAMMA - 1.0) * (s[4] - 0.5 * (s[1] * s[1] + s[2] * s[2] + s[3] * s[3]) * r)
        out = [s[1 + d]]
        for k in range(3):
            out.append(s[1 + k] * v + pressure if k == d else s[1 + k] * v)
        out.append((s[4] + pressure) * v)
        return out, v

    def difference(flux, d):
        if d == 0:
            return flux[1:X + 1] - flux[0:X]
        return flux[0:X] - ring(flux[0:X], flux[X:2 * X], -1, d)[0]

    base = [None] * 5
    speed = []
    for d in range(3):
        if d == 0:
            lr = [faces(x_stencil(c)) for c in xc]
        else:
            lr = [faces(ring_stencil(c, gh, d)) for c, gh in zip(core, (None, yc, zc)[d])]
        lf, lv = plain_flux([v[0] for v in lr], d)
        rf, rv = plain_flux([v[1] for v in lr], d)
        speed.append((lv, rv))
        for k in range(5):
            flux = 0.5 * (lf[k] + rf[k]) - (0.5 * LAMBDA) * (lr[k][1] - lr[k][0])
            change = difference(flux, d)
            base[k] = change if base[k] is None else base[k] + change
    base = [core[k] - STEP_DT * base[k] for k in range(5)]
    adv_ref[0] = base[0]

    def cut(part, e, step=0):
        value, reach = part
        return value[reach - e + step:reach + X + e + step]

    def around(field, reach, beyond=None):
        c, y, z, w = field
        ec, ey, ez, ew = reach
        inner = lambda t, e, to: t[e - to:e + X + to]
        cy = [ring(cut(c, ec), cut(y, ec), s, 1) for s in (1, -1)]
        cz = [ring(cut(c, ec), cut(z, ec), s, 2) for s in (1, -1)]
        zy = [ring(cut(z, ez), cut(w, ez), s, 1) for s in (1, -1)]
        yz = [ring(cut(y, ey), cut(w, ey), s, 2) for s in (1, -1)]
        yy = [inner(t[1], ec, ey) for t in cy]
        if beyond is not None:
            yy = [jnp.where(rows(t.shape) == at, beyond, t) for t, at in zip(yy, (H - 1, H))]
        xs = lambda part, e: (cut(part, e, 1), cut(part, e, -1))
        out = [[xs(c, ec), [t[0] for t in cy], [t[0] for t in cz]],
               [xs(y, ey), yy, [t[0] for t in yz]],
               [xs(z, ez), [t[0] for t in zy], [inner(t[1], ec, ez) for t in cz]]]
        if ew is not None:
            out.append([xs(w, ew), [inner(t[1], ez, ew) for t in zy], [inner(t[1], ey, ew) for t in yz]])
        return out

    late_rho.arrived()
    reach = (D, D - 1, D - 1, D - 2)
    rho_c = cat(g1[xt[0]:xt[0] + D - 1], xc[0], g1[xt[1]:xt[1] + D - 1])
    rho_ye = cat(*unpack_corner(g3, dr, -1, False), rho_y, *unpack_corner(g3, dr, 1, False))
    rho_buf = {o: g2[at] for o, at in side_slots.items()}
    rho_buf.update({o: g3[at] for o, at in zr_far.items()})
    rho_z, rho_w = z_tiles(rho_buf, {o: o for o in rho_buf}, D, D - 1, 4 * DZ)
    inv = [1.0 / v for v in (rho_c, rho_ye, rho_z, rho_w)]
    inv = tuple(zip(inv, (D + 1, D, D, D - 1)))
    edge = jnp.zeros((D - 1, R, L), jnp.float32)
    inv_n = around(inv, reach, cat(edge, 1.0 / rho_yy, edge))
    coef = [coefficients(cut(m, e), n) for m, e, n in zip(inv, reach, inv_n)]

    def mute(t, axis):
        size = t[0].shape[axis]
        depth = H if axis == 1 else DZ
        at = iota(t[0].shape, axis)
        return [jnp.where(at == depth - 1, 0.0, t[0]), jnp.where(at == size - depth, 0.0, t[1])]

    coef[1][0][1] = mute(coef[1][0][1], 1)
    coef[2][0][2] = mute(coef[2][0][2], 2)

    second.arrived()
    zero = jnp.zeros((1, R, L), jnp.float32)
    sig_z, sig_w = z_tiles(g4, z2, D, D - 1, 2 * DZ)
    src_z, src_w = z_tiles(g4, z2, D - 1, D - 2, 2 * DZ, 1)
    y_own = [unpack_rows(g4[y2[1] + t:y2[1] + t + X // 2], g4[y2[0] + t:y2[0] + t + X // 2], H) for t in (0, X // 2)]
    field = ((cat(zero, g4[x2[0]:x2[0] + D], sigma1, g4[x2[1]:x2[1] + D], zero), D + 1),
             (cat(*unpack_corner(g4, d2, -1, False), y_own[0], *unpack_corner(g4, d2, 1, False)), D),
             (sig_z, D), (sig_w, D - 1))
    sources = [cat(g4[x2[0] + D:x2[0] + 2 * D], source, g4[x2[1] + D:x2[1] + 2 * D]),
               cat(*unpack_corner(g4, d2, -1, True), y_own[1], *unpack_corner(g4, d2, 1, True)), src_z, src_w]
    have = reach
    for sweep in range(1, SWEEPS):
        last = sweep == SWEEPS - 1
        to = (2, 0, 0, None) if last else tuple(e - sweep + 1 for e in reach)
        nbr = around(field, to)
        out = []
        for t, n in enumerate(nbr):
            s = lambda v: cut((v, have[t]), to[t])
            ws, scale = coef[t]
            out.append(update(s(sources[t]), [[s(v) for v in pair] for pair in ws], s(scale), n))
        field = tuple(zip(out, to))

    c, y, z = (v for v, _ in field)
    sigma4 = c[2:X + 2]
    out_sig_ref[...] = sigma4
    total = base[4]
    for d in range(3):
        ls, rs = faces(x_stencil(c) if d == 0 else ring_stencil(sigma4, y if d == 1 else z, d))
        lv, rv = speed[d]
        adv_ref[1 + d] = base[1 + d] - (0.5 * STEP_DT) * difference(ls + rs, d)
        total = total - (0.5 * STEP_DT) * difference(ls * lv + rs * rv, d)
    adv_ref[4] = total
    for group in groups:
        group.left()


def solution(mesh):
    sizes = tuple(mesh.shape[a] for a in AXES)

    def on_device(conserved, sigma_guess):
        X, R, L = sigma_guess.shape
        A, B, H, D = X // R, 2 * X // R, X // 2, DEPTH
        f32 = jnp.float32
        vm = lambda *shape: pltpu.VMEM((*shape, R, L), f32)
        nd = len(XY_MOVES)
        tiles = landing(X, R, sizes)
        return pl.pallas_call(
            functools.partial(kernel, sizes),
            out_shape=(pltpu.VMEM(conserved.shape, f32), pltpu.VMEM(sigma_guess.shape, f32)),
            in_specs=[pl.BlockSpec(memory_space=pl.ANY)] * 2,
            out_specs=(pl.BlockSpec(memory_space=pltpu.VMEM),) * 2,
            scratch_shapes=[
                vm(5, X), vm(X), *[vm(n) for n in tiles],
                vm(2, 5 * A), vm(2), vm(2, 4 * B), vm(2, H + A), vm(), vm(nd, 2),
                vm(2, 2 * D), vm(2, 2 * H), vm(), vm(nd, 2),
                pltpu.SemaphoreType.DMA((2,)),
                pltpu.SemaphoreType.REGULAR,
                pltpu.SemaphoreType.DMA((len(tiles),)),
                pltpu.SemaphoreType.DMA((len(tiles),)),
            ],
            compiler_params=pltpu.CompilerParams(collective_id=0, has_side_effects=True),
        )(conserved, sigma_guess)

    specs = (P(None, "gx", "gy", "gz"), P("gx", "gy", "gz"))
    return jax.shard_map(on_device, mesh=mesh, in_specs=specs, out_specs=specs, check_vma=False)
```

```python
import functools
import itertools

import jax
import jax.numpy as jnp
from jax import lax
from jax.experimental import pallas as pl
from jax.experimental.pallas import tpu as pltpu
from jax.sharding import PartitionSpec as P

SWEEPS = 4
ALPHA = 10.0
GAMMA = 1.4
LAMBDA = 3.0
STEP_DT = 0.4
DEPTH = SWEEPS
MESH = pl.DeviceIdType.MESH
AXES = ("gx", "gy", "gz")

OFFSETS = [o for o in itertools.product((-1, 0, 1), repeat=3) if any(o)]
NEAR = [(0, 1, 0), (0, -1, 0), (1, 0, 0), (-1, 0, 0), (0, 0, 1), (0, 0, -1)]
XY_MOVES = [o for o in OFFSETS if o[0] != 0 and o[1] != 0 and o[2] == 0]
Z_NEAR = [(0, 0, 1), (0, 0, -1)]
Z_VERTEX = [o for o in OFFSETS if all(o)]
Z_EDGE = [o for o in OFFSETS if o[2] != 0 and o not in Z_NEAR and o not in Z_VERTEX]


def iota(shape, dim):
    return lax.broadcasted_iota(jnp.int32, shape, dim)


def roll(value, shift, axis):
    size = value.shape[axis]
    shift = shift % size
    return value if shift == 0 else pltpu.roll(value, shift, axis)


def ring(core, ghost, step, axis):
    size = core.shape[axis]
    a, b = roll(core, -step, axis), roll(ghost, -step, axis)
    edge = iota(core.shape, axis) == (size - 1 if step == 1 else 0)
    return jnp.where(edge, b, a), jnp.where(edge, a, b)


def distinct(moves, sizes):
    first = {}
    return {o: first.setdefault(tuple(v % s for v, s in zip(o, sizes)), o) for o in moves}


def landing(X, R, sizes):
    count = lambda moves: len(set(distinct(moves, sizes).values()))
    A, B, H = X // R, 2 * X // R, X // 2
    return [
        2 * (5 * A + 5 + 2),
        2 * (H + A + 4 * B + 5 + 1 + DEPTH - 1),
        count(Z_NEAR),
        2 * len(XY_MOVES) + count(Z_EDGE) + count(Z_VERTEX),
        2 * len(XY_MOVES) + count(Z_NEAR) + count(Z_EDGE) + count(Z_VERTEX) + 2 * 2 * H + 2 * 2 * DEPTH,
    ]


def kernel(sizes, cons_hbm, sig_hbm, adv_ref, out_sig_ref, cons, sig, g0, g1, g2, g3, g4,
           yas, zas, ybs, yrs, zrs, drs, x2s, y2s, z2s, d2s, in_sem, ready, send_sem, recv_sem):
    X, R, L = sig.shape
    H, D, DZ = R // 2, DEPTH, L // (4 * X)
    me = [lax.axis_index(a) for a in AXES]

    def device(offset):
        return {a: lax.rem(me[i] + offset[i] + sizes[i], sizes[i]) for i, a in enumerate(AXES)}

    load_c = pltpu.make_async_copy(cons_hbm, cons, in_sem.at[0])
    load_s = pltpu.make_async_copy(sig_hbm, sig, in_sem.at[1])
    load_c.start()
    load_s.start()
    barrier = pltpu.get_barrier_semaphore()
    for o in NEAR:
        pl.semaphore_signal(barrier, inc=1, device_id=device(o), device_id_type=MESH)

    class Group:
        def __init__(self, n, buf):
            self.n, self.buf, self.used = n, buf, 0

        def copy(self, src, dst, offset):
            return pltpu.make_async_remote_copy(
                src_ref=src, dst_ref=dst, send_sem=send_sem.at[self.n], recv_sem=recv_sem.at[self.n],
                device_id=device(offset), device_id_type=MESH)

        def send(self, src, offset):
            at = self.used
            if len(src.shape) == 2:
                self.used += 1
                self.copy(src, self.buf.at[at], offset).start()
            else:
                self.used += src.shape[0]
                self.copy(src, self.buf.at[at:self.used], offset).start()
            return at

        def arrived(self):
            assert self.used == self.buf.shape[0]
            self.copy(self.buf, self.buf, NEAR[0]).wait_recv()

        def left(self):
            self.copy(self.buf, self.buf, NEAR[0]).wait_send()

    groups = [Group(n, buf) for n, buf in enumerate((g0, g1, g2, g3, g4))]
    first, late, side, late_rho, second = groups

    rows = lambda shape: iota(shape, len(shape) - 2)
    lanes = lambda shape: iota(shape, len(shape) - 1)

    def pack_rows(field, first, n):
        size = X * n // R
        out = field[0:size]
        r = rows(out.shape)
        for g in range(1, R // n):
            part = roll(field[g * size:(g + 1) * size], n * g, 1)
            out = jnp.where((r + (2 * R - first - n * g)) % R < n, part, out)
        return out

    def unpack_rows(after, before, n, reach=0):
        low = rows(after.shape) < H
        return jnp.concatenate(
            [jnp.where(low, roll(after, -n * g - reach, 1), roll(before, reach - n * g, 1)) for g in range(R // n)],
            axis=0)

    lane2, row2 = lanes((R, L)), rows((R, L))
    low2 = row2 < H

    def pack_lanes(fields, width):
        out = jnp.zeros((R, L), jnp.float32)
        for k, tile in enumerate(f[p] for f in fields for p in range(X)):
            out = jnp.where(((lane2 + width // 2) % L) // width == k, roll(tile, width * k, 1), out)
        return out

    def merge_lanes(after, before, width):
        return jnp.where(lanes(after.shape) % width < width // 2, after, before)

    def unpack_lanes(packed, ks, width):
        return [roll(packed, -width * k, 1)[None] for k in ks]

    def pack_corner(f, s, o):
        a1, a2, a3, a4 = (f[X - a if o[0] == 1 else a - 1] for a in range(1, 5))
        if o[1] == 1:
            one = jnp.where(row2 >= H, a1, jnp.where(row2 >= 1, roll(a2, -H, 0), roll(a4, 1, 0)))
            two = roll(a3, 2, 0)
        else:
            one = jnp.where(row2 < H, a1, jnp.where(row2 < R - 1, roll(a2, H, 0), roll(a4, -1, 0)))
            two = roll(a3, -2, 0)
        if s is not None:
            s1, s2, s3 = (s[X - a if o[0] == 1 else a - 1] for a in range(1, 4))
            if o[1] == 1:
                two = jnp.where(row2 > H, s1, jnp.where(row2 == H, roll(s3, 1 - H, 0),
                                                        jnp.where(row2 >= 2, roll(s2, -H, 0), two)))
            else:
                two = jnp.where(row2 < H - 1, s1, jnp.where(row2 == H - 1, roll(s3, H - 1, 0),
                                                            jnp.where(row2 < R - 2, roll(s2, H, 0), two)))
        return one, two

    def unpack_corner(buf, slots, dx, source):
        after, before = slots[(-dx, -1, 0)], slots[(-dx, 1, 0)]
        fa, fb, sa, sb = buf[after], buf[before], buf[after + 1], buf[before + 1]
        if source:
            out = [jnp.where(low2, sa, sb), roll(jnp.where(low2, sb, sa), H, 0),
                   jnp.where(low2, roll(sa, 1 - H, 0), roll(sb, H - 1, 0))]
        else:
            out = [jnp.where(low2, fa, fb), roll(jnp.where(low2, fb, fa), H, 0),
                   jnp.where(low2, roll(sa, 2, 0), roll(sb, -2, 0)),
                   jnp.where(low2, roll(fa, 1, 0), roll(fb, -1, 0))]
        out = [v[None] for v in out]
        return out if dx == 1 else out[::-1]

    def cat(*parts):
        return jnp.concatenate(parts, axis=0)

    ups = ((0, 1), (1, -1))

    def plane(d, back=0):
        return X - 1 - back if d == 1 else back

    def planes(d, count, back=0):
        return slice(X - count - back, X - back) if d == 1 else slice(back, back + count)

    def send_z(group, src_ref, moves, slots):
        for o, same in distinct(moves, sizes).items():
            slots[o] = group.send(src_ref, o) if o == same else slots[same]

    def z_tiles(buf, slots, e, ew, width, f=0):
        def of(dx, dy):
            return merge_lanes(buf[slots[(-dx, -dy, -1)]], buf[slots[(-dx, -dy, 1)]], width)

        def diag(dx):
            return jnp.where(low2, of(dx, 1), of(dx, -1))

        k = f * X
        spread = lambda t, e: cat(*unpack_lanes(t(-1), range(k + X - e, k + X), width),
                                  *unpack_lanes(t(0), range(k, k + X), width),
                                  *unpack_lanes(t(1), range(k, k + e), width))
        return spread(lambda dx: of(dx, 0), e), spread(diag, ew)

    load_c.wait()
    load_s.wait()
    state = [cons[f] for f in range(4)] + [sig[...]]
    energy = cons[4]
    A, B = X // R, 2 * X // R
    for f in range(5):
        yas[0, f * A:(f + 1) * A] = pack_rows(state[f], R - 1, 1)
        yas[1, f * A:(f + 1) * A] = pack_rows(state[f], 0, 1)
    zas[0] = pack_lanes(state[0:4], 4)
    zas[1] = pack_lanes([state[4], energy], 4)
    pl.semaphore_wait(barrier, len(NEAR))
    ya = [first.send(yas.at[j], (0, d, 0)) for j, d in ups]
    xa = []
    for j, d in ups:
        xa.append(first.send(cons.at[0:4, plane(d)], (d, 0, 0)))
        first.send(sig.at[plane(d)], (d, 0, 0))
    za = [first.send(zas, (0, 0, d)) for j, d in ups]
    for o in NEAR:
        pl.semaphore_signal(ready, inc=1, device_id=device(o), device_id_type=MESH)

    for f in range(4):
        field = state[1 + f] if f < 3 else energy
        ybs[0, f * B:(f + 1) * B] = pack_rows(field, R - 2, 2)
        ybs[1, f * B:(f + 1) * B] = pack_rows(field, 0, 2)
    for j, start, beyond in ((0, H, H - 1), (1, 0, H)):
        yrs[j, 0:X // 2] = pack_rows(state[0], start, H)
        yrs[j, X // 2:X // 2 + A] = pack_rows(state[0], beyond, 1)
    yr, yb, xb, xe, xt = [], [], [], [], []
    for j, d in ups:
        yr.append(late.send(yrs.at[j], (0, d, 0)))
        yb.append(late.send(ybs.at[j], (0, d, 0)))
        xb.append(late.send(cons.at[0:5, plane(d, 1)], (d, 0, 0)))
        xe.append(late.send(cons.at[4, plane(d)], (d, 0, 0)))
        xt.append(late.send(cons.at[0, planes(d, D - 1, 2)], (d, 0, 0)))
    zrs[...] = pack_lanes([state[0]], 4 * DZ)
    for n, o in enumerate(XY_MOVES):
        drs[n, 0], drs[n, 1] = pack_corner(state[0], None, o)

    pl.semaphore_wait(ready, len(NEAR))
    zr, dr = {}, {}
    send_z(side, zrs, Z_NEAR, zr)
    side_slots = dict(zr)
    for n, o in enumerate(XY_MOVES):
        dr[o] = late_rho.send(drs.at[n], o)
    zr_far = {}
    send_z(late_rho, zrs, Z_EDGE, zr_far)
    side.arrived()
    send_z(late_rho, zrs, Z_VERTEX, zr_far)

    first.arrived()
    zmerged = [merge_lanes(g0[za[1] + v], g0[za[0] + v], 4) for v in range(2)]

    def near(f):
        y = unpack_rows(g0[ya[1] + f * A:ya[1] + (f + 1) * A], g0[ya[0] + f * A:ya[0] + (f + 1) * A], 1)
        z = cat(*unpack_lanes(zmerged[f // 4], [(f % 4) * X + p for p in range(X)], 4))
        return cat(g0[xa[0] + f][None], state[f], g0[xa[1] + f][None]), y, z

    def neighbours(field):
        c, y, z = field
        m = c[1:X + 1]
        return [(c[2:X + 2], c[0:X]),
                (ring(m, y, 1, 1)[0], ring(m, y, -1, 1)[0]),
                (ring(m, z, 1, 2)[0], ring(m, z, -1, 2)[0])]

    def coefficients(inv_m, inv_n):
        ws = [[0.5 * (inv_m + inv_n[d][s]) for s in range(2)] for d in range(3)]
        return ws, ALPHA / (inv_m + ALPHA * sum(w for pair in ws for w in pair))

    def update(source, ws, scale, nbr):
        acc = source
        for d in range(3):
            for s in range(2):
                acc = acc + ws[d][s] * nbr[d][s]
        return acc * scale

    ext = [near(f) for f in range(5)]
    inv = tuple(1.0 / v for v in ext[0])
    g = []
    for k in (1, 2, 3):
        n = neighbours(tuple(m * r for m, r in zip(ext[k], inv)))
        g.append([0.5 * (n[d][0] - n[d][1]) for d in range(3)])
    div = g[0][0] + g[1][1] + g[2][2]
    source = (g[0][0] * g[0][0] + g[1][1] * g[1][1] + g[2][2] * g[2][2]
              + 2.0 * (g[0][1] * g[1][0] + g[0][2] * g[2][0] + g[1][2] * g[2][1]) + div * div)
    near_w, near_scale = coefficients(inv[0][1:X + 1], neighbours(inv))
    sigma1 = update(source, near_w, near_scale, neighbours(ext[4]))

    z_fold = jnp.where(lanes(source.shape) == DZ - 1, near_w[2][0] * roll(sigma1, -1, 2),
                       jnp.where(lanes(source.shape) == L - DZ, near_w[2][1] * roll(sigma1, 1, 2), 0.0))
    z2s[...] = pack_lanes([sigma1, source + z_fold], 2 * DZ)
    z2, d2 = {}, {}
    send_z(second, z2s, Z_VERTEX, z2)
    for n, o in enumerate(XY_MOVES):
        d2s[n, 0], d2s[n, 1] = pack_corner(sigma1, source, o)
        d2[o] = second.send(d2s.at[n], o)
    send_z(second, z2s, Z_EDGE, z2)
    y_fold = jnp.where(rows(source.shape) == H - 1, near_w[1][0] * roll(sigma1, -1, 1),
                       jnp.where(rows(source.shape) == H, near_w[1][1] * roll(sigma1, 1, 1), 0.0))
    for j, start in ((0, H), (1, 0)):
        y2s[j, 0:X // 2] = pack_rows(sigma1, start, H)
        y2s[j, X // 2:X] = pack_rows(source + y_fold, start, H)
    y2 = [second.send(y2s.at[j], (0, d, 0)) for j, d in ups]
    for j, d in ups:
        x2s[j, 0:D] = sigma1[planes(d, D)]
        x2s[j, D:2 * D] = source[planes(d, D)]
    x2s[0, D] = source[X - D] + near_w[0][1][X - D] * sigma1[X - D - 1]
    x2s[1, 2 * D - 1] = source[D - 1] + near_w[0][0][D - 1] * sigma1[D]
    x2 = [second.send(x2s.at[j], (d, 0, 0)) for j, d in ups]
    send_z(second, z2s, Z_NEAR, z2)

    late.arrived()
    core = state[0:4] + [energy]
    rho_y = unpack_rows(g1[yr[1]:yr[1] + X // 2], g1[yr[0]:yr[0] + X // 2], H)
    rho_yy = unpack_rows(g1[yr[1] + X // 2:yr[1] + X // 2 + A], g1[yr[0] + X // 2:yr[0] + X // 2 + A], 1, 1)
    xn = [[g0[xa[j] + f][None] for f in range(4)] + [g1[xe[j]][None]] for j in range(2)]
    xc = [cat(g1[xb[0] + f][None], xn[0][f], core[f], xn[1][f], g1[xb[1] + f][None]) for f in range(5)]
    yc = [rho_y] + [unpack_rows(g1[yb[1] + f * B:yb[1] + (f + 1) * B], g1[yb[0] + f * B:yb[0] + (f + 1) * B], 2)
                    for f in range(4)]
    zc = [ext[f][2] for f in range(4)] + [cat(*unpack_lanes(zmerged[1], range(X, 2 * X), 4))]

    def x_stencil(c):
        return c[0:X + 1], c[1:X + 2], c[2:X + 3], c[3:X + 4]

    def ring_stencil(c, gh, axis):
        m, p = ring(c, gh, -1, axis), ring(c, gh, 1, axis)
        return cat(*m), cat(c, gh), cat(*p), cat(*ring(p[0], p[1], 1, axis))

    def faces(st):
        m, q, p, pp = st
        sixth = 1.0 / 6.0
        return (5.0 * q + 2.0 * p - m) * sixth, (2.0 * q + 5.0 * p - pp) * sixth

    def plain_flux(s, d):
        r = 1.0 / s[0]
        v = s[1 + d] * r
        pressure = (GAMMA - 1.0) * (s[4] - 0.5 * (s[1] * s[1] + s[2] * s[2] + s[3] * s[3]) * r)
        out = [s[1 + d]]
        for k in range(3):
            out.append(s[1 + k] * v + pressure if k == d else s[1 + k] * v)
        out.append((s[4] + pressure) * v)
        return out, v

    def difference(flux, d):
        if d == 0:
            return flux[1:X + 1] - flux[0:X]
        return flux[0:X] - ring(flux[0:X], flux[X:2 * X], -1, d)[0]

    base = [None] * 5
    speed = []
    for d in range(3):
        if d == 0:
            lr = [faces(x_stencil(c)) for c in xc]
        else:
            lr = [faces(ring_stencil(c, gh, d)) for c, gh in zip(core, (None, yc, zc)[d])]
        lf, lv = plain_flux([v[0] for v in lr], d)
        rf, rv = plain_flux([v[1] for v in lr], d)
        speed.append((lv, rv))
        for k in range(5):
            flux = 0.5 * (lf[k] + rf[k]) - (0.5 * LAMBDA) * (lr[k][1] - lr[k][0])
            change = difference(flux, d)
            base[k] = change if base[k] is None else base[k] + change
    base = [core[k] - STEP_DT * base[k] for k in range(5)]
    adv_ref[0] = base[0]

    def cut(part, e, step=0):
        value, reach = part
        return value[reach - e + step:reach + X + e + step]

    def around(field, reach, beyond=None):
        c, y, z, w = field
        ec, ey, ez, ew = reach
        inner = lambda t, e, to: t[e - to:e + X + to]
        cy = [ring(cut(c, ec), cut(y, ec), s, 1) for s in (1, -1)]
        cz = [ring(cut(c, ec), cut(z, ec), s, 2) for s in (1, -1)]
        zy = [ring(cut(z, ez), cut(w, ez), s, 1) for s in (1, -1)]
        yz = [ring(cut(y, ey), cut(w, ey), s, 2) for s in (1, -1)]
        yy = [inner(t[1], ec, ey) for t in cy]
        if beyond is not None:
            yy = [jnp.where(rows(t.shape) == at, beyond, t) for t, at in zip(yy, (H - 1, H))]
        xs = lambda part, e: (cut(part, e, 1), cut(part, e, -1))
        out = [[xs(c, ec), [t[0] for t in cy], [t[0] for t in cz]],
               [xs(y, ey), yy, [t[0] for t in yz]],
               [xs(z, ez), [t[0] for t in zy], [inner(t[1], ec, ez) for t in cz]]]
        if ew is not None:
            out.append([xs(w, ew), [inner(t[1], ez, ew) for t in zy], [inner(t[1], ey, ew) for t in yz]])
        return out

    late_rho.arrived()
    reach = (D, D - 1, D - 1, D - 2)
    rho_c = cat(g1[xt[0]:xt[0] + D - 1], xc[0], g1[xt[1]:xt[1] + D - 1])
    rho_ye = cat(*unpack_corner(g3, dr, -1, False), rho_y, *unpack_corner(g3, dr, 1, False))
    rho_buf = {o: g2[at] for o, at in side_slots.items()}
    rho_buf.update({o: g3[at] for o, at in zr_far.items()})
    rho_z, rho_w = z_tiles(rho_buf, {o: o for o in rho_buf}, D, D - 1, 4 * DZ)
    inv = [1.0 / v for v in (rho_c, rho_ye, rho_z, rho_w)]
    inv = tuple(zip(inv, (D + 1, D, D, D - 1)))
    edge = jnp.zeros((D - 1, R, L), jnp.float32)
    inv_n = around(inv, reach, cat(edge, 1.0 / rho_yy, edge))
    coef = [coefficients(cut(m, e), n) for m, e, n in zip(inv, reach, inv_n)]

    def mute(t, axis):
        size = t[0].shape[axis]
        depth = H if axis == 1 else DZ
        at = iota(t[0].shape, axis)
        return [jnp.where(at == depth - 1, 0.0, t[0]), jnp.where(at == size - depth, 0.0, t[1])]

    coef[1][0][1] = mute(coef[1][0][1], 1)
    coef[2][0][2] = mute(coef[2][0][2], 2)

    second.arrived()
    zero = jnp.zeros((1, R, L), jnp.float32)
    sig_z, sig_w = z_tiles(g4, z2, D, D - 1, 2 * DZ)
    src_z, src_w = z_tiles(g4, z2, D - 1, D - 2, 2 * DZ, 1)
    y_own = [unpack_rows(g4[y2[1] + t:y2[1] + t + X // 2], g4[y2[0] + t:y2[0] + t + X // 2], H) for t in (0, X // 2)]
    field = ((cat(zero, g4[x2[0]:x2[0] + D], sigma1, g4[x2[1]:x2[1] + D], zero), D + 1),
             (cat(*unpack_corner(g4, d2, -1, False), y_own[0], *unpack_corner(g4, d2, 1, False)), D),
             (sig_z, D), (sig_w, D - 1))
    sources = [cat(g4[x2[0] + D:x2[0] + 2 * D], source, g4[x2[1] + D:x2[1] + 2 * D]),
               cat(*unpack_corner(g4, d2, -1, True), y_own[1], *unpack_corner(g4, d2, 1, True)), src_z, src_w]
    have = reach
    for sweep in range(1, SWEEPS):
        last = sweep == SWEEPS - 1
        to = (2, 0, 0, None) if last else tuple(e - sweep + 1 for e in reach)
        nbr = around(field, to)
        out = []
        for t, n in enumerate(nbr):
            s = lambda v: cut((v, have[t]), to[t])
            ws, scale = coef[t]
            out.append(update(s(sources[t]), [[s(v) for v in pair] for pair in ws], s(scale), n))
        field = tuple(zip(out, to))

    c, y, z = (v for v, _ in field)
    sigma4 = c[2:X + 2]
    out_sig_ref[...] = sigma4
    total = base[4]
    for d in range(3):
        ls, rs = faces(x_stencil(c) if d == 0 else ring_stencil(sigma4, y if d == 1 else z, d))
        lv, rv = speed[d]
        adv_ref[1 + d] = base[1 + d] - (0.5 * STEP_DT) * difference(ls + rs, d)
        total = total - (0.5 * STEP_DT) * difference(ls * lv + rs * rv, d)
    adv_ref[4] = total
    for group in groups:
        group.left()


def write(adv, sig, adv_hbm, sig_hbm, sem):
    copies = [pltpu.make_async_copy(src, dst, sem.at[n])
              for n, (src, dst) in enumerate(((adv, adv_hbm), (sig, sig_hbm)))]
    for copy in copies:
        copy.start()
    for copy in copies:
        copy.wait()


def solution(mesh):
    sizes = tuple(mesh.shape[a] for a in AXES)

    def on_device(conserved, sigma_guess):
        X, R, L = sigma_guess.shape
        A, B, H, D = X // R, 2 * X // R, X // 2, DEPTH
        f32 = jnp.float32
        vm = lambda *shape: pltpu.VMEM((*shape, R, L), f32)
        nd = len(XY_MOVES)
        tiles = landing(X, R, sizes)
        outs = pl.pallas_call(
            functools.partial(kernel, sizes),
            out_shape=(pltpu.VMEM(conserved.shape, f32), pltpu.VMEM(sigma_guess.shape, f32)),
            in_specs=[pl.BlockSpec(memory_space=pl.ANY)] * 2,
            out_specs=(pl.BlockSpec(memory_space=pltpu.VMEM),) * 2,
            scratch_shapes=[
                vm(5, X), vm(X), *[vm(n) for n in tiles],
                vm(2, 5 * A), vm(2), vm(2, 4 * B), vm(2, H + A), vm(), vm(nd, 2),
                vm(2, 2 * D), vm(2, 2 * H), vm(), vm(nd, 2),
                pltpu.SemaphoreType.DMA((2,)),
                pltpu.SemaphoreType.REGULAR,
                pltpu.SemaphoreType.DMA((len(tiles),)),
                pltpu.SemaphoreType.DMA((len(tiles),)),
            ],
            compiler_params=pltpu.CompilerParams(collective_id=0, has_side_effects=True),
        )(conserved, sigma_guess)
        return pl.pallas_call(
            write,
            out_shape=tuple(jax.ShapeDtypeStruct(a.shape, f32) for a in (conserved, sigma_guess)),
            in_specs=[pl.BlockSpec(memory_space=pltpu.VMEM)] * 2,
            out_specs=(pl.BlockSpec(memory_space=pl.ANY),) * 2,
            scratch_shapes=[pltpu.SemaphoreType.DMA((2,))],
        )(*(pltpu.with_memory_space_constraint(v, pltpu.VMEM) for v in outs))

    specs = (P(None, "gx", "gy", "gz"), P("gx", "gy", "gz"))
    return jax.shard_map(on_device, mesh=mesh, in_specs=specs, out_specs=specs, check_vma=False)
```

```python
import functools
import itertools

import jax
import jax.numpy as jnp
from jax import lax
from jax.experimental import pallas as pl
from jax.experimental.pallas import tpu as pltpu
from jax.sharding import PartitionSpec as P

SWEEPS = 4
ALPHA = 10.0
GAMMA = 1.4
LAMBDA = 3.0
STEP_DT = 0.4
DEPTH = SWEEPS
MESH = pl.DeviceIdType.MESH
AXES = ("gx", "gy", "gz")

OFFSETS = [o for o in itertools.product((-1, 0, 1), repeat=3) if any(o)]
NEAR = [(0, 1, 0), (0, -1, 0), (1, 0, 0), (-1, 0, 0), (0, 0, 1), (0, 0, -1)]
XY_MOVES = [o for o in OFFSETS if o[0] != 0 and o[1] != 0 and o[2] == 0]
Z_NEAR = [(0, 0, 1), (0, 0, -1)]
Z_VERTEX = [o for o in OFFSETS if all(o)]
Z_EDGE = [o for o in OFFSETS if o[2] != 0 and o not in Z_NEAR and o not in Z_VERTEX]


def iota(shape, dim):
    return lax.broadcasted_iota(jnp.int32, shape, dim)


def roll(value, shift, axis):
    size = value.shape[axis]
    shift = shift % size
    return value if shift == 0 else pltpu.roll(value, shift, axis)


def ring(core, ghost, step, axis):
    size = core.shape[axis]
    a, b = roll(core, -step, axis), roll(ghost, -step, axis)
    edge = iota(core.shape, axis) == (size - 1 if step == 1 else 0)
    return jnp.where(edge, b, a), jnp.where(edge, a, b)


def distinct(moves, sizes):
    first = {}
    return {o: first.setdefault(tuple(v % s for v, s in zip(o, sizes)), o) for o in moves}


def landing(X, R, sizes):
    count = lambda moves: len(set(distinct(moves, sizes).values()))
    A, B, H = X // R, 2 * X // R, X // 2
    return [
        2 * (5 * A + 5 + 2),
        2 * (H + A + 4 * B + 5 + 1 + DEPTH - 1),
        count(Z_NEAR),
        2 * len(XY_MOVES) + count(Z_EDGE) + count(Z_VERTEX),
        2 * len(XY_MOVES) + count(Z_NEAR) + count(Z_EDGE) + count(Z_VERTEX) + 2 * 2 * H + 2 * 2 * DEPTH,
    ]


def kernel(sizes, cons_hbm, sig_hbm, adv_ref, out_sig_ref, cons, sig, g0, g1, g2, g3, g4,
           yas, zas, ybs, yrs, zrs, drs, x2s, y2s, z2s, d2s, in_sem, ready, send_sem, recv_sem):
    X, R, L = sig.shape
    H, D, DZ = R // 2, DEPTH, L // (4 * X)
    wide = 2 * DZ
    me = [lax.axis_index(a) for a in AXES]

    def device(offset):
        return {a: lax.rem(me[i] + offset[i] + sizes[i], sizes[i]) for i, a in enumerate(AXES)}

    load_c = pltpu.make_async_copy(cons_hbm, cons, in_sem.at[0])
    load_s = pltpu.make_async_copy(sig_hbm, sig, in_sem.at[1])
    load_c.start()
    load_s.start()
    barrier = pltpu.get_barrier_semaphore()
    for o in NEAR:
        pl.semaphore_signal(barrier, inc=1, device_id=device(o), device_id_type=MESH)

    class Group:
        def __init__(self, n, buf):
            self.n, self.buf, self.used = n, buf, 0

        def copy(self, src, dst, offset):
            return pltpu.make_async_remote_copy(
                src_ref=src, dst_ref=dst, send_sem=send_sem.at[self.n], recv_sem=recv_sem.at[self.n],
                device_id=device(offset), device_id_type=MESH)

        def send(self, src, offset):
            at = self.used
            if len(src.shape) == 2:
                self.used += 1
                self.copy(src, self.buf.at[at], offset).start()
            else:
                self.used += src.shape[0]
                self.copy(src, self.buf.at[at:self.used], offset).start()
            return at

        def arrived(self):
            assert self.used == self.buf.shape[0]
            self.copy(self.buf, self.buf, NEAR[0]).wait_recv()

        def left(self):
            self.copy(self.buf, self.buf, NEAR[0]).wait_send()

    groups = [Group(n, buf) for n, buf in enumerate((g0, g1, g2, g3, g4))]
    first, late, side, late_rho, second = groups

    rows = lambda shape: iota(shape, len(shape) - 2)
    lanes = lambda shape: iota(shape, len(shape) - 1)

    def pack_rows(field, first, n):
        size = X * n // R
        out = field[0:size]
        r = rows(out.shape)
        for g in range(1, R // n):
            part = roll(field[g * size:(g + 1) * size], n * g, 1)
            out = jnp.where((r + (2 * R - first - n * g)) % R < n, part, out)
        return out

    def unpack_rows(after, before, n, reach=0):
        low = rows(after.shape) < H
        return jnp.concatenate(
            [jnp.where(low, roll(after, -n * g - reach, 1), roll(before, reach - n * g, 1)) for g in range(R // n)],
            axis=0)

    lane2, row2 = lanes((R, L)), rows((R, L))
    low2 = row2 < H

    def pack_lanes(fields, width):
        out = jnp.zeros((R, L), jnp.float32)
        for k, tile in enumerate(f[p] for f in fields for p in range(X)):
            out = jnp.where(((lane2 + width // 2) % L) // width == k, roll(tile, width * k, 1), out)
        return out

    slot2 = ((lane2 + DZ) % L) // wide
    side2 = lane2 % wide >= DZ

    def pack_planes(out, value, ps):
        for k, p in enumerate(ps):
            out = jnp.where(slot2 == p % (2 * X), roll(value[k], wide * p, 1), out)
        return out

    def pack_corner(f, s, o):
        a1, a2, a3, a4 = (f[X - a if o[0] == 1 else a - 1] for a in range(1, 5))
        if o[1] == 1:
            one = jnp.where(row2 >= H, a1, jnp.where(row2 >= 1, roll(a2, -H, 0), roll(a4, 1, 0)))
            two = roll(a3, 2, 0)
        else:
            one = jnp.where(row2 < H, a1, jnp.where(row2 < R - 1, roll(a2, H, 0), roll(a4, -1, 0)))
            two = roll(a3, -2, 0)
        if s is not None:
            s1, s2, s3 = (s[X - a if o[0] == 1 else a - 1] for a in range(1, 4))
            if o[1] == 1:
                two = jnp.where(row2 > H, s1, jnp.where(row2 == H, roll(s3, 1 - H, 0),
                                                        jnp.where(row2 >= 2, roll(s2, -H, 0), two)))
            else:
                two = jnp.where(row2 < H - 1, s1, jnp.where(row2 == H - 1, roll(s3, H - 1, 0),
                                                            jnp.where(row2 < R - 2, roll(s2, H, 0), two)))
        return one, two

    def unpack_corner(buf, slots, dx, source):
        after, before = slots[(-dx, -1, 0)], slots[(-dx, 1, 0)]
        fa, fb, sa, sb = buf[after], buf[before], buf[after + 1], buf[before + 1]
        if source:
            out = [jnp.where(low2, sa, sb), roll(jnp.where(low2, sb, sa), H, 0),
                   jnp.where(low2, roll(sa, 1 - H, 0), roll(sb, H - 1, 0))]
        else:
            out = [jnp.where(low2, fa, fb), roll(jnp.where(low2, fb, fa), H, 0),
                   jnp.where(low2, roll(sa, 2, 0), roll(sb, -2, 0)),
                   jnp.where(low2, roll(fa, 1, 0), roll(fb, -1, 0))]
        out = [v[None] for v in out]
        return out if dx == 1 else out[::-1]

    def cat(*parts):
        return jnp.concatenate(parts, axis=0)

    ups = ((0, 1), (1, -1))

    def plane(d, back=0):
        return X - 1 - back if d == 1 else back

    def planes(d, count, back=0):
        return slice(X - count - back, X - back) if d == 1 else slice(back, back + count)

    def send_z(group, src_ref, moves, slots):
        for o, same in distinct(moves, sizes).items():
            slots[o] = group.send(src_ref, o) if o == same else slots[same]

    def z_side(of, dy, dz, f):
        own, after, before = (of(dx, dy, dz) for dx in (0, 1, -1))
        if f == 0:
            return jnp.where(slot2 < X, own, roll(jnp.where(slot2 < X // 2, after, before), L // 2, 1))
        return jnp.where(slot2 < X, roll(own, L // 2, 1), jnp.where(slot2 < X + X // 2, after, before))

    def sides(own, low, high):
        return jnp.where(side2, low, own), jnp.where(side2, own, high)

    def z_pairs(of, f, own_z, own_w):
        z = [z_side(of, 0, dz, f) for dz in (-1, 1)]
        w = [jnp.where(low2, z_side(of, 1, dz, f), z_side(of, -1, dz, f)) for dz in (-1, 1)]
        return sides(own_z, *z), sides(own_w, *w)

    load_c.wait()
    load_s.wait()
    state = [cons[f] for f in range(4)] + [sig[...]]
    energy = cons[4]
    A, B = X // R, 2 * X // R
    for f in range(5):
        yas[0, f * A:(f + 1) * A] = pack_rows(state[f], R - 1, 1)
        yas[1, f * A:(f + 1) * A] = pack_rows(state[f], 0, 1)
    zas[0] = pack_lanes(state[0:4], 4)
    zas[1] = pack_lanes([state[4], energy], 4)
    pl.semaphore_wait(barrier, len(NEAR))
    ya = [first.send(yas.at[j], (0, d, 0)) for j, d in ups]
    xa = []
    for j, d in ups:
        xa.append(first.send(cons.at[0:4, plane(d)], (d, 0, 0)))
        first.send(sig.at[plane(d)], (d, 0, 0))
    za = [first.send(zas, (0, 0, d)) for j, d in ups]
    for o in NEAR:
        pl.semaphore_signal(ready, inc=1, device_id=device(o), device_id_type=MESH)

    for f in range(4):
        field = state[1 + f] if f < 3 else energy
        ybs[0, f * B:(f + 1) * B] = pack_rows(field, R - 2, 2)
        ybs[1, f * B:(f + 1) * B] = pack_rows(field, 0, 2)
    for j, start, beyond in ((0, H, H - 1), (1, 0, H)):
        yrs[j, 0:X // 2] = pack_rows(state[0], start, H)
        yrs[j, X // 2:X // 2 + A] = pack_rows(state[0], beyond, 1)
    yr, yb, xb, xe, xt = [], [], [], [], []
    for j, d in ups:
        yr.append(late.send(yrs.at[j], (0, d, 0)))
        yb.append(late.send(ybs.at[j], (0, d, 0)))
        xb.append(late.send(cons.at[0:5, plane(d, 1)], (d, 0, 0)))
        xe.append(late.send(cons.at[4, plane(d)], (d, 0, 0)))
        xt.append(late.send(cons.at[0, planes(d, D - 1, 2)], (d, 0, 0)))
    lane3 = lanes(energy.shape)
    row3 = rows(energy.shape)
    rho_zz = jnp.where(lane3 == DZ - 1, roll(state[0], -1, 2), roll(state[0], 1, 2))
    rho_own = pack_lanes([state[0], rho_zz], wide)
    zrs[...] = rho_own
    for n, o in enumerate(XY_MOVES):
        drs[n, 0], drs[n, 1] = pack_corner(state[0], None, o)

    pl.semaphore_wait(ready, len(NEAR))
    zr, dr = {}, {}
    send_z(side, zrs, Z_NEAR, zr)
    side_slots = dict(zr)
    for n, o in enumerate(XY_MOVES):
        dr[o] = late_rho.send(drs.at[n], o)
    zr_far = {}
    send_z(late_rho, zrs, Z_EDGE, zr_far)
    side.arrived()
    send_z(late_rho, zrs, Z_VERTEX, zr_far)

    inv0 = 1.0 / state[0]
    fields = [inv0] + [state[k] * inv0 for k in (1, 2, 3)] + [state[4]]
    own = [[[roll(v, -s, axis) for s in (1, -1)] for axis in (1, 2)] for v in fields]
    region = ((lane2 + 2) % L) // (4 * X)

    first.arrived()

    def to_speed(t):
        r = 1.0 / t[0]
        return [r] + [m * r for m in t[1:4]] + [t[4]]

    xg = [to_speed([g0[xa[j] + f] for f in range(5)]) for j in range(2)]
    yg = [to_speed([g0[ya[j] + f * A:ya[j] + (f + 1) * A] for f in range(5)]) for j in range(2)]
    zmerged = [jnp.where(lane2 % 4 < 2, g0[za[1] + v], g0[za[0] + v]) for v in range(2)]
    zinv = 1.0 / jnp.where(region == 0, zmerged[0], 1.0)
    shifted = [roll(zinv, 4 * X * k, 1) for k in (1, 2, 3)]
    zspeed = zmerged[0] * jnp.where(region == 1, shifted[0], jnp.where(region == 2, shifted[1], shifted[2]))
    zspeed = jnp.where(region == 0, zinv, zspeed)

    def neighbours(f):
        v, ((yp, ym), (zp, zm)) = fields[f], own[f]
        after = cat(*[roll(yg[1][f], R - 1 - p, 1) for p in range(R)])
        before = cat(*[roll(yg[0][f], 1 - p, 1) for p in range(R)])
        t, k = (zspeed, f * X) if f < 4 else (zmerged[1], 0)
        high = cat(*[roll(t, L - 1 - 4 * (k + p), 1)[None] for p in range(X)])
        low = cat(*[roll(t, 1 - 4 * (k + p), 1)[None] for p in range(X)])
        return [(cat(v[1:X], xg[1][f][None]), cat(xg[0][f][None], v[0:X - 1])),
                (jnp.where(row3 == R - 1, after, yp), jnp.where(row3 == 0, before, ym)),
                (jnp.where(lane3 == L - 1, high, zp), jnp.where(lane3 == 0, low, zm))]

    def coefficients(inv_m, inv_n):
        ws = [[inv_m + inv_n[d][s] for s in range(2)] for d in range(3)]
        scale = ALPHA / (2.0 * inv_m + ALPHA * sum(w for pair in ws for w in pair))
        return [[w * scale for w in pair] for pair in ws], scale

    def update(source, ws, nbr):
        acc = source
        for d in range(3):
            for s in range(2):
                acc = acc + ws[d][s] * nbr[d][s]
        return acc

    near_w, near_scale = coefficients(inv0, neighbours(0))
    g = []
    for k in (1, 2, 3):
        n = neighbours(k)
        g.append([n[d][0] - n[d][1] for d in range(3)])
    div = g[0][0] + g[1][1] + g[2][2]
    source = (g[0][0] * g[0][0] + g[1][1] * g[1][1] + g[2][2] * g[2][2]
              + 2.0 * (g[0][1] * g[1][0] + g[0][2] * g[2][0] + g[1][2] * g[2][1]) + div * div)
    source = source * (0.5 * near_scale)
    sigma1 = update(source, near_w, neighbours(4))

    z_fold = jnp.where(lane3 == DZ - 1, near_w[2][0] * roll(sigma1, -1, 2),
                       jnp.where(lane3 == L - DZ, near_w[2][1] * roll(sigma1, 1, 2), 0.0))
    z_own = pack_lanes([sigma1, source + z_fold], wide)
    z2s[...] = z_own
    z2, d2 = {}, {}
    send_z(second, z2s, Z_VERTEX, z2)
    for n, o in enumerate(XY_MOVES):
        d2s[n, 0], d2s[n, 1] = pack_corner(sigma1, source, o)
        d2[o] = second.send(d2s.at[n], o)
    send_z(second, z2s, Z_EDGE, z2)
    y_fold = jnp.where(row3 == H - 1, near_w[1][0] * roll(sigma1, -1, 1),
                       jnp.where(row3 == H, near_w[1][1] * roll(sigma1, 1, 1), 0.0))
    for j, start in ((0, H), (1, 0)):
        y2s[j, 0:X // 2] = pack_rows(sigma1, start, H)
        y2s[j, X // 2:X] = pack_rows(source + y_fold, start, H)
    y2 = [second.send(y2s.at[j], (0, d, 0)) for j, d in ups]
    for j, d in ups:
        x2s[j, 0:D] = sigma1[planes(d, D)]
        x2s[j, D:2 * D] = source[planes(d, D)]
    x2s[0, D] = source[X - D] + near_w[0][1][X - D] * sigma1[X - D - 1]
    x2s[1, 2 * D - 1] = source[D - 1] + near_w[0][0][D - 1] * sigma1[D]
    x2 = [second.send(x2s.at[j], (d, 0, 0)) for j, d in ups]
    send_z(second, z2s, Z_NEAR, z2)

    late.arrived()
    core = state[0:4] + [energy]
    rho_y = unpack_rows(g1[yr[1]:yr[1] + X // 2], g1[yr[0]:yr[0] + X // 2], H)
    rho_yy = unpack_rows(g1[yr[1] + X // 2:yr[1] + X // 2 + A], g1[yr[0] + X // 2:yr[0] + X // 2 + A], 1, 1)
    xn = [[g0[xa[j] + f][None] for f in range(4)] + [g1[xe[j]][None]] for j in range(2)]
    xc = [cat(g1[xb[0] + f][None], xn[0][f], core[f], xn[1][f], g1[xb[1] + f][None]) for f in range(5)]
    yc = [rho_y] + [unpack_rows(g1[yb[1] + f * B:yb[1] + (f + 1) * B], g1[yb[0] + f * B:yb[0] + (f + 1) * B], 2)
                    for f in range(4)]
    zc = [cat(*[roll(zmerged[f // 4], -4 * (f * X + p), 1)[None] for p in range(X)]) for f in range(4)]
    zc.append(cat(*[roll(zmerged[1], -4 * (X + p), 1)[None] for p in range(X)]))

    def x_stencil(c):
        return c[0:X + 1], c[1:X + 2], c[2:X + 3], c[3:X + 4]

    def ring_stencil(c, gh, axis):
        m, p = ring(c, gh, -1, axis), ring(c, gh, 1, axis)
        return cat(*m), cat(c, gh), cat(*p), cat(*ring(p[0], p[1], 1, axis))

    def faces(st):
        m, q, p, pp = st
        sixth = 1.0 / 6.0
        return (5.0 * q + 2.0 * p - m) * sixth, (2.0 * q + 5.0 * p - pp) * sixth

    def plain_flux(s, d):
        r = 1.0 / s[0]
        v = s[1 + d] * r
        pressure = (GAMMA - 1.0) * (s[4] - 0.5 * (s[1] * s[1] + s[2] * s[2] + s[3] * s[3]) * r)
        out = [s[1 + d]]
        for k in range(3):
            out.append(s[1 + k] * v + pressure if k == d else s[1 + k] * v)
        out.append((s[4] + pressure) * v)
        return out, v

    def difference(flux, d):
        if d == 0:
            return flux[1:X + 1] - flux[0:X]
        return flux[0:X] - ring(flux[0:X], flux[X:2 * X], -1, d)[0]

    base = [None] * 5
    speed = []
    for d in range(3):
        if d == 0:
            lr = [faces(x_stencil(c)) for c in xc]
        else:
            lr = [faces(ring_stencil(c, gh, d)) for c, gh in zip(core, (None, yc, zc)[d])]
        lf, lv = plain_flux([v[0] for v in lr], d)
        rf, rv = plain_flux([v[1] for v in lr], d)
        speed.append((lv, rv))
        for k in range(5):
            flux = 0.5 * (lf[k] + rf[k]) - (0.5 * LAMBDA) * (lr[k][1] - lr[k][0])
            change = difference(flux, d)
            base[k] = change if base[k] is None else base[k] + change
    base = [core[k] - STEP_DT * base[k] for k in range(5)]
    adv_ref[0] = base[0]

    def lower(v, d):
        return v[0:X] if d == 0 else ring(v[0:X], v[X:2 * X], -1, d)[0]

    part = []
    for d, (lv, rv) in enumerate(speed):
        ll, rl = lower(lv, d), lower(rv, d)
        lv, rv = (lv[1:X + 1], rv[1:X + 1]) if d == 0 else (lv[0:X], rv[0:X])
        k = -0.5 * STEP_DT / 6.0
        part.append([k * ll, k * (-lv - 5.0 * ll - 2.0 * rl), k * (5.0 * lv + 2.0 * rv - 2.0 * ll - 5.0 * rl),
                     k * (2.0 * lv + 5.0 * rv + rl), -k * rv])
    middle = part[0][2] + part[1][2] + part[2][2]

    def pick(part, ps, step=0):
        value, reach = part
        return cat(*[value[reach + a + step:reach + b + step] for a, b in ps])

    def z_shift(value, ps, pair, step, by=1):
        at = [p for a, b in ps for p in range(a, b)]
        lane = lanes(value.shape)
        if step == 1:
            ghost, edge = [roll(pair[1], L - by - wide * p, 1) for p in at], lane >= L - by
        else:
            ghost, edge = [roll(pair[0], by - wide * p, 1) for p in at], lane < by
        return jnp.where(edge, cat(*[v[None] for v in ghost]), roll(value, -step * by, 2))

    def around_planes(c, y, pair, ps):
        m = pick(c, ps)
        cy = [ring(m, pick(y, ps), s, 1) for s in (1, -1)]
        z = [z_shift(m, ps, pair, s) for s in (1, -1)]
        return [(pick(c, ps, 1), pick(c, ps, -1)), [t[0] for t in cy], z], [t[1] for t in cy]

    def around_ghosts(y, yy, pair, e):
        ps = [(-e, X + e)]
        return [(pick(y, ps, 1), pick(y, ps, -1)), yy, [z_shift(pick(y, ps), ps, pair, s) for s in (1, -1)]]

    def around_packed(z, w):
        out = [], []
        for zt, wt in zip(z, w):
            zy = [ring(zt, wt, s, 0) for s in (1, -1)]
            for to, t, k in ((out[0], zt, 0), (out[1], wt, 1)):
                to.append([(roll(t, -wide, 1), roll(t, wide, 1)), [v[k] for v in zy], (roll(t, -1, 1), roll(t, 1, 1))])
        return out

    late_rho.arrived()
    rho_of = lambda dx, dy, dz: g2[side_slots[(0, 0, -dz)]] if dx == dy == 0 else g3[zr_far[(-dx, -dy, -dz)]]
    every = range(-D, X + D)
    outer = [p for p in every if not 0 <= p < X]
    rho_c = cat(g1[xt[0]:xt[0] + D - 1], xc[0], g1[xt[1]:xt[1] + D - 1])
    rho_ye = cat(*unpack_corner(g3, dr, -1, False), rho_y, *unpack_corner(g3, dr, 1, False))
    rho_z, rho_w = z_pairs(rho_of, 0, pack_planes(rho_own, pick((rho_c, D + 1), [(-D, 0), (X, X + D)]), outer),
                           pack_planes(rho_own, rho_ye, every))
    inv_c, inv_y = (1.0 / rho_c, D + 1), (1.0 / rho_ye, D)
    inv_z, inv_w = [1.0 / t for t in rho_z], [1.0 / t for t in rho_w]
    beyond = [1.0 / z_side(rho_of, 0, dz, 1) for dz in (-1, 1)]
    far_coef = coefficients(pick(inv_c, [(-D, 0), (X, X + D)]),
                            around_planes(inv_c, inv_y, inv_z, [(-D, 0), (X, X + D)])[0])[0]
    coef_c = [[cat(far[0:D], mine, far[D:2 * D]) for far, mine in zip(*pair)] for pair in zip(far_coef, near_w)]
    e = D - 1
    rim = jnp.zeros((e, R, L), jnp.float32)
    yy = around_planes(inv_c, inv_y, inv_z, [(-e, X + e)])[1]
    inv_yy = cat(rim, 1.0 / rho_yy, rim)
    row = rows(inv_yy.shape)
    yy = [jnp.where(row == at, inv_yy, t) for t, at in zip(yy, (H - 1, H))]
    coef_y = coefficients(pick(inv_y, [(-e, X + e)]), around_ghosts(inv_y, yy, inv_w, e))[0]
    coef_y[1] = [jnp.where(row == at, 0.0, t) for t, at in zip(coef_y[1], (H - 1, H))]
    zn, wn = around_packed(inv_z, inv_w)
    coef_z, coef_w = [], []
    for j, at in ((0, DZ), (1, DZ - 1)):
        last = lane2 % wide == at
        pair = list(zn[j][2])
        pair[1 - j] = jnp.where(last, beyond[j], pair[1 - j])
        ws = coefficients(inv_z[j], [*zn[j][0:2], pair])[0]
        ws[2][1 - j] = jnp.where(last, 0.0, ws[2][1 - j])
        coef_z.append(ws)
        coef_w.append(coefficients(inv_w[j], wn[j])[0])

    second.arrived()
    zero = jnp.zeros((1, R, L), jnp.float32)
    sig_of = lambda dx, dy, dz: g4[z2[(-dx, -dy, -dz)]]
    sx, qx = [cat(g4[x2[0] + t:x2[0] + t + D], g4[x2[1] + t:x2[1] + t + D]) for t in (0, D)]
    sy, qy = [unpack_rows(g4[y2[1] + t:y2[1] + t + X // 2], g4[y2[0] + t:y2[0] + t + X // 2], H) for t in (0, X // 2)]
    sy = cat(*unpack_corner(g4, d2, -1, False), sy, *unpack_corner(g4, d2, 1, False))
    qy = cat(*unpack_corner(g4, d2, -1, True), qy, *unpack_corner(g4, d2, 1, True))
    z, w = z_pairs(sig_of, 0, pack_planes(z_own, sx, outer), pack_planes(z_own, sy, every))
    q_own = roll(z_own, L // 2, 1)
    qz, qw = z_pairs(sig_of, 1, pack_planes(q_own, qx, outer), pack_planes(q_own, qy, range(-e, X + e)))
    c, y = (cat(zero, sx[0:D], sigma1, sx[D:2 * D], zero), D + 1), (sy, D)
    qc = cat(qx[0:D], source, qx[D:2 * D])
    for sweep in range(1, SWEEPS):
        last = sweep == SWEEPS - 1
        ec, ey = D + 1 - sweep, 0 if last else D - sweep
        cn, yy = around_planes(c, y, z, [(-ec, X + ec)])
        yn = around_ghosts(y, [t[ec - ey:ec + X + ey] for t in yy], w, ey)
        zn, wn = around_packed(z, w)
        cut = lambda v, have, e: v[have - e:have + X + e]
        c = update(cut(qc, D, ec), [[cut(v, D, ec) for v in pair] for pair in coef_c], cn), ec
        y = update(cut(qy, D - 1, ey), [[cut(v, D - 1, ey) for v in pair] for pair in coef_y], yn), ey
        z = [update(qz[j], coef_z[j], zn[j]) for j in range(2)]
        if not last:
            w = [update(qw[j], coef_w[j], wn[j]) for j in range(2)]

    own_planes = [(0, X)]
    sigma4 = pick(c, own_planes)
    out_sig_ref[...] = sigma4

    def y_shift(step, by):
        edge = row3 >= R - by if step == 1 else row3 < by
        return jnp.where(edge, roll(y[0], -step * by, 1), roll(sigma4, -step * by, 1))

    total = base[4] + middle * sigma4
    for d in range(3):
        if d == 0:
            near_far = [[pick(c, own_planes, s * by) for by in (1, 2)] for s in (1, -1)]
        elif d == 1:
            near_far = [[y_shift(s, by) for by in (1, 2)] for s in (1, -1)]
        else:
            near_far = [[z_shift(sigma4, own_planes, z, s, by) for by in (1, 2)] for s in (1, -1)]
        (p1, p2), (m1, m2) = near_far
        adv_ref[1 + d] = base[1 + d] + ((-4.0 * STEP_DT / 6.0) * (p1 - m1) + (0.5 * STEP_DT / 6.0) * (p2 - m2))
        a = part[d]
        total = total + (a[0] * m2 + a[1] * m1 + a[3] * p1 + a[4] * p2)
    adv_ref[4] = total
    for group in groups:
        group.left()


def write(adv, sig, adv_hbm, sig_hbm, sem):
    copies = [pltpu.make_async_copy(src, dst, sem.at[n])
              for n, (src, dst) in enumerate(((adv, adv_hbm), (sig, sig_hbm)))]
    for copy in copies:
        copy.start()
    for copy in copies:
        copy.wait()


def solution(mesh):
    sizes = tuple(mesh.shape[a] for a in AXES)

    def on_device(conserved, sigma_guess):
        X, R, L = sigma_guess.shape
        A, B, H, D = X // R, 2 * X // R, X // 2, DEPTH
        f32 = jnp.float32
        vm = lambda *shape: pltpu.VMEM((*shape, R, L), f32)
        nd = len(XY_MOVES)
        tiles = landing(X, R, sizes)
        outs = pl.pallas_call(
            functools.partial(kernel, sizes),
            out_shape=(pltpu.VMEM(conserved.shape, f32), pltpu.VMEM(sigma_guess.shape, f32)),
            in_specs=[pl.BlockSpec(memory_space=pl.ANY)] * 2,
            out_specs=(pl.BlockSpec(memory_space=pltpu.VMEM),) * 2,
            scratch_shapes=[
                vm(5, X), vm(X), *[vm(n) for n in tiles],
                vm(2, 5 * A), vm(2), vm(2, 4 * B), vm(2, H + A), vm(), vm(nd, 2),
                vm(2, 2 * D), vm(2, 2 * H), vm(), vm(nd, 2),
                pltpu.SemaphoreType.DMA((2,)),
                pltpu.SemaphoreType.REGULAR,
                pltpu.SemaphoreType.DMA((len(tiles),)),
                pltpu.SemaphoreType.DMA((len(tiles),)),
            ],
            compiler_params=pltpu.CompilerParams(collective_id=0, has_side_effects=True),
        )(conserved, sigma_guess)
        return pl.pallas_call(
            write,
            out_shape=tuple(jax.ShapeDtypeStruct(a.shape, f32) for a in (conserved, sigma_guess)),
            in_specs=[pl.BlockSpec(memory_space=pltpu.VMEM)] * 2,
            out_specs=(pl.BlockSpec(memory_space=pl.ANY),) * 2,
            scratch_shapes=[pltpu.SemaphoreType.DMA((2,))],
        )(*(pltpu.with_memory_space_constraint(v, pltpu.VMEM) for v in outs))

    specs = (P(None, "gx", "gy", "gz"), P("gx", "gy", "gz"))
    return jax.shard_map(on_device, mesh=mesh, in_specs=specs, out_specs=specs, check_vma=False)
```

```python
import functools
import itertools

import jax
import jax.numpy as jnp
from jax import lax
from jax.experimental import pallas as pl
from jax.experimental.pallas import tpu as pltpu
from jax.sharding import PartitionSpec as P

SWEEPS = 4
ALPHA = 10.0
GAMMA = 1.4
LAMBDA = 3.0
STEP_DT = 0.4
DEPTH = SWEEPS
MESH = pl.DeviceIdType.MESH
AXES = ("gx", "gy", "gz")

OFFSETS = [o for o in itertools.product((-1, 0, 1), repeat=3) if any(o)]
NEAR = [(0, 1, 0), (0, -1, 0), (1, 0, 0), (-1, 0, 0), (0, 0, 1), (0, 0, -1)]
XY_MOVES = [o for o in OFFSETS if o[0] != 0 and o[1] != 0 and o[2] == 0]
Z_NEAR = [(0, 0, 1), (0, 0, -1)]
Z_VERTEX = [o for o in OFFSETS if all(o)]
Z_EDGE = [o for o in OFFSETS if o[2] != 0 and o not in Z_NEAR and o not in Z_VERTEX]


def iota(shape, dim):
    return lax.broadcasted_iota(jnp.int32, shape, dim)


def roll(value, shift, axis):
    size = value.shape[axis]
    shift = shift % size
    return value if shift == 0 else pltpu.roll(value, shift, axis)


def ring(core, ghost, step, axis):
    size = core.shape[axis]
    a, b = roll(core, -step, axis), roll(ghost, -step, axis)
    edge = iota(core.shape, axis) == (size - 1 if step == 1 else 0)
    return jnp.where(edge, b, a), jnp.where(edge, a, b)


def distinct(moves, sizes):
    first = {}
    return {o: first.setdefault(tuple(v % s for v, s in zip(o, sizes)), o) for o in moves}


def z_rows(offset, R):
    n = R if offset[1] == 0 else DEPTH - 1 if offset[0] else DEPTH
    return slice(0, n) if offset[1] == -1 else slice(R - n, R)


def landing(X, R, sizes):
    sent = lambda moves: sorted(set(distinct(moves, sizes).values()))
    rows = [z_rows(o, R).stop - z_rows(o, R).start for o in sent(Z_EDGE) + sent(Z_VERTEX)]
    part = [n for n in rows if n < R]
    full = len(rows) - len(part)
    A, B, H = X // R, 2 * X // R, X // 2
    near, corner = len(sent(Z_NEAR)), 2 * len(XY_MOVES)
    return [
        (2 * (5 * A + 5 + 2), []),
        (2 * (H + A + 4 * B + 5 + 1 + DEPTH - 1), []),
        (near, []),
        (corner + full, part),
        (corner + near + full + 2 * 2 * H + 2 * 2 * DEPTH, part),
    ]


def kernel(sizes, cons_hbm, sig_hbm, adv_ref, out_sig_ref, cons, sig, g0, g1, g2, g3, g4, t3, t4,
           yas, zas, ybs, yrs, zrs, drs, x2s, y2s, z2s, d2s, in_sem, ready, send_sem, recv_sem):
    X, R, L = sig.shape
    H, D, DZ = R // 2, DEPTH, L // (4 * X)
    wide = 2 * DZ
    me = [lax.axis_index(a) for a in AXES]

    def device(offset):
        return {a: lax.rem(me[i] + offset[i] + sizes[i], sizes[i]) for i, a in enumerate(AXES)}

    load_c = pltpu.make_async_copy(cons_hbm, cons, in_sem.at[0])
    load_s = pltpu.make_async_copy(sig_hbm, sig, in_sem.at[1])
    load_c.start()
    load_s.start()
    barrier = pltpu.get_barrier_semaphore()
    for o in NEAR:
        pl.semaphore_signal(barrier, inc=1, device_id=device(o), device_id_type=MESH)

    class Group:
        def __init__(self, n, buf, spare):
            self.n, self.buf, self.spare, self.used, self.rows = n, buf, spare, 0, 0

        def copy(self, src, dst, offset):
            return pltpu.make_async_remote_copy(
                src_ref=src, dst_ref=dst, send_sem=send_sem.at[self.n], recv_sem=recv_sem.at[self.n],
                device_id=device(offset), device_id_type=MESH)

        def send(self, src, offset, part=None):
            at = self.used
            if part is not None:
                self.used += 1
                self.rows += part.stop - part.start
                self.copy(src.at[part], self.buf.at[at, part], offset).start()
            elif len(src.shape) == 2:
                self.used, self.rows = at + 1, self.rows + R
                self.copy(src, self.buf.at[at], offset).start()
            else:
                self.used, self.rows = at + src.shape[0], self.rows + R * src.shape[0]
                self.copy(src, self.buf.at[at:self.used], offset).start()
            return at

        def whole(self):
            assert self.used == self.buf.shape[0] and self.rows == self.spare.shape[0] * self.spare.shape[1]
            return self.copy(self.spare, self.spare, NEAR[0])

        def arrived(self):
            self.whole().wait_recv()

        def left(self):
            self.whole().wait_send()

    groups = [Group(n, buf, size) for n, (buf, size) in enumerate(zip((g0, g1, g2, g3, g4), (g0, g1, g2, t3, t4)))]
    first, late, side, late_rho, second = groups

    rows = lambda shape: iota(shape, len(shape) - 2)
    lanes = lambda shape: iota(shape, len(shape) - 1)

    def pack_rows(field, first, n):
        size = X * n // R
        out = field[0:size]
        r = rows(out.shape)
        for g in range(1, R // n):
            part = roll(field[g * size:(g + 1) * size], n * g, 1)
            out = jnp.where((r + (2 * R - first - n * g)) % R < n, part, out)
        return out

    def unpack_rows(after, before, n, reach=0):
        low = rows(after.shape) < H
        return jnp.concatenate(
            [jnp.where(low, roll(after, -n * g - reach, 1), roll(before, reach - n * g, 1)) for g in range(R // n)],
            axis=0)

    lane2, row2 = lanes((R, L)), rows((R, L))
    low2 = row2 < H

    def pack_lanes(fields, width):
        out = jnp.zeros((R, L), jnp.float32)
        for k, tile in enumerate(f[p] for f in fields for p in range(X)):
            out = jnp.where(((lane2 + width // 2) % L) // width == k, roll(tile, width * k, 1), out)
        return out

    slot2 = ((lane2 + DZ) % L) // wide
    side2 = lane2 % wide >= DZ

    def pack_planes(out, value, ps):
        for k, p in enumerate(ps):
            out = jnp.where(slot2 == p % (2 * X), roll(value[k], wide * p, 1), out)
        return out

    def pack_corner(f, s, o):
        a1, a2, a3, a4 = (f[X - a if o[0] == 1 else a - 1] for a in range(1, 5))
        if o[1] == 1:
            one = jnp.where(row2 >= H, a1, jnp.where(row2 >= 1, roll(a2, -H, 0), roll(a4, 1, 0)))
            two = roll(a3, 2, 0)
        else:
            one = jnp.where(row2 < H, a1, jnp.where(row2 < R - 1, roll(a2, H, 0), roll(a4, -1, 0)))
            two = roll(a3, -2, 0)
        if s is not None:
            s1, s2, s3 = (s[X - a if o[0] == 1 else a - 1] for a in range(1, 4))
            if o[1] == 1:
                two = jnp.where(row2 > H, s1, jnp.where(row2 == H, roll(s3, 1 - H, 0),
                                                        jnp.where(row2 >= 2, roll(s2, -H, 0), two)))
            else:
                two = jnp.where(row2 < H - 1, s1, jnp.where(row2 == H - 1, roll(s3, H - 1, 0),
                                                            jnp.where(row2 < R - 2, roll(s2, H, 0), two)))
        return one, two

    def unpack_corner(buf, slots, dx, source):
        after, before = slots[(-dx, -1, 0)], slots[(-dx, 1, 0)]
        fa, fb, sa, sb = buf[after], buf[before], buf[after + 1], buf[before + 1]
        if source:
            out = [jnp.where(low2, sa, sb), roll(jnp.where(low2, sb, sa), H, 0),
                   jnp.where(low2, roll(sa, 1 - H, 0), roll(sb, H - 1, 0))]
        else:
            out = [jnp.where(low2, fa, fb), roll(jnp.where(low2, fb, fa), H, 0),
                   jnp.where(low2, roll(sa, 2, 0), roll(sb, -2, 0)),
                   jnp.where(low2, roll(fa, 1, 0), roll(fb, -1, 0))]
        out = [v[None] for v in out]
        return out if dx == 1 else out[::-1]

    def cat(*parts):
        return jnp.concatenate(parts, axis=0)

    ups = ((0, 1), (1, -1))

    def plane(d, back=0):
        return X - 1 - back if d == 1 else back

    def planes(d, count, back=0):
        return slice(X - count - back, X - back) if d == 1 else slice(back, back + count)

    def send_z(group, src_ref, moves, slots):
        for o, same in distinct(moves, sizes).items():
            slots[o] = group.send(src_ref, o, z_rows(o, R)) if o == same else slots[same]

    def z_side(of, dy, dz, f):
        own, after, before = (of(dx, dy, dz) for dx in (0, 1, -1))
        if f == 0:
            return jnp.where(slot2 < X, own, roll(jnp.where(slot2 < X // 2, after, before), L // 2, 1))
        return jnp.where(slot2 < X, roll(own, L // 2, 1), jnp.where(slot2 < X + X // 2, after, before))

    def sides(own, low, high):
        return jnp.where(side2, low, own), jnp.where(side2, own, high)

    def z_pairs(of, f, own_z, own_w):
        z = [z_side(of, 0, dz, f) for dz in (-1, 1)]
        w = [jnp.where(low2, z_side(of, 1, dz, f), z_side(of, -1, dz, f)) for dz in (-1, 1)]
        return sides(own_z, *z), sides(own_w, *w)

    load_c.wait()
    load_s.wait()
    state = [cons[f] for f in range(4)] + [sig[...]]
    energy = cons[4]
    A, B = X // R, 2 * X // R
    for f in range(5):
        yas[0, f * A:(f + 1) * A] = pack_rows(state[f], R - 1, 1)
        yas[1, f * A:(f + 1) * A] = pack_rows(state[f], 0, 1)
    zas[0] = pack_lanes(state[0:4], 4)
    zas[1] = pack_lanes([state[4], energy], 4)
    pl.semaphore_wait(barrier, len(NEAR))
    ya = [first.send(yas.at[j], (0, d, 0)) for j, d in ups]
    xa = []
    for j, d in ups:
        xa.append(first.send(cons.at[0:4, plane(d)], (d, 0, 0)))
        first.send(sig.at[plane(d)], (d, 0, 0))
    za = [first.send(zas, (0, 0, d)) for j, d in ups]
    for o in NEAR:
        pl.semaphore_signal(ready, inc=1, device_id=device(o), device_id_type=MESH)

    for f in range(4):
        field = state[1 + f] if f < 3 else energy
        ybs[0, f * B:(f + 1) * B] = pack_rows(field, R - 2, 2)
        ybs[1, f * B:(f + 1) * B] = pack_rows(field, 0, 2)
    for j, start, beyond in ((0, H, H - 1), (1, 0, H)):
        yrs[j, 0:X // 2] = pack_rows(state[0], start, H)
        yrs[j, X // 2:X // 2 + A] = pack_rows(state[0], beyond, 1)
    yr, yb, xb, xe, xt = [], [], [], [], []
    for j, d in ups:
        yr.append(late.send(yrs.at[j], (0, d, 0)))
        yb.append(late.send(ybs.at[j], (0, d, 0)))
        xb.append(late.send(cons.at[0:5, plane(d, 1)], (d, 0, 0)))
        xe.append(late.send(cons.at[4, plane(d)], (d, 0, 0)))
        xt.append(late.send(cons.at[0, planes(d, D - 1, 2)], (d, 0, 0)))
    lane3 = lanes(energy.shape)
    row3 = rows(energy.shape)
    rho_zz = jnp.where(lane3 == DZ - 1, roll(state[0], -1, 2), roll(state[0], 1, 2))
    rho_own = pack_lanes([state[0], rho_zz], wide)
    zrs[...] = rho_own
    for n, o in enumerate(XY_MOVES):
        drs[n, 0], drs[n, 1] = pack_corner(state[0], None, o)

    pl.semaphore_wait(ready, len(NEAR))
    zr, dr = {}, {}
    send_z(side, zrs, Z_NEAR, zr)
    side_slots = dict(zr)
    for n, o in enumerate(XY_MOVES):
        dr[o] = late_rho.send(drs.at[n], o)
    zr_far = {}
    send_z(late_rho, zrs, Z_EDGE, zr_far)
    side.arrived()
    send_z(late_rho, zrs, Z_VERTEX, zr_far)

    inv0 = 1.0 / state[0]
    fields = [inv0] + [state[k] * inv0 for k in (1, 2, 3)] + [state[4]]
    own = [[[roll(v, -s, axis) for s in (1, -1)] for axis in (1, 2)] for v in fields]
    region = ((lane2 + 2) % L) // (4 * X)

    first.arrived()

    def to_speed(t):
        r = 1.0 / t[0]
        return [r] + [m * r for m in t[1:4]] + [t[4]]

    xg = [to_speed([g0[xa[j] + f] for f in range(5)]) for j in range(2)]
    yg = [to_speed([g0[ya[j] + f * A:ya[j] + (f + 1) * A] for f in range(5)]) for j in range(2)]
    zmerged = [jnp.where(lane2 % 4 < 2, g0[za[1] + v], g0[za[0] + v]) for v in range(2)]
    zinv = 1.0 / jnp.where(region == 0, zmerged[0], 1.0)
    shifted = [roll(zinv, 4 * X * k, 1) for k in (1, 2, 3)]
    zspeed = zmerged[0] * jnp.where(region == 1, shifted[0], jnp.where(region == 2, shifted[1], shifted[2]))
    zspeed = jnp.where(region == 0, zinv, zspeed)

    def neighbours(f):
        v, ((yp, ym), (zp, zm)) = fields[f], own[f]
        after = cat(*[roll(yg[1][f], R - 1 - p, 1) for p in range(R)])
        before = cat(*[roll(yg[0][f], 1 - p, 1) for p in range(R)])
        t, k = (zspeed, f * X) if f < 4 else (zmerged[1], 0)
        high = cat(*[roll(t, L - 1 - 4 * (k + p), 1)[None] for p in range(X)])
        low = cat(*[roll(t, 1 - 4 * (k + p), 1)[None] for p in range(X)])
        return [(cat(v[1:X], xg[1][f][None]), cat(xg[0][f][None], v[0:X - 1])),
                (jnp.where(row3 == R - 1, after, yp), jnp.where(row3 == 0, before, ym)),
                (jnp.where(lane3 == L - 1, high, zp), jnp.where(lane3 == 0, low, zm))]

    def coefficients(inv_m, inv_n):
        ws = [[inv_m + inv_n[d][s] for s in range(2)] for d in range(3)]
        scale = ALPHA / (2.0 * inv_m + ALPHA * sum(w for pair in ws for w in pair))
        return [[w * scale for w in pair] for pair in ws], scale

    def update(source, ws, nbr):
        acc = source
        for d in range(3):
            for s in range(2):
                acc = acc + ws[d][s] * nbr[d][s]
        return acc

    near_w, near_scale = coefficients(inv0, neighbours(0))
    g = []
    for k in (1, 2, 3):
        n = neighbours(k)
        g.append([n[d][0] - n[d][1] for d in range(3)])
    div = g[0][0] + g[1][1] + g[2][2]
    source = (g[0][0] * g[0][0] + g[1][1] * g[1][1] + g[2][2] * g[2][2]
              + 2.0 * (g[0][1] * g[1][0] + g[0][2] * g[2][0] + g[1][2] * g[2][1]) + div * div)
    source = source * (0.5 * near_scale)
    sigma1 = update(source, near_w, neighbours(4))

    z_fold = jnp.where(lane3 == DZ - 1, near_w[2][0] * roll(sigma1, -1, 2),
                       jnp.where(lane3 == L - DZ, near_w[2][1] * roll(sigma1, 1, 2), 0.0))
    z_own = pack_lanes([sigma1, source + z_fold], wide)
    z2s[...] = z_own
    z2, d2 = {}, {}
    send_z(second, z2s, Z_VERTEX, z2)
    for n, o in enumerate(XY_MOVES):
        d2s[n, 0], d2s[n, 1] = pack_corner(sigma1, source, o)
        d2[o] = second.send(d2s.at[n], o)
    send_z(second, z2s, Z_EDGE, z2)
    y_fold = jnp.where(row3 == H - 1, near_w[1][0] * roll(sigma1, -1, 1),
                       jnp.where(row3 == H, near_w[1][1] * roll(sigma1, 1, 1), 0.0))
    for j, start in ((0, H), (1, 0)):
        y2s[j, 0:X // 2] = pack_rows(sigma1, start, H)
        y2s[j, X // 2:X] = pack_rows(source + y_fold, start, H)
    y2 = [second.send(y2s.at[j], (0, d, 0)) for j, d in ups]
    for j, d in ups:
        x2s[j, 0:D] = sigma1[planes(d, D)]
        x2s[j, D:2 * D] = source[planes(d, D)]
    x2s[0, D] = source[X - D] + near_w[0][1][X - D] * sigma1[X - D - 1]
    x2s[1, 2 * D - 1] = source[D - 1] + near_w[0][0][D - 1] * sigma1[D]
    x2 = [second.send(x2s.at[j], (d, 0, 0)) for j, d in ups]
    send_z(second, z2s, Z_NEAR, z2)

    late.arrived()
    core = state[0:4] + [energy]
    rho_y = unpack_rows(g1[yr[1]:yr[1] + X // 2], g1[yr[0]:yr[0] + X // 2], H)
    rho_yy = unpack_rows(g1[yr[1] + X // 2:yr[1] + X // 2 + A], g1[yr[0] + X // 2:yr[0] + X // 2 + A], 1, 1)
    xn = [[g0[xa[j] + f][None] for f in range(4)] + [g1[xe[j]][None]] for j in range(2)]
    xc = [cat(g1[xb[0] + f][None], xn[0][f], core[f], xn[1][f], g1[xb[1] + f][None]) for f in range(5)]
    yc = [rho_y] + [unpack_rows(g1[yb[1] + f * B:yb[1] + (f + 1) * B], g1[yb[0] + f * B:yb[0] + (f + 1) * B], 2)
                    for f in range(4)]
    zc = [cat(*[roll(zmerged[f // 4], -4 * (f * X + p), 1)[None] for p in range(X)]) for f in range(4)]
    zc.append(cat(*[roll(zmerged[1], -4 * (X + p), 1)[None] for p in range(X)]))

    def x_stencil(c):
        return c[0:X + 1], c[1:X + 2], c[2:X + 3], c[3:X + 4]

    def ring_stencil(c, gh, axis):
        m, p = ring(c, gh, -1, axis), ring(c, gh, 1, axis)
        return cat(*m), cat(c, gh), cat(*p), cat(*ring(p[0], p[1], 1, axis))

    def faces(st):
        m, q, p, pp = st
        sixth = 1.0 / 6.0
        return (5.0 * q + 2.0 * p - m) * sixth, (2.0 * q + 5.0 * p - pp) * sixth

    def plain_flux(s, d):
        r = 1.0 / s[0]
        v = s[1 + d] * r
        pressure = (GAMMA - 1.0) * (s[4] - 0.5 * (s[1] * s[1] + s[2] * s[2] + s[3] * s[3]) * r)
        out = [s[1 + d]]
        for k in range(3):
            out.append(s[1 + k] * v + pressure if k == d else s[1 + k] * v)
        out.append((s[4] + pressure) * v)
        return out, v

    def difference(flux, d):
        if d == 0:
            return flux[1:X + 1] - flux[0:X]
        return flux[0:X] - ring(flux[0:X], flux[X:2 * X], -1, d)[0]

    base = [None] * 5
    speed = []
    for d in range(3):
        if d == 0:
            lr = [faces(x_stencil(c)) for c in xc]
        else:
            lr = [faces(ring_stencil(c, gh, d)) for c, gh in zip(core, (None, yc, zc)[d])]
        lf, lv = plain_flux([v[0] for v in lr], d)
        rf, rv = plain_flux([v[1] for v in lr], d)
        speed.append((lv, rv))
        for k in range(5):
            flux = 0.5 * (lf[k] + rf[k]) - (0.5 * LAMBDA) * (lr[k][1] - lr[k][0])
            change = difference(flux, d)
            base[k] = change if base[k] is None else base[k] + change
    base = [core[k] - STEP_DT * base[k] for k in range(5)]
    adv_ref[0] = base[0]

    def lower(v, d):
        return v[0:X] if d == 0 else ring(v[0:X], v[X:2 * X], -1, d)[0]

    part = []
    for d, (lv, rv) in enumerate(speed):
        ll, rl = lower(lv, d), lower(rv, d)
        lv, rv = (lv[1:X + 1], rv[1:X + 1]) if d == 0 else (lv[0:X], rv[0:X])
        k = -0.5 * STEP_DT / 6.0
        part.append([k * ll, k * (-lv - 5.0 * ll - 2.0 * rl), k * (5.0 * lv + 2.0 * rv - 2.0 * ll - 5.0 * rl),
                     k * (2.0 * lv + 5.0 * rv + rl), -k * rv])
    middle = part[0][2] + part[1][2] + part[2][2]

    def pick(part, ps, step=0):
        value, reach = part
        return cat(*[value[reach + a + step:reach + b + step] for a, b in ps])

    def z_shift(value, ps, pair, step, by=1):
        at = [p for a, b in ps for p in range(a, b)]
        lane = lanes(value.shape)
        if step == 1:
            ghost, edge = [roll(pair[1], L - by - wide * p, 1) for p in at], lane >= L - by
        else:
            ghost, edge = [roll(pair[0], by - wide * p, 1) for p in at], lane < by
        return jnp.where(edge, cat(*[v[None] for v in ghost]), roll(value, -step * by, 2))

    def around_planes(c, y, pair, ps):
        m = pick(c, ps)
        cy = [ring(m, pick(y, ps), s, 1) for s in (1, -1)]
        z = [z_shift(m, ps, pair, s) for s in (1, -1)]
        return [(pick(c, ps, 1), pick(c, ps, -1)), [t[0] for t in cy], z], [t[1] for t in cy]

    def around_ghosts(y, yy, pair, e):
        ps = [(-e, X + e)]
        return [(pick(y, ps, 1), pick(y, ps, -1)), yy, [z_shift(pick(y, ps), ps, pair, s) for s in (1, -1)]]

    def around_packed(z, w):
        out = [], []
        for zt, wt in zip(z, w):
            zy = [ring(zt, wt, s, 0) for s in (1, -1)]
            for to, t, k in ((out[0], zt, 0), (out[1], wt, 1)):
                to.append([(roll(t, -wide, 1), roll(t, wide, 1)), [v[k] for v in zy], (roll(t, -1, 1), roll(t, 1, 1))])
        return out

    late_rho.arrived()
    rho_of = lambda dx, dy, dz: g2[side_slots[(0, 0, -dz)]] if dx == dy == 0 else g3[zr_far[(-dx, -dy, -dz)]]
    every = range(-D, X + D)
    outer = [p for p in every if not 0 <= p < X]
    rho_c = cat(g1[xt[0]:xt[0] + D - 1], xc[0], g1[xt[1]:xt[1] + D - 1])
    rho_ye = cat(*unpack_corner(g3, dr, -1, False), rho_y, *unpack_corner(g3, dr, 1, False))
    rho_z, rho_w = z_pairs(rho_of, 0, pack_planes(rho_own, pick((rho_c, D + 1), [(-D, 0), (X, X + D)]), outer),
                           pack_planes(rho_own, rho_ye, every))
    inv_c, inv_y = (1.0 / rho_c, D + 1), (1.0 / rho_ye, D)
    inv_z, inv_w = [1.0 / t for t in rho_z], [1.0 / t for t in rho_w]
    beyond = [1.0 / z_side(rho_of, 0, dz, 1) for dz in (-1, 1)]
    far_coef = coefficients(pick(inv_c, [(-D, 0), (X, X + D)]),
                            around_planes(inv_c, inv_y, inv_z, [(-D, 0), (X, X + D)])[0])[0]
    coef_c = [[cat(far[0:D], mine, far[D:2 * D]) for far, mine in zip(*pair)] for pair in zip(far_coef, near_w)]
    e = D - 1
    rim = jnp.zeros((e, R, L), jnp.float32)
    yy = around_planes(inv_c, inv_y, inv_z, [(-e, X + e)])[1]
    inv_yy = cat(rim, 1.0 / rho_yy, rim)
    row = rows(inv_yy.shape)
    yy = [jnp.where(row == at, inv_yy, t) for t, at in zip(yy, (H - 1, H))]
    coef_y = coefficients(pick(inv_y, [(-e, X + e)]), around_ghosts(inv_y, yy, inv_w, e))[0]
    coef_y[1] = [jnp.where(row == at, 0.0, t) for t, at in zip(coef_y[1], (H - 1, H))]
    zn, wn = around_packed(inv_z, inv_w)
    coef_z, coef_w = [], []
    for j, at in ((0, DZ), (1, DZ - 1)):
        last = lane2 % wide == at
        pair = list(zn[j][2])
        pair[1 - j] = jnp.where(last, beyond[j], pair[1 - j])
        ws = coefficients(inv_z[j], [*zn[j][0:2], pair])[0]
        ws[2][1 - j] = jnp.where(last, 0.0, ws[2][1 - j])
        coef_z.append(ws)
        coef_w.append(coefficients(inv_w[j], wn[j])[0])

    second.arrived()
    zero = jnp.zeros((1, R, L), jnp.float32)
    sig_of = lambda dx, dy, dz: g4[z2[(-dx, -dy, -dz)]]
    sx, qx = [cat(g4[x2[0] + t:x2[0] + t + D], g4[x2[1] + t:x2[1] + t + D]) for t in (0, D)]
    sy, qy = [unpack_rows(g4[y2[1] + t:y2[1] + t + X // 2], g4[y2[0] + t:y2[0] + t + X // 2], H) for t in (0, X // 2)]
    sy = cat(*unpack_corner(g4, d2, -1, False), sy, *unpack_corner(g4, d2, 1, False))
    qy = cat(*unpack_corner(g4, d2, -1, True), qy, *unpack_corner(g4, d2, 1, True))
    z, w = z_pairs(sig_of, 0, pack_planes(z_own, sx, outer), pack_planes(z_own, sy, every))
    q_own = roll(z_own, L // 2, 1)
    qz, qw = z_pairs(sig_of, 1, pack_planes(q_own, qx, outer), pack_planes(q_own, qy, range(-e, X + e)))
    c, y = (cat(zero, sx[0:D], sigma1, sx[D:2 * D], zero), D + 1), (sy, D)
    qc = cat(qx[0:D], source, qx[D:2 * D])
    for sweep in range(1, SWEEPS):
        last = sweep == SWEEPS - 1
        ec, ey = D + 1 - sweep, 0 if last else D - sweep
        cn, yy = around_planes(c, y, z, [(-ec, X + ec)])
        yn = around_ghosts(y, [t[ec - ey:ec + X + ey] for t in yy], w, ey)
        zn, wn = around_packed(z, w)
        cut = lambda v, have, e: v[have - e:have + X + e]
        c = update(cut(qc, D, ec), [[cut(v, D, ec) for v in pair] for pair in coef_c], cn), ec
        y = update(cut(qy, D - 1, ey), [[cut(v, D - 1, ey) for v in pair] for pair in coef_y], yn), ey
        z = [update(qz[j], coef_z[j], zn[j]) for j in range(2)]
        if not last:
            w = [update(qw[j], coef_w[j], wn[j]) for j in range(2)]

    own_planes = [(0, X)]
    sigma4 = pick(c, own_planes)
    out_sig_ref[...] = sigma4

    def y_shift(step, by):
        edge = row3 >= R - by if step == 1 else row3 < by
        return jnp.where(edge, roll(y[0], -step * by, 1), roll(sigma4, -step * by, 1))

    total = base[4] + middle * sigma4
    for d in range(3):
        if d == 0:
            near_far = [[pick(c, own_planes, s * by) for by in (1, 2)] for s in (1, -1)]
        elif d == 1:
            near_far = [[y_shift(s, by) for by in (1, 2)] for s in (1, -1)]
        else:
            near_far = [[z_shift(sigma4, own_planes, z, s, by) for by in (1, 2)] for s in (1, -1)]
        (p1, p2), (m1, m2) = near_far
        adv_ref[1 + d] = base[1 + d] + ((-4.0 * STEP_DT / 6.0) * (p1 - m1) + (0.5 * STEP_DT / 6.0) * (p2 - m2))
        a = part[d]
        total = total + (a[0] * m2 + a[1] * m1 + a[3] * p1 + a[4] * p2)
    adv_ref[4] = total
    for group in groups:
        group.left()


def write(adv, sig, adv_hbm, sig_hbm, sem):
    copies = [pltpu.make_async_copy(src, dst, sem.at[n])
              for n, (src, dst) in enumerate(((adv, adv_hbm), (sig, sig_hbm)))]
    for copy in copies:
        copy.start()
    for copy in copies:
        copy.wait()


def solution(mesh):
    sizes = tuple(mesh.shape[a] for a in AXES)

    def on_device(conserved, sigma_guess):
        X, R, L = sigma_guess.shape
        A, B, H, D = X // R, 2 * X // R, X // 2, DEPTH
        f32 = jnp.float32
        vm = lambda *shape: pltpu.VMEM((*shape, R, L), f32)
        nd = len(XY_MOVES)
        tiles = landing(X, R, sizes)
        spare = [pltpu.VMEM((R * n + sum(part), 1, L), f32) for n, part in tiles[3:]]
        outs = pl.pallas_call(
            functools.partial(kernel, sizes),
            out_shape=(pltpu.VMEM(conserved.shape, f32), pltpu.VMEM(sigma_guess.shape, f32)),
            in_specs=[pl.BlockSpec(memory_space=pl.ANY)] * 2,
            out_specs=(pl.BlockSpec(memory_space=pltpu.VMEM),) * 2,
            scratch_shapes=[
                vm(5, X), vm(X), *[vm(n + len(part)) for n, part in tiles], *spare,
                vm(2, 5 * A), vm(2), vm(2, 4 * B), vm(2, H + A), vm(), vm(nd, 2),
                vm(2, 2 * D), vm(2, 2 * H), vm(), vm(nd, 2),
                pltpu.SemaphoreType.DMA((2,)),
                pltpu.SemaphoreType.REGULAR,
                pltpu.SemaphoreType.DMA((len(tiles),)),
                pltpu.SemaphoreType.DMA((len(tiles),)),
            ],
            compiler_params=pltpu.CompilerParams(collective_id=0, has_side_effects=True),
        )(conserved, sigma_guess)
        return pl.pallas_call(
            write,
            out_shape=tuple(jax.ShapeDtypeStruct(a.shape, f32) for a in (conserved, sigma_guess)),
            in_specs=[pl.BlockSpec(memory_space=pltpu.VMEM)] * 2,
            out_specs=(pl.BlockSpec(memory_space=pl.ANY),) * 2,
            scratch_shapes=[pltpu.SemaphoreType.DMA((2,))],
        )(*(pltpu.with_memory_space_constraint(v, pltpu.VMEM) for v in outs))

    specs = (P(None, "gx", "gy", "gz"), P("gx", "gy", "gz"))
    return jax.shard_map(on_device, mesh=mesh, in_specs=specs, out_specs=specs, check_vma=False)
```

```python
import functools
import itertools

import jax
import jax.numpy as jnp
from jax import lax
from jax.experimental import pallas as pl
from jax.experimental.pallas import tpu as pltpu
from jax.sharding import PartitionSpec as P

SWEEPS = 4
ALPHA = 10.0
GAMMA = 1.4
LAMBDA = 3.0
STEP_DT = 0.4
DEPTH = SWEEPS
MESH = pl.DeviceIdType.MESH
AXES = ("gx", "gy", "gz")

OFFSETS = [o for o in itertools.product((-1, 0, 1), repeat=3) if any(o)]
NEAR = [(0, 1, 0), (0, -1, 0), (1, 0, 0), (-1, 0, 0), (0, 0, 1), (0, 0, -1)]
XY_MOVES = [o for o in OFFSETS if o[0] != 0 and o[1] != 0 and o[2] == 0]
Z_NEAR = [(0, 0, 1), (0, 0, -1)]
Z_VERTEX = [o for o in OFFSETS if all(o)]
Z_EDGE = [o for o in OFFSETS if o[2] != 0 and o not in Z_NEAR and o not in Z_VERTEX]


def iota(shape, dim):
    return lax.broadcasted_iota(jnp.int32, shape, dim)


def roll(value, shift, axis):
    size = value.shape[axis]
    shift = shift % size
    return value if shift == 0 else pltpu.roll(value, shift, axis)


def ring(core, ghost, step, axis):
    size = core.shape[axis]
    a, b = roll(core, -step, axis), roll(ghost, -step, axis)
    edge = iota(core.shape, axis) == (size - 1 if step == 1 else 0)
    return jnp.where(edge, b, a), jnp.where(edge, a, b)


def distinct(moves, sizes):
    first = {}
    return {o: first.setdefault(tuple(v % s for v, s in zip(o, sizes)), o) for o in moves}


def z_rows(offset, R):
    n = R if offset[1] == 0 else DEPTH - 1 if offset[0] else DEPTH
    return slice(0, n) if offset[1] == -1 else slice(R - n, R)


def landing(X, R, sizes):
    sent = lambda moves: sorted(set(distinct(moves, sizes).values()))
    rows = [z_rows(o, R).stop - z_rows(o, R).start for o in sent(Z_EDGE) + sent(Z_VERTEX)]
    part = [n for n in rows if n < R]
    full = len(rows) - len(part)
    A, B, H = X // R, 2 * X // R, X // 2
    near, corner = len(sent(Z_NEAR)), 2 * len(XY_MOVES)
    return [
        (2 * (5 * A + 5 + 2), []),
        (2 * (H + A + 4 * B + 5 + 1 + DEPTH - 1), []),
        (near, []),
        (corner + full, part),
        (corner + near + full + 2 * 2 * H + 2 * 2 * DEPTH, part),
    ]


def kernel(sizes, cons_hbm, sig_hbm, adv_ref, out_sig_ref, cons, sig, g0, g1, g2, g3, g4, t3, t4, sent,
           yas, zas, ybs, yrs, zrs, drs, x2s, y2s, z2s, d2s, in_sem, ready, send_sem, recv_sem):
    X, R, L = sig.shape
    H, D, DZ = R // 2, DEPTH, L // (4 * X)
    wide = 2 * DZ
    me = [lax.axis_index(a) for a in AXES]

    def device(offset):
        return {a: lax.rem(me[i] + offset[i] + sizes[i], sizes[i]) for i, a in enumerate(AXES)}

    load_c = pltpu.make_async_copy(cons_hbm, cons, in_sem.at[0])
    load_s = pltpu.make_async_copy(sig_hbm, sig, in_sem.at[1])
    load_c.start()
    load_s.start()
    barrier = pltpu.get_barrier_semaphore()
    for o in NEAR:
        pl.semaphore_signal(barrier, inc=1, device_id=device(o), device_id_type=MESH)

    class Group:
        def __init__(self, n, buf, spare):
            self.n, self.buf, self.spare, self.used, self.rows = n, buf, spare, 0, 0

        def copy(self, src, dst, offset):
            return pltpu.make_async_remote_copy(
                src_ref=src, dst_ref=dst, send_sem=send_sem, recv_sem=recv_sem.at[self.n],
                device_id=device(offset), device_id_type=MESH)

        def send(self, src, offset, part=None):
            at = self.used
            if part is not None:
                self.used += 1
                self.rows += part.stop - part.start
                self.copy(src.at[part], self.buf.at[at, part], offset).start()
            elif len(src.shape) == 2:
                self.used, self.rows = at + 1, self.rows + R
                self.copy(src, self.buf.at[at], offset).start()
            else:
                self.used, self.rows = at + src.shape[0], self.rows + R * src.shape[0]
                self.copy(src, self.buf.at[at:self.used], offset).start()
            return at

        def arrived(self):
            assert self.used == self.buf.shape[0] and self.rows == self.spare.shape[0] * self.spare.shape[1]
            self.copy(self.spare, self.spare, NEAR[0]).wait_recv()

    groups = [Group(n, buf, size) for n, (buf, size) in enumerate(zip((g0, g1, g2, g3, g4), (g0, g1, g2, t3, t4)))]
    first, late, side, late_rho, second = groups

    rows = lambda shape: iota(shape, len(shape) - 2)
    lanes = lambda shape: iota(shape, len(shape) - 1)

    def pack_rows(field, first, n):
        size = X * n // R
        out = field[0:size]
        r = rows(out.shape)
        for g in range(1, R // n):
            part = roll(field[g * size:(g + 1) * size], n * g, 1)
            out = jnp.where((r + (2 * R - first - n * g)) % R < n, part, out)
        return out

    def unpack_rows(after, before, n, reach=0):
        low = rows(after.shape) < H
        return jnp.concatenate(
            [jnp.where(low, roll(after, -n * g - reach, 1), roll(before, reach - n * g, 1)) for g in range(R // n)],
            axis=0)

    lane2, row2 = lanes((R, L)), rows((R, L))
    low2 = row2 < H

    def pack_lanes(fields, width):
        out = jnp.zeros((R, L), jnp.float32)
        for k, tile in enumerate(f[p] for f in fields for p in range(X)):
            out = jnp.where(((lane2 + width // 2) % L) // width == k, roll(tile, width * k, 1), out)
        return out

    slot2 = ((lane2 + DZ) % L) // wide
    side2 = lane2 % wide >= DZ

    def pack_planes(out, value, ps):
        for k, p in enumerate(ps):
            out = jnp.where(slot2 == p % (2 * X), roll(value[k], wide * p, 1), out)
        return out

    def pack_corner(f, s, o):
        a1, a2, a3, a4 = (f[X - a if o[0] == 1 else a - 1] for a in range(1, 5))
        if o[1] == 1:
            one = jnp.where(row2 >= H, a1, jnp.where(row2 >= 1, roll(a2, -H, 0), roll(a4, 1, 0)))
            two = roll(a3, 2, 0)
        else:
            one = jnp.where(row2 < H, a1, jnp.where(row2 < R - 1, roll(a2, H, 0), roll(a4, -1, 0)))
            two = roll(a3, -2, 0)
        if s is not None:
            s1, s2, s3 = (s[X - a if o[0] == 1 else a - 1] for a in range(1, 4))
            if o[1] == 1:
                two = jnp.where(row2 > H, s1, jnp.where(row2 == H, roll(s3, 1 - H, 0),
                                                        jnp.where(row2 >= 2, roll(s2, -H, 0), two)))
            else:
                two = jnp.where(row2 < H - 1, s1, jnp.where(row2 == H - 1, roll(s3, H - 1, 0),
                                                            jnp.where(row2 < R - 2, roll(s2, H, 0), two)))
        return one, two

    def unpack_corner(buf, slots, dx, source):
        after, before = slots[(-dx, -1, 0)], slots[(-dx, 1, 0)]
        fa, fb, sa, sb = buf[after], buf[before], buf[after + 1], buf[before + 1]
        if source:
            out = [jnp.where(low2, sa, sb), roll(jnp.where(low2, sb, sa), H, 0),
                   jnp.where(low2, roll(sa, 1 - H, 0), roll(sb, H - 1, 0))]
        else:
            out = [jnp.where(low2, fa, fb), roll(jnp.where(low2, fb, fa), H, 0),
                   jnp.where(low2, roll(sa, 2, 0), roll(sb, -2, 0)),
                   jnp.where(low2, roll(fa, 1, 0), roll(fb, -1, 0))]
        out = [v[None] for v in out]
        return out if dx == 1 else out[::-1]

    def cat(*parts):
        return jnp.concatenate(parts, axis=0)

    ups = ((0, 1), (1, -1))

    def plane(d, back=0):
        return X - 1 - back if d == 1 else back

    def planes(d, count, back=0):
        return slice(X - count - back, X - back) if d == 1 else slice(back, back + count)

    def send_z(group, src_ref, moves, slots):
        for o, same in distinct(moves, sizes).items():
            slots[o] = group.send(src_ref, o, z_rows(o, R)) if o == same else slots[same]

    def z_side(of, dy, dz, f):
        own, after, before = (of(dx, dy, dz) for dx in (0, 1, -1))
        if f == 0:
            return jnp.where(slot2 < X, own, roll(jnp.where(slot2 < X // 2, after, before), L // 2, 1))
        return jnp.where(slot2 < X, roll(own, L // 2, 1), jnp.where(slot2 < X + X // 2, after, before))

    def sides(own, low, high):
        return jnp.where(side2, low, own), jnp.where(side2, own, high)

    def z_pairs(of, f, own_z, own_w):
        z = [z_side(of, 0, dz, f) for dz in (-1, 1)]
        w = [jnp.where(low2, z_side(of, 1, dz, f), z_side(of, -1, dz, f)) for dz in (-1, 1)]
        return sides(own_z, *z), sides(own_w, *w)

    load_c.wait()
    load_s.wait()
    state = [cons[f] for f in range(4)] + [sig[...]]
    energy = cons[4]
    A, B = X // R, 2 * X // R
    for f in range(5):
        yas[0, f * A:(f + 1) * A] = pack_rows(state[f], R - 1, 1)
        yas[1, f * A:(f + 1) * A] = pack_rows(state[f], 0, 1)
    zas[0] = pack_lanes(state[0:4], 4)
    zas[1] = pack_lanes([state[4], energy], 4)
    pl.semaphore_wait(barrier, len(NEAR))
    ya = [first.send(yas.at[j], (0, d, 0)) for j, d in ups]
    xa = []
    for j, d in ups:
        xa.append(first.send(cons.at[0:4, plane(d)], (d, 0, 0)))
        first.send(sig.at[plane(d)], (d, 0, 0))
    za = [first.send(zas, (0, 0, d)) for j, d in ups]
    for o in NEAR:
        pl.semaphore_signal(ready, inc=1, device_id=device(o), device_id_type=MESH)

    for f in range(4):
        field = state[1 + f] if f < 3 else energy
        ybs[0, f * B:(f + 1) * B] = pack_rows(field, R - 2, 2)
        ybs[1, f * B:(f + 1) * B] = pack_rows(field, 0, 2)
    for j, start, beyond in ((0, H, H - 1), (1, 0, H)):
        yrs[j, 0:X // 2] = pack_rows(state[0], start, H)
        yrs[j, X // 2:X // 2 + A] = pack_rows(state[0], beyond, 1)
    xb, xe, xt = [], [], []
    for j, d in ups:
        xb.append(late.send(cons.at[0:5, plane(d, 1)], (d, 0, 0)))
        xe.append(late.send(cons.at[4, plane(d)], (d, 0, 0)))
        xt.append(late.send(cons.at[0, planes(d, D - 1, 2)], (d, 0, 0)))
    lane3 = lanes(energy.shape)
    row3 = rows(energy.shape)
    rho_zz = jnp.where(lane3 == DZ - 1, roll(state[0], -1, 2), roll(state[0], 1, 2))
    rho_own = pack_lanes([state[0], rho_zz], wide)
    zrs[...] = rho_own
    for n, o in enumerate(XY_MOVES):
        drs[n, 0], drs[n, 1] = pack_corner(state[0], None, o)

    pl.semaphore_wait(ready, len(NEAR))
    zr, dr = {}, {}
    send_z(side, zrs, Z_NEAR, zr)
    side_slots = dict(zr)
    for n, o in enumerate(XY_MOVES):
        dr[o] = late_rho.send(drs.at[n], o)
    zr_far = {}
    send_z(late_rho, zrs, Z_EDGE, zr_far)
    yr, yb = [], []
    for j, d in ups:
        yr.append(late.send(yrs.at[j], (0, d, 0)))
        yb.append(late.send(ybs.at[j], (0, d, 0)))
    side.arrived()
    send_z(late_rho, zrs, Z_VERTEX, zr_far)

    inv0 = 1.0 / state[0]
    fields = [inv0] + [state[k] * inv0 for k in (1, 2, 3)] + [state[4]]
    own = [[[roll(v, -s, axis) for s in (1, -1)] for axis in (1, 2)] for v in fields]
    region = ((lane2 + 2) % L) // (4 * X)

    first.arrived()

    def to_speed(t):
        r = 1.0 / t[0]
        return [r] + [m * r for m in t[1:4]] + [t[4]]

    xg = [to_speed([g0[xa[j] + f] for f in range(5)]) for j in range(2)]
    yg = [to_speed([g0[ya[j] + f * A:ya[j] + (f + 1) * A] for f in range(5)]) for j in range(2)]
    zmerged = [jnp.where(lane2 % 4 < 2, g0[za[1] + v], g0[za[0] + v]) for v in range(2)]
    zinv = 1.0 / jnp.where(region == 0, zmerged[0], 1.0)
    shifted = [roll(zinv, 4 * X * k, 1) for k in (1, 2, 3)]
    zspeed = zmerged[0] * jnp.where(region == 1, shifted[0], jnp.where(region == 2, shifted[1], shifted[2]))
    zspeed = jnp.where(region == 0, zinv, zspeed)

    def neighbours(f):
        v, ((yp, ym), (zp, zm)) = fields[f], own[f]
        after = cat(*[roll(yg[1][f], R - 1 - p, 1) for p in range(R)])
        before = cat(*[roll(yg[0][f], 1 - p, 1) for p in range(R)])
        t, k = (zspeed, f * X) if f < 4 else (zmerged[1], 0)
        high = cat(*[roll(t, L - 1 - 4 * (k + p), 1)[None] for p in range(X)])
        low = cat(*[roll(t, 1 - 4 * (k + p), 1)[None] for p in range(X)])
        return [(cat(v[1:X], xg[1][f][None]), cat(xg[0][f][None], v[0:X - 1])),
                (jnp.where(row3 == R - 1, after, yp), jnp.where(row3 == 0, before, ym)),
                (jnp.where(lane3 == L - 1, high, zp), jnp.where(lane3 == 0, low, zm))]

    def coefficients(inv_m, inv_n):
        ws = [[inv_m + inv_n[d][s] for s in range(2)] for d in range(3)]
        scale = ALPHA / (2.0 * inv_m + ALPHA * sum(w for pair in ws for w in pair))
        return [[w * scale for w in pair] for pair in ws], scale

    def update(source, ws, nbr):
        acc = source
        for d in range(3):
            for s in range(2):
                acc = acc + ws[d][s] * nbr[d][s]
        return acc

    near_w, near_scale = coefficients(inv0, neighbours(0))
    g = []
    for k in (1, 2, 3):
        n = neighbours(k)
        g.append([n[d][0] - n[d][1] for d in range(3)])
    div = g[0][0] + g[1][1] + g[2][2]
    source = (g[0][0] * g[0][0] + g[1][1] * g[1][1] + g[2][2] * g[2][2]
              + 2.0 * (g[0][1] * g[1][0] + g[0][2] * g[2][0] + g[1][2] * g[2][1]) + div * div)
    source = source * (0.5 * near_scale)
    sigma1 = update(source, near_w, neighbours(4))

    z_fold = jnp.where(lane3 == DZ - 1, near_w[2][0] * roll(sigma1, -1, 2),
                       jnp.where(lane3 == L - DZ, near_w[2][1] * roll(sigma1, 1, 2), 0.0))
    z_own = pack_lanes([sigma1, source + z_fold], wide)
    z2s[...] = z_own
    z2, d2 = {}, {}
    send_z(second, z2s, Z_VERTEX, z2)
    for n, o in enumerate(XY_MOVES):
        d2s[n, 0], d2s[n, 1] = pack_corner(sigma1, source, o)
        d2[o] = second.send(d2s.at[n], o)
    send_z(second, z2s, Z_EDGE, z2)
    y_fold = jnp.where(row3 == H - 1, near_w[1][0] * roll(sigma1, -1, 1),
                       jnp.where(row3 == H, near_w[1][1] * roll(sigma1, 1, 1), 0.0))
    for j, start in ((0, H), (1, 0)):
        y2s[j, 0:X // 2] = pack_rows(sigma1, start, H)
        y2s[j, X // 2:X] = pack_rows(source + y_fold, start, H)
    y2 = [second.send(y2s.at[j], (0, d, 0)) for j, d in ups]
    for j, d in ups:
        x2s[j, 0:D] = sigma1[planes(d, D)]
        x2s[j, D:2 * D] = source[planes(d, D)]
    x2s[0, D] = source[X - D] + near_w[0][1][X - D] * sigma1[X - D - 1]
    x2s[1, 2 * D - 1] = source[D - 1] + near_w[0][0][D - 1] * sigma1[D]
    x2 = [second.send(x2s.at[j], (d, 0, 0)) for j, d in ups]
    send_z(second, z2s, Z_NEAR, z2)

    late.arrived()
    core = state[0:4] + [energy]
    rho_y = unpack_rows(g1[yr[1]:yr[1] + X // 2], g1[yr[0]:yr[0] + X // 2], H)
    rho_yy = unpack_rows(g1[yr[1] + X // 2:yr[1] + X // 2 + A], g1[yr[0] + X // 2:yr[0] + X // 2 + A], 1, 1)
    xn = [[g0[xa[j] + f][None] for f in range(4)] + [g1[xe[j]][None]] for j in range(2)]
    xc = [cat(g1[xb[0] + f][None], xn[0][f], core[f], xn[1][f], g1[xb[1] + f][None]) for f in range(5)]
    yc = [rho_y] + [unpack_rows(g1[yb[1] + f * B:yb[1] + (f + 1) * B], g1[yb[0] + f * B:yb[0] + (f + 1) * B], 2)
                    for f in range(4)]
    zc = [cat(*[roll(zmerged[f // 4], -4 * (f * X + p), 1)[None] for p in range(X)]) for f in range(4)]
    zc.append(cat(*[roll(zmerged[1], -4 * (X + p), 1)[None] for p in range(X)]))

    def x_stencil(c):
        return c[0:X + 1], c[1:X + 2], c[2:X + 3], c[3:X + 4]

    def ring_stencil(c, gh, axis):
        m, p = ring(c, gh, -1, axis), ring(c, gh, 1, axis)
        return cat(*m), cat(c, gh), cat(*p), cat(*ring(p[0], p[1], 1, axis))

    def faces(st):
        m, q, p, pp = st
        sixth = 1.0 / 6.0
        return (5.0 * q + 2.0 * p - m) * sixth, (2.0 * q + 5.0 * p - pp) * sixth

    def plain_flux(s, d):
        r = 1.0 / s[0]
        v = s[1 + d] * r
        pressure = (GAMMA - 1.0) * (s[4] - 0.5 * (s[1] * s[1] + s[2] * s[2] + s[3] * s[3]) * r)
        out = [s[1 + d]]
        for k in range(3):
            out.append(s[1 + k] * v + pressure if k == d else s[1 + k] * v)
        out.append((s[4] + pressure) * v)
        return out, v

    def difference(flux, d):
        if d == 0:
            return flux[1:X + 1] - flux[0:X]
        return flux[0:X] - ring(flux[0:X], flux[X:2 * X], -1, d)[0]

    base = [None] * 5
    speed = []
    for d in range(3):
        if d == 0:
            lr = [faces(x_stencil(c)) for c in xc]
        else:
            lr = [faces(ring_stencil(c, gh, d)) for c, gh in zip(core, (None, yc, zc)[d])]
        lf, lv = plain_flux([v[0] for v in lr], d)
        rf, rv = plain_flux([v[1] for v in lr], d)
        speed.append((lv, rv))
        for k in range(5):
            flux = 0.5 * (lf[k] + rf[k]) - (0.5 * LAMBDA) * (lr[k][1] - lr[k][0])
            change = difference(flux, d)
            base[k] = change if base[k] is None else base[k] + change
    base = [core[k] - STEP_DT * base[k] for k in range(5)]
    adv_ref[0] = base[0]

    def lower(v, d):
        return v[0:X] if d == 0 else ring(v[0:X], v[X:2 * X], -1, d)[0]

    part = []
    for d, (lv, rv) in enumerate(speed):
        ll, rl = lower(lv, d), lower(rv, d)
        lv, rv = (lv[1:X + 1], rv[1:X + 1]) if d == 0 else (lv[0:X], rv[0:X])
        k = -0.5 * STEP_DT / 6.0
        part.append([k * ll, k * (-lv - 5.0 * ll - 2.0 * rl), k * (5.0 * lv + 2.0 * rv - 2.0 * ll - 5.0 * rl),
                     k * (2.0 * lv + 5.0 * rv + rl), -k * rv])
    middle = part[0][2] + part[1][2] + part[2][2]

    def pick(part, ps, step=0):
        value, reach = part
        return cat(*[value[reach + a + step:reach + b + step] for a, b in ps])

    def z_shift(value, ps, pair, step, by=1):
        at = [p for a, b in ps for p in range(a, b)]
        lane = lanes(value.shape)
        if step == 1:
            ghost, edge = [roll(pair[1], L - by - wide * p, 1) for p in at], lane >= L - by
        else:
            ghost, edge = [roll(pair[0], by - wide * p, 1) for p in at], lane < by
        return jnp.where(edge, cat(*[v[None] for v in ghost]), roll(value, -step * by, 2))

    def around_planes(c, y, pair, ps):
        m = pick(c, ps)
        cy = [ring(m, pick(y, ps), s, 1) for s in (1, -1)]
        z = [z_shift(m, ps, pair, s) for s in (1, -1)]
        return [(pick(c, ps, 1), pick(c, ps, -1)), [t[0] for t in cy], z], [t[1] for t in cy]

    def around_ghosts(y, yy, pair, e):
        ps = [(-e, X + e)]
        return [(pick(y, ps, 1), pick(y, ps, -1)), yy, [z_shift(pick(y, ps), ps, pair, s) for s in (1, -1)]]

    def around_packed(z, w):
        out = [], []
        for zt, wt in zip(z, w):
            zy = [ring(zt, wt, s, 0) for s in (1, -1)]
            for to, t, k in ((out[0], zt, 0), (out[1], wt, 1)):
                to.append([(roll(t, -wide, 1), roll(t, wide, 1)), [v[k] for v in zy], (roll(t, -1, 1), roll(t, 1, 1))])
        return out

    late_rho.arrived()
    rho_of = lambda dx, dy, dz: g2[side_slots[(0, 0, -dz)]] if dx == dy == 0 else g3[zr_far[(-dx, -dy, -dz)]]
    every = range(-D, X + D)
    outer = [p for p in every if not 0 <= p < X]
    rho_c = cat(g1[xt[0]:xt[0] + D - 1], xc[0], g1[xt[1]:xt[1] + D - 1])
    rho_ye = cat(*unpack_corner(g3, dr, -1, False), rho_y, *unpack_corner(g3, dr, 1, False))
    rho_z, rho_w = z_pairs(rho_of, 0, pack_planes(rho_own, pick((rho_c, D + 1), [(-D, 0), (X, X + D)]), outer),
                           pack_planes(rho_own, rho_ye, every))
    inv_c, inv_y = (1.0 / rho_c, D + 1), (1.0 / rho_ye, D)
    inv_z, inv_w = [1.0 / t for t in rho_z], [1.0 / t for t in rho_w]
    beyond = [1.0 / z_side(rho_of, 0, dz, 1) for dz in (-1, 1)]
    far_coef = coefficients(pick(inv_c, [(-D, 0), (X, X + D)]),
                            around_planes(inv_c, inv_y, inv_z, [(-D, 0), (X, X + D)])[0])[0]
    coef_c = [[cat(far[0:D], mine, far[D:2 * D]) for far, mine in zip(*pair)] for pair in zip(far_coef, near_w)]
    e = D - 1
    rim = jnp.zeros((e, R, L), jnp.float32)
    yy = around_planes(inv_c, inv_y, inv_z, [(-e, X + e)])[1]
    inv_yy = cat(rim, 1.0 / rho_yy, rim)
    row = rows(inv_yy.shape)
    yy = [jnp.where(row == at, inv_yy, t) for t, at in zip(yy, (H - 1, H))]
    coef_y = coefficients(pick(inv_y, [(-e, X + e)]), around_ghosts(inv_y, yy, inv_w, e))[0]
    coef_y[1] = [jnp.where(row == at, 0.0, t) for t, at in zip(coef_y[1], (H - 1, H))]
    zn, wn = around_packed(inv_z, inv_w)
    coef_z, coef_w = [], []
    for j, at in ((0, DZ), (1, DZ - 1)):
        last = lane2 % wide == at
        pair = list(zn[j][2])
        pair[1 - j] = jnp.where(last, beyond[j], pair[1 - j])
        ws = coefficients(inv_z[j], [*zn[j][0:2], pair])[0]
        ws[2][1 - j] = jnp.where(last, 0.0, ws[2][1 - j])
        coef_z.append(ws)
        coef_w.append(coefficients(inv_w[j], wn[j])[0])

    second.arrived()
    zero = jnp.zeros((1, R, L), jnp.float32)
    sig_of = lambda dx, dy, dz: g4[z2[(-dx, -dy, -dz)]]
    sx, qx = [cat(g4[x2[0] + t:x2[0] + t + D], g4[x2[1] + t:x2[1] + t + D]) for t in (0, D)]
    sy, qy = [unpack_rows(g4[y2[1] + t:y2[1] + t + X // 2], g4[y2[0] + t:y2[0] + t + X // 2], H) for t in (0, X // 2)]
    sy = cat(*unpack_corner(g4, d2, -1, False), sy, *unpack_corner(g4, d2, 1, False))
    qy = cat(*unpack_corner(g4, d2, -1, True), qy, *unpack_corner(g4, d2, 1, True))
    z, w = z_pairs(sig_of, 0, pack_planes(z_own, sx, outer), pack_planes(z_own, sy, every))
    q_own = roll(z_own, L // 2, 1)
    qz, qw = z_pairs(sig_of, 1, pack_planes(q_own, qx, outer), pack_planes(q_own, qy, range(-e, X + e)))
    ghosts = [(z, w)]
    for sweep in range(1, SWEEPS):
        zn, wn = around_packed(z, w)
        z = [update(qz[j], coef_z[j], zn[j]) for j in range(2)]
        if sweep < SWEEPS - 1:
            w = [update(qw[j], coef_w[j], wn[j]) for j in range(2)]
        ghosts.append((z, w))

    def lane_ghost(sweep, which, p):
        return sweep, which, p

    def one_shift(tile, ghost, step, by=1):
        sweep, which, p = ghost
        pair = ghosts[sweep][which]
        if step == 1:
            return jnp.where(lane2 >= L - by, roll(pair[1], L - by - wide * p, 1), roll(tile, -by, 1))
        return jnp.where(lane2 < by, roll(pair[0], by - wide * p, 1), roll(tile, by, 1))

    tiles = lambda value, lo: {lo + k: value[k] for k in range(value.shape[0])}
    c = {**tiles(sigma1, 0), **tiles(sx[0:D], -D), **tiles(sx[D:2 * D], X), -D - 1: zero[0], X + D: zero[0]}
    qc = {**tiles(source, 0), **tiles(qx[0:D], -D), **tiles(qx[D:2 * D], X)}
    y, qy = tiles(sy, -D), tiles(qy, -e)
    cs, ys = [c] + [{} for _ in range(1, SWEEPS)], [y] + [{} for _ in range(1, SWEEPS)]

    def sweep_plane(sweep, p):
        c, y = cs[sweep - 1], ys[sweep - 1]
        ec, ey = D + 1 - sweep, 0 if sweep == SWEEPS - 1 else D - sweep
        if not -ec <= p < X + ec:
            return
        cy = [ring(c[p], y[p], s, 0) for s in (1, -1)]
        ghost = lane_ghost(sweep - 1, 0, p)
        nbr = [(c[p + 1], c[p - 1]), [t[0] for t in cy], [one_shift(c[p], ghost, s) for s in (1, -1)]]
        cs[sweep][p] = update(qc[p], [[v[D + p] for v in pair] for pair in coef_c], nbr)
        if -ey <= p < X + ey:
            ghost = lane_ghost(sweep - 1, 1, p)
            nbr = [(y[p + 1], y[p - 1]), [t[1] for t in cy], [one_shift(y[p], ghost, s) for s in (1, -1)]]
            ys[sweep][p] = update(qy[p], [[v[e + p] for v in pair] for pair in coef_y], nbr)

    def flux_plane(p):
        if not 0 <= p < X:
            return
        c, y, ghost = cs[SWEEPS - 1], ys[SWEEPS - 1], lane_ghost(SWEEPS - 1, 0, p)
        out_sig_ref[p] = c[p]

        def y_shift(step, by):
            edge = row2 >= R - by if step == 1 else row2 < by
            return jnp.where(edge, roll(y[p], -step * by, 0), roll(c[p], -step * by, 0))

        total = base[4][p] + middle[p] * c[p]
        shifts = [lambda s, by: c[p + s * by], y_shift, lambda s, by: one_shift(c[p], ghost, s, by)]
        for d in range(3):
            (p1, p2), (m1, m2) = [[shifts[d](s, by) for by in (1, 2)] for s in (1, -1)]
            adv_ref[1 + d, p] = base[1 + d][p] + ((-4.0 * STEP_DT / 6.0) * (p1 - m1) + (0.5 * STEP_DT / 6.0) * (p2 - m2))
            a = [v[p] for v in part[d]]
            total = total + (a[0] * m2 + a[1] * m1 + a[3] * p1 + a[4] * p2)
        adv_ref[4, p] = total

    for step in range(-D, X + D + 2 * SWEEPS):
        for sweep in range(1, SWEEPS):
            sweep_plane(sweep, step - 2 * (sweep - 1))
        flux_plane(step - 2 * (SWEEPS - 1) - 1)
    assert sum(group.rows for group in groups) == sent.shape[0]
    second.copy(sent, sent, NEAR[0]).wait_send()


def write(adv, sig, adv_hbm, sig_hbm, sem):
    copies = [pltpu.make_async_copy(src, dst, sem.at[n])
              for n, (src, dst) in enumerate(((adv, adv_hbm), (sig, sig_hbm)))]
    for copy in copies:
        copy.start()
    for copy in copies:
        copy.wait()


def solution(mesh):
    sizes = tuple(mesh.shape[a] for a in AXES)

    def on_device(conserved, sigma_guess):
        X, R, L = sigma_guess.shape
        A, B, H, D = X // R, 2 * X // R, X // 2, DEPTH
        f32 = jnp.float32
        vm = lambda *shape: pltpu.VMEM((*shape, R, L), f32)
        nd = len(XY_MOVES)
        tiles = landing(X, R, sizes)
        rows = [R * n + sum(part) for n, part in tiles]
        spare = [pltpu.VMEM((n, 1, L), f32) for n in (rows[3], rows[4], sum(rows))]
        outs = pl.pallas_call(
            functools.partial(kernel, sizes),
            out_shape=(pltpu.VMEM(conserved.shape, f32), pltpu.VMEM(sigma_guess.shape, f32)),
            in_specs=[pl.BlockSpec(memory_space=pl.ANY)] * 2,
            out_specs=(pl.BlockSpec(memory_space=pltpu.VMEM),) * 2,
            scratch_shapes=[
                vm(5, X), vm(X), *[vm(n + len(part)) for n, part in tiles], *spare,
                vm(2, 5 * A), vm(2), vm(2, 4 * B), vm(2, H + A), vm(), vm(nd, 2),
                vm(2, 2 * D), vm(2, 2 * H), vm(), vm(nd, 2),
                pltpu.SemaphoreType.DMA((2,)),
                pltpu.SemaphoreType.REGULAR,
                pltpu.SemaphoreType.DMA,
                pltpu.SemaphoreType.DMA((len(tiles),)),
            ],
            compiler_params=pltpu.CompilerParams(collective_id=0, has_side_effects=True),
        )(conserved, sigma_guess)
        return pl.pallas_call(
            write,
            out_shape=tuple(jax.ShapeDtypeStruct(a.shape, f32) for a in (conserved, sigma_guess)),
            in_specs=[pl.BlockSpec(memory_space=pltpu.VMEM)] * 2,
            out_specs=(pl.BlockSpec(memory_space=pl.ANY),) * 2,
            scratch_shapes=[pltpu.SemaphoreType.DMA((2,))],
        )(*(pltpu.with_memory_space_constraint(v, pltpu.VMEM) for v in outs))

    specs = (P(None, "gx", "gy", "gz"), P("gx", "gy", "gz"))
    return jax.shard_map(on_device, mesh=mesh, in_specs=specs, out_specs=specs, check_vma=False)
```

```python
import functools
import itertools

import jax
import jax.numpy as jnp
from jax import lax
from jax.experimental import pallas as pl
from jax.experimental.pallas import tpu as pltpu
from jax.sharding import PartitionSpec as P

SWEEPS = 4
ALPHA = 10.0
GAMMA = 1.4
LAMBDA = 3.0
STEP_DT = 0.4
DEPTH = SWEEPS
MESH = pl.DeviceIdType.MESH
AXES = ("gx", "gy", "gz")

OFFSETS = [o for o in itertools.product((-1, 0, 1), repeat=3) if any(o)]
NEAR = [(0, 1, 0), (0, -1, 0), (1, 0, 0), (-1, 0, 0), (0, 0, 1), (0, 0, -1)]
XY_MOVES = [o for o in OFFSETS if o[0] != 0 and o[1] != 0 and o[2] == 0]
Z_NEAR = [(0, 0, 1), (0, 0, -1)]
Z_VERTEX = [o for o in OFFSETS if all(o)]
Z_EDGE = [o for o in OFFSETS if o[2] != 0 and o not in Z_NEAR and o not in Z_VERTEX]


def iota(shape, dim):
    return lax.broadcasted_iota(jnp.int32, shape, dim)


def roll(value, shift, axis):
    size = value.shape[axis]
    shift = shift % size
    return value if shift == 0 else pltpu.roll(value, shift, axis)


def ring(core, ghost, step, axis):
    size = core.shape[axis]
    a, b = roll(core, -step, axis), roll(ghost, -step, axis)
    edge = iota(core.shape, axis) == (size - 1 if step == 1 else 0)
    return jnp.where(edge, b, a), jnp.where(edge, a, b)


def distinct(moves, sizes):
    first = {}
    return {o: first.setdefault(tuple(v % s for v, s in zip(o, sizes)), o) for o in moves}


def z_rows(offset, R):
    n = R if offset[1] == 0 else DEPTH - 1 if offset[0] else DEPTH
    return slice(0, n) if offset[1] == -1 else slice(R - n, R)


def landing(X, R, sizes):
    sent = lambda moves: sorted(set(distinct(moves, sizes).values()))
    rows = [z_rows(o, R).stop - z_rows(o, R).start for o in sent(Z_EDGE) + sent(Z_VERTEX)]
    part = [n for n in rows if n < R]
    full = len(rows) - len(part)
    A, B, H = X // R, 2 * X // R, X // 2
    near, corner = len(sent(Z_NEAR)), 2 * len(XY_MOVES)
    return [
        (2 * (5 * A + 5 + 2), []),
        (2 * (H + 3 * A + B + 5 + 1 + DEPTH - 1), []),
        (near, []),
        (len(XY_MOVES) + full, part + [2] * len(XY_MOVES)),
        (corner + near + full + 2 * 2 * H + 2 * 2 * DEPTH, part),
    ]


def kernel(sizes, cons_hbm, sig_hbm, adv_ref, out_sig_ref, cons, sig, g0, g1, g2, g3, g4, t3, t4, sent,
           yas, zas, ybs, yrs, zrs, drs, x2s, y2s, z2s, d2s, in_sem, ready, send_sem, recv_sem):
    X, R, L = sig.shape
    H, D, DZ = R // 2, DEPTH, L // (4 * X)
    wide = 2 * DZ
    me = [lax.axis_index(a) for a in AXES]

    def device(offset):
        return {a: lax.rem(me[i] + offset[i] + sizes[i], sizes[i]) for i, a in enumerate(AXES)}

    load_c = pltpu.make_async_copy(cons_hbm, cons, in_sem.at[0])
    load_s = pltpu.make_async_copy(sig_hbm, sig, in_sem.at[1])
    load_c.start()
    load_s.start()
    barrier = pltpu.get_barrier_semaphore()
    for o in NEAR:
        pl.semaphore_signal(barrier, inc=1, device_id=device(o), device_id_type=MESH)

    class Group:
        def __init__(self, n, buf, spare):
            self.n, self.buf, self.spare, self.used, self.rows = n, buf, spare, 0, 0

        def copy(self, src, dst, offset):
            return pltpu.make_async_remote_copy(
                src_ref=src, dst_ref=dst, send_sem=send_sem, recv_sem=recv_sem.at[self.n],
                device_id=device(offset), device_id_type=MESH)

        def send(self, src, offset, part=None):
            at = self.used
            if part is not None:
                self.used += 1
                self.rows += part.stop - part.start
                self.copy(src.at[part], self.buf.at[at, part], offset).start()
            elif len(src.shape) == 2:
                self.used, self.rows = at + 1, self.rows + R
                self.copy(src, self.buf.at[at], offset).start()
            else:
                self.used, self.rows = at + src.shape[0], self.rows + R * src.shape[0]
                self.copy(src, self.buf.at[at:self.used], offset).start()
            return at

        def arrived(self):
            assert self.used == self.buf.shape[0] and self.rows == self.spare.shape[0] * self.spare.shape[1]
            self.copy(self.spare, self.spare, NEAR[0]).wait_recv()

    groups = [Group(n, buf, size) for n, (buf, size) in enumerate(zip((g0, g1, g2, g3, g4), (g0, g1, g2, t3, t4)))]
    first, late, side, late_rho, second = groups

    rows = lambda shape: iota(shape, len(shape) - 2)
    lanes = lambda shape: iota(shape, len(shape) - 1)

    def pack_rows(field, first, n):
        size = X * n // R
        out = field[0:size]
        r = rows(out.shape)
        for g in range(1, R // n):
            part = roll(field[g * size:(g + 1) * size], n * g, 1)
            out = jnp.where((r + (2 * R - first - n * g)) % R < n, part, out)
        return out

    def unpack_rows(after, before, n):
        low = rows(after.shape) < H
        return jnp.concatenate(
            [jnp.where(low, roll(after, -n * g, 1), roll(before, -n * g, 1)) for g in range(R // n)],
            axis=0)

    lane2, row2 = lanes((R, L)), rows((R, L))
    low2 = row2 < H

    def pack_lanes(fields, width):
        out = jnp.zeros((R, L), jnp.float32)
        for k, tile in enumerate(f[p] for f in fields for p in range(X)):
            out = jnp.where(((lane2 + width // 2) % L) // width == k, roll(tile, width * k, 1), out)
        return out

    slot2 = ((lane2 + DZ) % L) // wide
    side2 = lane2 % wide >= DZ

    def pack_planes(out, value, ps):
        for k, p in enumerate(ps):
            out = jnp.where(slot2 == p % (2 * X), roll(value[k], wide * p, 1), out)
        return out

    def pack_corner(f, s, o):
        a1, a2, a3, a4 = (f[X - a if o[0] == 1 else a - 1] for a in range(1, 5))
        if o[1] == 1:
            one = jnp.where(row2 >= H, a1, jnp.where(row2 >= 1, roll(a2, -H, 0), roll(a4, 1, 0)))
            two = roll(a3, 2, 0)
        else:
            one = jnp.where(row2 < H, a1, jnp.where(row2 < R - 1, roll(a2, H, 0), roll(a4, -1, 0)))
            two = roll(a3, -2, 0)
        if s is not None:
            s1, s2, s3 = (s[X - a if o[0] == 1 else a - 1] for a in range(1, 4))
            if o[1] == 1:
                two = jnp.where(row2 > H, s1, jnp.where(row2 == H, roll(s3, 1 - H, 0),
                                                        jnp.where(row2 >= 2, roll(s2, -H, 0), two)))
            else:
                two = jnp.where(row2 < H - 1, s1, jnp.where(row2 == H - 1, roll(s3, H - 1, 0),
                                                            jnp.where(row2 < R - 2, roll(s2, H, 0), two)))
        return one, two

    def unpack_corner(buf, slots, dx, source):
        after, before = slots[(-dx, -1, 0)], slots[(-dx, 1, 0)]
        fa, fb, sa, sb = buf[after], buf[before], buf[after + 1], buf[before + 1]
        if source:
            out = [jnp.where(low2, sa, sb), roll(jnp.where(low2, sb, sa), H, 0),
                   jnp.where(low2, roll(sa, 1 - H, 0), roll(sb, H - 1, 0))]
        else:
            out = [jnp.where(low2, fa, fb), roll(jnp.where(low2, fb, fa), H, 0),
                   jnp.where(low2, roll(sa, 2, 0), roll(sb, -2, 0)),
                   jnp.where(low2, roll(fa, 1, 0), roll(fb, -1, 0))]
        out = [v[None] for v in out]
        return out if dx == 1 else out[::-1]

    def cat(*parts):
        return jnp.concatenate(parts, axis=0)

    ups = ((0, 1), (1, -1))

    def plane(d, back=0):
        return X - 1 - back if d == 1 else back

    def planes(d, count, back=0):
        return slice(X - count - back, X - back) if d == 1 else slice(back, back + count)

    def send_z(group, src_ref, moves, slots):
        for o, same in distinct(moves, sizes).items():
            slots[o] = group.send(src_ref, o, z_rows(o, R)) if o == same else slots[same]

    def z_side(of, dy, dz, f):
        own, after, before = (of(dx, dy, dz) for dx in (0, 1, -1))
        if f == 0:
            return jnp.where(slot2 < X, own, roll(jnp.where(slot2 < X // 2, after, before), L // 2, 1))
        return jnp.where(slot2 < X, roll(own, L // 2, 1), jnp.where(slot2 < X + X // 2, after, before))

    def sides(own, low, high):
        return jnp.where(side2, low, own), jnp.where(side2, own, high)

    def z_pairs(of, f, own_z, own_w):
        z = [z_side(of, 0, dz, f) for dz in (-1, 1)]
        w = [jnp.where(low2, z_side(of, 1, dz, f), z_side(of, -1, dz, f)) for dz in (-1, 1)]
        return sides(own_z, *z), sides(own_w, *w)

    load_c.wait()
    load_s.wait()
    state = [cons[f] for f in range(4)] + [sig[...]]
    energy = cons[4]
    A, B = X // R, 2 * X // R
    for f in range(5):
        yas[0, f * A:(f + 1) * A] = pack_rows(state[f], R - 1, 1)
        yas[1, f * A:(f + 1) * A] = pack_rows(state[f], 0, 1)
    zas[0] = pack_lanes(state[0:4], 4)
    zas[1] = pack_lanes([state[4], energy], 4)
    pl.semaphore_wait(barrier, len(NEAR))
    ya = [first.send(yas.at[j], (0, d, 0)) for j, d in ups]
    xa = []
    for j, d in ups:
        xa.append(first.send(cons.at[0:4, plane(d)], (d, 0, 0)))
        first.send(sig.at[plane(d)], (d, 0, 0))
    za = [first.send(zas, (0, 0, d)) for j, d in ups]
    for o in NEAR:
        pl.semaphore_signal(ready, inc=1, device_id=device(o), device_id_type=MESH)

    for j, second_row, start in ((0, R - 2, R - 1 - H), (1, 1, 1)):
        for f in range(3):
            ybs[j, f * A:(f + 1) * A] = pack_rows(state[1 + f], second_row, 1)
        ybs[j, 3 * A:3 * A + B] = pack_rows(energy, (R - 2, 0)[j], 2)
        yrs[j] = pack_rows(state[0], start, H)
    xb, xe, xt = [], [], []
    for j, d in ups:
        xb.append(late.send(cons.at[0:5, plane(d, 1)], (d, 0, 0)))
        xe.append(late.send(cons.at[4, plane(d)], (d, 0, 0)))
        xt.append(late.send(cons.at[0, planes(d, D - 1, 2)], (d, 0, 0)))
    lane3 = lanes(energy.shape)
    row3 = rows(energy.shape)
    rho_zz = jnp.where(lane3 == DZ - 1, roll(state[0], -1, 2), roll(state[0], 1, 2))
    rho_own = pack_lanes([state[0], rho_zz], wide)
    zrs[...] = rho_own
    for n, o in enumerate(XY_MOVES):
        drs[n, 0], drs[n, 1] = pack_corner(state[0], None, o)

    pl.semaphore_wait(ready, len(NEAR))
    zr, dr = {}, {}
    send_z(side, zrs, Z_NEAR, zr)
    side_slots = dict(zr)
    for n, o in enumerate(XY_MOVES):
        dr[o] = late_rho.send(drs.at[n, 0], o)
        late_rho.send(drs.at[n, 1], o, slice(0, 2) if o[1] == 1 else slice(R - 2, R))
    zr_far = {}
    send_z(late_rho, zrs, Z_EDGE, zr_far)
    yr, yb = [], []
    for j, d in ups:
        yr.append(late.send(yrs.at[j], (0, d, 0)))
        yb.append(late.send(ybs.at[j], (0, d, 0)))
    side.arrived()
    send_z(late_rho, zrs, Z_VERTEX, zr_far)

    inv0 = 1.0 / state[0]
    fields = [inv0] + [state[k] * inv0 for k in (1, 2, 3)] + [state[4]]
    own = [[[roll(v, -s, axis) for s in (1, -1)] for axis in (1, 2)] for v in fields]
    region = ((lane2 + 2) % L) // (4 * X)

    first.arrived()

    def to_speed(t):
        r = 1.0 / t[0]
        return [r] + [m * r for m in t[1:4]] + [t[4]]

    xg = [to_speed([g0[xa[j] + f] for f in range(5)]) for j in range(2)]
    yg = [to_speed([g0[ya[j] + f * A:ya[j] + (f + 1) * A] for f in range(5)]) for j in range(2)]
    zmerged = [jnp.where(lane2 % 4 < 2, g0[za[1] + v], g0[za[0] + v]) for v in range(2)]
    zinv = 1.0 / jnp.where(region == 0, zmerged[0], 1.0)
    shifted = [roll(zinv, 4 * X * k, 1) for k in (1, 2, 3)]
    zspeed = zmerged[0] * jnp.where(region == 1, shifted[0], jnp.where(region == 2, shifted[1], shifted[2]))
    zspeed = jnp.where(region == 0, zinv, zspeed)

    def neighbours(f):
        v, ((yp, ym), (zp, zm)) = fields[f], own[f]
        after = cat(*[roll(yg[1][f], R - 1 - p, 1) for p in range(R)])
        before = cat(*[roll(yg[0][f], 1 - p, 1) for p in range(R)])
        t, k = (zspeed, f * X) if f < 4 else (zmerged[1], 0)
        high = cat(*[roll(t, L - 1 - 4 * (k + p), 1)[None] for p in range(X)])
        low = cat(*[roll(t, 1 - 4 * (k + p), 1)[None] for p in range(X)])
        return [(cat(v[1:X], xg[1][f][None]), cat(xg[0][f][None], v[0:X - 1])),
                (jnp.where(row3 == R - 1, after, yp), jnp.where(row3 == 0, before, ym)),
                (jnp.where(lane3 == L - 1, high, zp), jnp.where(lane3 == 0, low, zm))]

    def coefficients(inv_m, inv_n):
        ws = [[inv_m + inv_n[d][s] for s in range(2)] for d in range(3)]
        scale = ALPHA / (2.0 * inv_m + ALPHA * sum(w for pair in ws for w in pair))
        return [[w * scale for w in pair] for pair in ws], scale

    def update(source, ws, nbr):
        acc = source
        for d in range(3):
            for s in range(2):
                acc = acc + ws[d][s] * nbr[d][s]
        return acc

    near_w, near_scale = coefficients(inv0, neighbours(0))
    g = []
    for k in (1, 2, 3):
        n = neighbours(k)
        g.append([n[d][0] - n[d][1] for d in range(3)])
    div = g[0][0] + g[1][1] + g[2][2]
    source = (g[0][0] * g[0][0] + g[1][1] * g[1][1] + g[2][2] * g[2][2]
              + 2.0 * (g[0][1] * g[1][0] + g[0][2] * g[2][0] + g[1][2] * g[2][1]) + div * div)
    source = source * (0.5 * near_scale)
    sigma1 = update(source, near_w, neighbours(4))

    z_fold = jnp.where(lane3 == DZ - 1, near_w[2][0] * roll(sigma1, -1, 2),
                       jnp.where(lane3 == L - DZ, near_w[2][1] * roll(sigma1, 1, 2), 0.0))
    z_own = pack_lanes([sigma1, source + z_fold], wide)
    z2s[...] = z_own
    z2, d2 = {}, {}
    send_z(second, z2s, Z_VERTEX, z2)
    for n, o in enumerate(XY_MOVES):
        d2s[n, 0], d2s[n, 1] = pack_corner(sigma1, source, o)
        d2[o] = second.send(d2s.at[n], o)
    send_z(second, z2s, Z_EDGE, z2)
    y_fold = jnp.where(row3 == H - 1, near_w[1][0] * roll(sigma1, -1, 1),
                       jnp.where(row3 == H, near_w[1][1] * roll(sigma1, 1, 1), 0.0))
    for j, start in ((0, H), (1, 0)):
        y2s[j, 0:X // 2] = pack_rows(sigma1, start, H)
        y2s[j, X // 2:X] = pack_rows(source + y_fold, start, H)
    y2 = [second.send(y2s.at[j], (0, d, 0)) for j, d in ups]
    for j, d in ups:
        x2s[j, 0:D] = sigma1[planes(d, D)]
        x2s[j, D:2 * D] = source[planes(d, D)]
    x2s[0, D] = source[X - D] + near_w[0][1][X - D] * sigma1[X - D - 1]
    x2s[1, 2 * D - 1] = source[D - 1] + near_w[0][0][D - 1] * sigma1[D]
    x2 = [second.send(x2s.at[j], (d, 0, 0)) for j, d in ups]
    send_z(second, z2s, Z_NEAR, z2)

    late.arrived()
    core = state[0:4] + [energy]
    near_row = (row3 == 0) | (row3 == R - 1)

    def first_rows(f):
        return unpack_rows(g0[ya[1] + f * A:ya[1] + (f + 1) * A], g0[ya[0] + f * A:ya[0] + (f + 1) * A], 1)

    def late_rows(at, to, n):
        return unpack_rows(g1[yb[1] + at:yb[1] + to], g1[yb[0] + at:yb[0] + to], n)

    rho_before, rho_after = [cat(*[roll(g1[yr[j]:yr[j] + X // 2], -H * k, 1) for k in range(R // H)]) for j in range(2)]
    rho_y = jnp.where(near_row, first_rows(0), jnp.where(row3 < H, rho_after, rho_before))
    rho_yy = jnp.where(row3 < H, roll(rho_after, -1, 1), roll(rho_before, 1, 1))
    xn = [[g0[xa[j] + f][None] for f in range(4)] + [g1[xe[j]][None]] for j in range(2)]
    xc = [cat(g1[xb[0] + f][None], xn[0][f], core[f], xn[1][f], g1[xb[1] + f][None]) for f in range(5)]
    yc = [rho_y] + [jnp.where(near_row, first_rows(1 + f), late_rows(f * A, (f + 1) * A, 1)) for f in range(3)]
    yc.append(late_rows(3 * A, 3 * A + B, 2))
    zc = [cat(*[roll(zmerged[f // 4], -4 * (f * X + p), 1)[None] for p in range(X)]) for f in range(4)]
    zc.append(cat(*[roll(zmerged[1], -4 * (X + p), 1)[None] for p in range(X)]))

    def x_stencil(c):
        return c[0:X + 1], c[1:X + 2], c[2:X + 3], c[3:X + 4]

    def ring_stencil(c, gh, axis):
        m, p = ring(c, gh, -1, axis), ring(c, gh, 1, axis)
        return cat(*m), cat(c, gh), cat(*p), cat(*ring(p[0], p[1], 1, axis))

    def faces(st):
        m, q, p, pp = st
        sixth = 1.0 / 6.0
        return (5.0 * q + 2.0 * p - m) * sixth, (2.0 * q + 5.0 * p - pp) * sixth

    def plain_flux(s, d):
        r = 1.0 / s[0]
        v = s[1 + d] * r
        pressure = (GAMMA - 1.0) * (s[4] - 0.5 * (s[1] * s[1] + s[2] * s[2] + s[3] * s[3]) * r)
        out = [s[1 + d]]
        for k in range(3):
            out.append(s[1 + k] * v + pressure if k == d else s[1 + k] * v)
        out.append((s[4] + pressure) * v)
        return out, v

    def difference(flux, d):
        if d == 0:
            return flux[1:X + 1] - flux[0:X]
        return flux[0:X] - ring(flux[0:X], flux[X:2 * X], -1, d)[0]

    base = [None] * 5
    speed = []
    for d in range(3):
        if d == 0:
            lr = [faces(x_stencil(c)) for c in xc]
        else:
            lr = [faces(ring_stencil(c, gh, d)) for c, gh in zip(core, (None, yc, zc)[d])]
        lf, lv = plain_flux([v[0] for v in lr], d)
        rf, rv = plain_flux([v[1] for v in lr], d)
        speed.append((lv, rv))
        for k in range(5):
            flux = 0.5 * (lf[k] + rf[k]) - (0.5 * LAMBDA) * (lr[k][1] - lr[k][0])
            change = difference(flux, d)
            base[k] = change if base[k] is None else base[k] + change
    base = [core[k] - STEP_DT * base[k] for k in range(5)]
    adv_ref[0] = base[0]

    def lower(v, d):
        return v[0:X] if d == 0 else ring(v[0:X], v[X:2 * X], -1, d)[0]

    part = []
    for d, (lv, rv) in enumerate(speed):
        ll, rl = lower(lv, d), lower(rv, d)
        lv, rv = (lv[1:X + 1], rv[1:X + 1]) if d == 0 else (lv[0:X], rv[0:X])
        k = -0.5 * STEP_DT / 6.0
        part.append([k * ll, k * (-lv - 5.0 * ll - 2.0 * rl), k * (5.0 * lv + 2.0 * rv - 2.0 * ll - 5.0 * rl),
                     k * (2.0 * lv + 5.0 * rv + rl), -k * rv])
    middle = part[0][2] + part[1][2] + part[2][2]

    def pick(part, ps, step=0):
        value, reach = part
        return cat(*[value[reach + a + step:reach + b + step] for a, b in ps])

    def z_shift(value, ps, pair, step, by=1):
        at = [p for a, b in ps for p in range(a, b)]
        lane = lanes(value.shape)
        if step == 1:
            ghost, edge = [roll(pair[1], L - by - wide * p, 1) for p in at], lane >= L - by
        else:
            ghost, edge = [roll(pair[0], by - wide * p, 1) for p in at], lane < by
        return jnp.where(edge, cat(*[v[None] for v in ghost]), roll(value, -step * by, 2))

    def around_planes(c, y, pair, ps):
        m = pick(c, ps)
        cy = [ring(m, pick(y, ps), s, 1) for s in (1, -1)]
        z = [z_shift(m, ps, pair, s) for s in (1, -1)]
        return [(pick(c, ps, 1), pick(c, ps, -1)), [t[0] for t in cy], z], [t[1] for t in cy]

    def around_ghosts(y, yy, pair, e):
        ps = [(-e, X + e)]
        return [(pick(y, ps, 1), pick(y, ps, -1)), yy, [z_shift(pick(y, ps), ps, pair, s) for s in (1, -1)]]

    def around_packed(z, w):
        out = [], []
        for zt, wt in zip(z, w):
            zy = [ring(zt, wt, s, 0) for s in (1, -1)]
            for to, t, k in ((out[0], zt, 0), (out[1], wt, 1)):
                to.append([(roll(t, -wide, 1), roll(t, wide, 1)), [v[k] for v in zy], (roll(t, -1, 1), roll(t, 1, 1))])
        return out

    late_rho.arrived()
    rho_of = lambda dx, dy, dz: g2[side_slots[(0, 0, -dz)]] if dx == dy == 0 else g3[zr_far[(-dx, -dy, -dz)]]
    every = range(-D, X + D)
    outer = [p for p in every if not 0 <= p < X]
    rho_c = cat(g1[xt[0]:xt[0] + D - 1], xc[0], g1[xt[1]:xt[1] + D - 1])
    rho_ye = cat(*unpack_corner(g3, dr, -1, False), rho_y, *unpack_corner(g3, dr, 1, False))
    rho_z, rho_w = z_pairs(rho_of, 0, pack_planes(rho_own, pick((rho_c, D + 1), [(-D, 0), (X, X + D)]), outer),
                           pack_planes(rho_own, rho_ye, every))
    inv_c, inv_y = (1.0 / rho_c, D + 1), (1.0 / rho_ye, D)
    inv_z, inv_w = [1.0 / t for t in rho_z], [1.0 / t for t in rho_w]
    beyond = [1.0 / z_side(rho_of, 0, dz, 1) for dz in (-1, 1)]
    far_coef = coefficients(pick(inv_c, [(-D, 0), (X, X + D)]),
                            around_planes(inv_c, inv_y, inv_z, [(-D, 0), (X, X + D)])[0])[0]
    coef_c = [[cat(far[0:D], mine, far[D:2 * D]) for far, mine in zip(*pair)] for pair in zip(far_coef, near_w)]
    e = D - 1
    rim = jnp.zeros((e, R, L), jnp.float32)
    yy = around_planes(inv_c, inv_y, inv_z, [(-e, X + e)])[1]
    inv_yy = cat(rim, 1.0 / rho_yy, rim)
    row = rows(inv_yy.shape)
    yy = [jnp.where(row == at, inv_yy, t) for t, at in zip(yy, (H - 1, H))]
    coef_y = coefficients(pick(inv_y, [(-e, X + e)]), around_ghosts(inv_y, yy, inv_w, e))[0]
    coef_y[1] = [jnp.where(row == at, 0.0, t) for t, at in zip(coef_y[1], (H - 1, H))]
    zn, wn = around_packed(inv_z, inv_w)
    coef_z, coef_w = [], []
    for j, at in ((0, DZ), (1, DZ - 1)):
        last = lane2 % wide == at
        pair = list(zn[j][2])
        pair[1 - j] = jnp.where(last, beyond[j], pair[1 - j])
        ws = coefficients(inv_z[j], [*zn[j][0:2], pair])[0]
        ws[2][1 - j] = jnp.where(last, 0.0, ws[2][1 - j])
        coef_z.append(ws)
        coef_w.append(coefficients(inv_w[j], wn[j])[0])

    second.arrived()
    zero = jnp.zeros((1, R, L), jnp.float32)
    sig_of = lambda dx, dy, dz: g4[z2[(-dx, -dy, -dz)]]
    sx, qx = [cat(g4[x2[0] + t:x2[0] + t + D], g4[x2[1] + t:x2[1] + t + D]) for t in (0, D)]
    sy, qy = [unpack_rows(g4[y2[1] + t:y2[1] + t + X // 2], g4[y2[0] + t:y2[0] + t + X // 2], H) for t in (0, X // 2)]
    sy = cat(*unpack_corner(g4, d2, -1, False), sy, *unpack_corner(g4, d2, 1, False))
    qy = cat(*unpack_corner(g4, d2, -1, True), qy, *unpack_corner(g4, d2, 1, True))
    z, w = z_pairs(sig_of, 0, pack_planes(z_own, sx, outer), pack_planes(z_own, sy, every))
    q_own = roll(z_own, L // 2, 1)
    qz, qw = z_pairs(sig_of, 1, pack_planes(q_own, qx, outer), pack_planes(q_own, qy, range(-e, X + e)))
    ghosts = [(z, w)]
    for sweep in range(1, SWEEPS):
        zn, wn = around_packed(z, w)
        z = [update(qz[j], coef_z[j], zn[j]) for j in range(2)]
        if sweep < SWEEPS - 1:
            w = [update(qw[j], coef_w[j], wn[j]) for j in range(2)]
        ghosts.append((z, w))

    def lane_ghost(sweep, which, p):
        return sweep, which, p

    def one_shift(tile, ghost, step, by=1):
        sweep, which, p = ghost
        pair = ghosts[sweep][which]
        if step == 1:
            return jnp.where(lane2 >= L - by, roll(pair[1], L - by - wide * p, 1), roll(tile, -by, 1))
        return jnp.where(lane2 < by, roll(pair[0], by - wide * p, 1), roll(tile, by, 1))

    tiles = lambda value, lo: {lo + k: value[k] for k in range(value.shape[0])}
    c = {**tiles(sigma1, 0), **tiles(sx[0:D], -D), **tiles(sx[D:2 * D], X), -D - 1: zero[0], X + D: zero[0]}
    qc = {**tiles(source, 0), **tiles(qx[0:D], -D), **tiles(qx[D:2 * D], X)}
    y, qy = tiles(sy, -D), tiles(qy, -e)
    cs, ys = [c] + [{} for _ in range(1, SWEEPS)], [y] + [{} for _ in range(1, SWEEPS)]

    def sweep_plane(sweep, p):
        c, y = cs[sweep - 1], ys[sweep - 1]
        ec, ey = D + 1 - sweep, 0 if sweep == SWEEPS - 1 else D - sweep
        if not -ec <= p < X + ec:
            return
        cy = [ring(c[p], y[p], s, 0) for s in (1, -1)]
        ghost = lane_ghost(sweep - 1, 0, p)
        nbr = [(c[p + 1], c[p - 1]), [t[0] for t in cy], [one_shift(c[p], ghost, s) for s in (1, -1)]]
        cs[sweep][p] = update(qc[p], [[v[D + p] for v in pair] for pair in coef_c], nbr)
        if -ey <= p < X + ey:
            ghost = lane_ghost(sweep - 1, 1, p)
            nbr = [(y[p + 1], y[p - 1]), [t[1] for t in cy], [one_shift(y[p], ghost, s) for s in (1, -1)]]
            ys[sweep][p] = update(qy[p], [[v[e + p] for v in pair] for pair in coef_y], nbr)

    def flux_plane(p):
        if not 0 <= p < X:
            return
        c, y, ghost = cs[SWEEPS - 1], ys[SWEEPS - 1], lane_ghost(SWEEPS - 1, 0, p)
        out_sig_ref[p] = c[p]

        def y_shift(step, by):
            edge = row2 >= R - by if step == 1 else row2 < by
            return jnp.where(edge, roll(y[p], -step * by, 0), roll(c[p], -step * by, 0))

        total = base[4][p] + middle[p] * c[p]
        shifts = [lambda s, by: c[p + s * by], y_shift, lambda s, by: one_shift(c[p], ghost, s, by)]
        for d in range(3):
            (p1, p2), (m1, m2) = [[shifts[d](s, by) for by in (1, 2)] for s in (1, -1)]
            adv_ref[1 + d, p] = base[1 + d][p] + ((-4.0 * STEP_DT / 6.0) * (p1 - m1) + (0.5 * STEP_DT / 6.0) * (p2 - m2))
            a = [v[p] for v in part[d]]
            total = total + (a[0] * m2 + a[1] * m1 + a[3] * p1 + a[4] * p2)
        adv_ref[4, p] = total

    for step in range(-D, X + D + 2 * SWEEPS):
        for sweep in range(1, SWEEPS):
            sweep_plane(sweep, step - 2 * (sweep - 1))
        flux_plane(step - 2 * (SWEEPS - 1) - 1)
    assert sum(group.rows for group in groups) == sent.shape[0]
    second.copy(sent, sent, NEAR[0]).wait_send()


def write(adv, sig, adv_hbm, sig_hbm, sem):
    copies = [pltpu.make_async_copy(src, dst, sem.at[n])
              for n, (src, dst) in enumerate(((adv, adv_hbm), (sig, sig_hbm)))]
    for copy in copies:
        copy.start()
    for copy in copies:
        copy.wait()


def solution(mesh):
    sizes = tuple(mesh.shape[a] for a in AXES)

    def on_device(conserved, sigma_guess):
        X, R, L = sigma_guess.shape
        A, B, H, D = X // R, 2 * X // R, X // 2, DEPTH
        f32 = jnp.float32
        vm = lambda *shape: pltpu.VMEM((*shape, R, L), f32)
        nd = len(XY_MOVES)
        tiles = landing(X, R, sizes)
        rows = [R * n + sum(part) for n, part in tiles]
        spare = [pltpu.VMEM((n, 1, L), f32) for n in (rows[3], rows[4], sum(rows))]
        outs = pl.pallas_call(
            functools.partial(kernel, sizes),
            out_shape=(pltpu.VMEM(conserved.shape, f32), pltpu.VMEM(sigma_guess.shape, f32)),
            in_specs=[pl.BlockSpec(memory_space=pl.ANY)] * 2,
            out_specs=(pl.BlockSpec(memory_space=pltpu.VMEM),) * 2,
            scratch_shapes=[
                vm(5, X), vm(X), *[vm(n + len(part)) for n, part in tiles], *spare,
                vm(2, 5 * A), vm(2), vm(2, 3 * A + B), vm(2, H), vm(), vm(nd, 2),
                vm(2, 2 * D), vm(2, 2 * H), vm(), vm(nd, 2),
                pltpu.SemaphoreType.DMA((2,)),
                pltpu.SemaphoreType.REGULAR,
                pltpu.SemaphoreType.DMA,
                pltpu.SemaphoreType.DMA((len(tiles),)),
            ],
            compiler_params=pltpu.CompilerParams(collective_id=0, has_side_effects=True),
        )(conserved, sigma_guess)
        return pl.pallas_call(
            write,
            out_shape=tuple(jax.ShapeDtypeStruct(a.shape, f32) for a in (conserved, sigma_guess)),
            in_specs=[pl.BlockSpec(memory_space=pltpu.VMEM)] * 2,
            out_specs=(pl.BlockSpec(memory_space=pl.ANY),) * 2,
            scratch_shapes=[pltpu.SemaphoreType.DMA((2,))],
        )(*(pltpu.with_memory_space_constraint(v, pltpu.VMEM) for v in outs))

    specs = (P(None, "gx", "gy", "gz"), P("gx", "gy", "gz"))
    return jax.shard_map(on_device, mesh=mesh, in_specs=specs, out_specs=specs, check_vma=False)
```

```python
import functools
import itertools

import jax
import jax.numpy as jnp
from jax import lax
from jax.experimental import pallas as pl
from jax.experimental.pallas import tpu as pltpu
from jax.sharding import PartitionSpec as P

SWEEPS = 4
ALPHA = 10.0
GAMMA = 1.4
LAMBDA = 3.0
STEP_DT = 0.4
DEPTH = SWEEPS
MESH = pl.DeviceIdType.MESH
AXES = ("gx", "gy", "gz")

OFFSETS = [o for o in itertools.product((-1, 0, 1), repeat=3) if any(o)]
NEAR = [(0, 1, 0), (0, -1, 0), (1, 0, 0), (-1, 0, 0), (0, 0, 1), (0, 0, -1)]
XY_MOVES = [o for o in OFFSETS if o[0] != 0 and o[1] != 0 and o[2] == 0]
Z_NEAR = [(0, 0, 1), (0, 0, -1)]
Z_VERTEX = [o for o in OFFSETS if all(o)]
Z_EDGE = [o for o in OFFSETS if o[2] != 0 and o not in Z_NEAR and o not in Z_VERTEX]


def iota(shape, dim):
    return lax.broadcasted_iota(jnp.int32, shape, dim)


def roll(value, shift, axis):
    size = value.shape[axis]
    shift = shift % size
    return value if shift == 0 else pltpu.roll(value, shift, axis)


def ring(core, ghost, step, axis):
    size = core.shape[axis]
    a, b = roll(core, -step, axis), roll(ghost, -step, axis)
    edge = iota(core.shape, axis) == (size - 1 if step == 1 else 0)
    return jnp.where(edge, b, a), jnp.where(edge, a, b)


def distinct(moves, sizes):
    first = {}
    return {o: first.setdefault(tuple(v % s for v, s in zip(o, sizes)), o) for o in moves}


def z_rows(offset, R):
    n = R if offset[1] == 0 else DEPTH - 1 if offset[0] else DEPTH
    return slice(0, n) if offset[1] == -1 else slice(R - n, R)


def landing(X, R, sizes):
    sent = lambda moves: sorted(set(distinct(moves, sizes).values()))
    rows = [z_rows(o, R).stop - z_rows(o, R).start for o in sent(Z_EDGE) + sent(Z_VERTEX)]
    part = [n for n in rows if n < R]
    full = len(rows) - len(part)
    A, B, H = X // R, 2 * X // R, X // 2
    near, corner = len(sent(Z_NEAR)), 2 * len(XY_MOVES)
    return [
        (2 * (5 + 2), []),
        (2 * (H + 3 * A + B + 5 + 1 + DEPTH - 1), []),
        (near, []),
        (len(XY_MOVES) + full, part + [2] * len(XY_MOVES)),
        (corner + near + full + 2 * 2 * H + 2 * 2 * DEPTH, part),
        (2 * 5 * A, []),
    ]


def kernel(sizes, cons_hbm, sig_hbm, adv_ref, out_sig_ref, cons, sig, g0, g1, g2, g3, g4, g5, t3, t4, sent,
           yas, zas, ybs, yrs, zrs, drs, x2s, y2s, z2s, d2s, in_sem, ready, send_sem, recv_sem):
    X, R, L = sig.shape
    H, D, DZ = R // 2, DEPTH, L // (4 * X)
    wide = 2 * DZ
    me = [lax.axis_index(a) for a in AXES]

    def device(offset):
        return {a: lax.rem(me[i] + offset[i] + sizes[i], sizes[i]) for i, a in enumerate(AXES)}

    load_c = pltpu.make_async_copy(cons_hbm, cons, in_sem.at[0])
    load_s = pltpu.make_async_copy(sig_hbm, sig, in_sem.at[1])
    load_c.start()
    load_s.start()
    barrier = pltpu.get_barrier_semaphore()
    for o in NEAR:
        pl.semaphore_signal(barrier, inc=1, device_id=device(o), device_id_type=MESH)

    class Group:
        def __init__(self, n, buf, spare):
            self.n, self.buf, self.spare, self.used, self.rows = n, buf, spare, 0, 0

        def copy(self, src, dst, offset):
            return pltpu.make_async_remote_copy(
                src_ref=src, dst_ref=dst, send_sem=send_sem, recv_sem=recv_sem.at[self.n],
                device_id=device(offset), device_id_type=MESH)

        def send(self, src, offset, part=None):
            at = self.used
            if part is not None:
                self.used += 1
                self.rows += part.stop - part.start
                self.copy(src.at[part], self.buf.at[at, part], offset).start()
            elif len(src.shape) == 2:
                self.used, self.rows = at + 1, self.rows + R
                self.copy(src, self.buf.at[at], offset).start()
            else:
                self.used, self.rows = at + src.shape[0], self.rows + R * src.shape[0]
                self.copy(src, self.buf.at[at:self.used], offset).start()
            return at

        def arrived(self):
            assert self.used == self.buf.shape[0] and self.rows == self.spare.shape[0] * self.spare.shape[1]
            self.copy(self.spare, self.spare, NEAR[0]).wait_recv()

    groups = [Group(n, buf, size)
              for n, (buf, size) in enumerate(zip((g0, g1, g2, g3, g4, g5), (g0, g1, g2, t3, t4, g5)))]
    first, late, side, late_rho, second, first_y = groups

    rows = lambda shape: iota(shape, len(shape) - 2)
    lanes = lambda shape: iota(shape, len(shape) - 1)

    def pack_rows(field, first, n):
        size = X * n // R
        out = field[0:size]
        r = rows(out.shape)
        for g in range(1, R // n):
            part = roll(field[g * size:(g + 1) * size], n * g, 1)
            out = jnp.where((r + (2 * R - first - n * g)) % R < n, part, out)
        return out

    def unpack_rows(after, before, n):
        low = rows(after.shape) < H
        return jnp.concatenate(
            [jnp.where(low, roll(after, -n * g, 1), roll(before, -n * g, 1)) for g in range(R // n)],
            axis=0)

    lane2, row2 = lanes((R, L)), rows((R, L))
    low2 = row2 < H

    def pack_lanes(fields, width):
        out = jnp.zeros((R, L), jnp.float32)
        for k, tile in enumerate(f[p] for f in fields for p in range(X)):
            out = jnp.where(((lane2 + width // 2) % L) // width == k, roll(tile, width * k, 1), out)
        return out

    slot2 = ((lane2 + DZ) % L) // wide
    side2 = lane2 % wide >= DZ

    def pack_planes(out, value, ps):
        for k, p in enumerate(ps):
            out = jnp.where(slot2 == p % (2 * X), roll(value[k], wide * p, 1), out)
        return out

    def pack_corner(f, s, o):
        a1, a2, a3, a4 = (f[X - a if o[0] == 1 else a - 1] for a in range(1, 5))
        if o[1] == 1:
            one = jnp.where(row2 >= H, a1, jnp.where(row2 >= 1, roll(a2, -H, 0), roll(a4, 1, 0)))
            two = roll(a3, 2, 0)
        else:
            one = jnp.where(row2 < H, a1, jnp.where(row2 < R - 1, roll(a2, H, 0), roll(a4, -1, 0)))
            two = roll(a3, -2, 0)
        if s is not None:
            s1, s2, s3 = (s[X - a if o[0] == 1 else a - 1] for a in range(1, 4))
            if o[1] == 1:
                two = jnp.where(row2 > H, s1, jnp.where(row2 == H, roll(s3, 1 - H, 0),
                                                        jnp.where(row2 >= 2, roll(s2, -H, 0), two)))
            else:
                two = jnp.where(row2 < H - 1, s1, jnp.where(row2 == H - 1, roll(s3, H - 1, 0),
                                                            jnp.where(row2 < R - 2, roll(s2, H, 0), two)))
        return one, two

    def unpack_corner(buf, slots, dx, source):
        after, before = slots[(-dx, -1, 0)], slots[(-dx, 1, 0)]
        fa, fb, sa, sb = buf[after], buf[before], buf[after + 1], buf[before + 1]
        if source:
            out = [jnp.where(low2, sa, sb), roll(jnp.where(low2, sb, sa), H, 0),
                   jnp.where(low2, roll(sa, 1 - H, 0), roll(sb, H - 1, 0))]
        else:
            out = [jnp.where(low2, fa, fb), roll(jnp.where(low2, fb, fa), H, 0),
                   jnp.where(low2, roll(sa, 2, 0), roll(sb, -2, 0)),
                   jnp.where(low2, roll(fa, 1, 0), roll(fb, -1, 0))]
        out = [v[None] for v in out]
        return out if dx == 1 else out[::-1]

    def cat(*parts):
        return jnp.concatenate(parts, axis=0)

    ups = ((0, 1), (1, -1))

    def plane(d, back=0):
        return X - 1 - back if d == 1 else back

    def planes(d, count, back=0):
        return slice(X - count - back, X - back) if d == 1 else slice(back, back + count)

    def send_z(group, src_ref, moves, slots):
        for o, same in distinct(moves, sizes).items():
            slots[o] = group.send(src_ref, o, z_rows(o, R)) if o == same else slots[same]

    def z_side(of, dy, dz, f):
        own, after, before = (of(dx, dy, dz) for dx in (0, 1, -1))
        if f == 0:
            return jnp.where(slot2 < X, own, roll(jnp.where(slot2 < X // 2, after, before), L // 2, 1))
        return jnp.where(slot2 < X, roll(own, L // 2, 1), jnp.where(slot2 < X + X // 2, after, before))

    def sides(own, low, high):
        return jnp.where(side2, low, own), jnp.where(side2, own, high)

    def z_pairs(of, f, own_z, own_w):
        z = [z_side(of, 0, dz, f) for dz in (-1, 1)]
        w = [jnp.where(low2, z_side(of, 1, dz, f), z_side(of, -1, dz, f)) for dz in (-1, 1)]
        return sides(own_z, *z), sides(own_w, *w)

    load_c.wait()
    load_s.wait()
    state = [cons[f] for f in range(4)] + [sig[...]]
    energy = cons[4]
    A, B = X // R, 2 * X // R
    for f in range(5):
        yas[0, f * A:(f + 1) * A] = pack_rows(state[f], R - 1, 1)
        yas[1, f * A:(f + 1) * A] = pack_rows(state[f], 0, 1)
    zas[0] = pack_lanes(state[0:4], 4)
    zas[1] = pack_lanes([state[4], energy], 4)
    pl.semaphore_wait(barrier, len(NEAR))
    ya = [first_y.send(yas.at[j], (0, d, 0)) for j, d in ups]
    xa = []
    for j, d in ups:
        xa.append(first.send(cons.at[0:4, plane(d)], (d, 0, 0)))
        first.send(sig.at[plane(d)], (d, 0, 0))
    za = [first.send(zas, (0, 0, d)) for j, d in ups]
    for o in NEAR:
        pl.semaphore_signal(ready, inc=1, device_id=device(o), device_id_type=MESH)

    for j, second_row, start in ((0, R - 2, R - 1 - H), (1, 1, 1)):
        for f in range(3):
            ybs[j, f * A:(f + 1) * A] = pack_rows(state[1 + f], second_row, 1)
        ybs[j, 3 * A:3 * A + B] = pack_rows(energy, (R - 2, 0)[j], 2)
        yrs[j] = pack_rows(state[0], start, H)
    xb, xe, xt = [], [], []
    for j, d in ups:
        xb.append(late.send(cons.at[0:5, plane(d, 1)], (d, 0, 0)))
        xe.append(late.send(cons.at[4, plane(d)], (d, 0, 0)))
        xt.append(late.send(cons.at[0, planes(d, D - 1, 2)], (d, 0, 0)))
    lane3 = lanes(energy.shape)
    row3 = rows(energy.shape)
    rho_zz = jnp.where(lane3 == DZ - 1, roll(state[0], -1, 2), roll(state[0], 1, 2))
    rho_own = pack_lanes([state[0], rho_zz], wide)
    zrs[...] = rho_own
    for n, o in enumerate(XY_MOVES):
        drs[n, 0], drs[n, 1] = pack_corner(state[0], None, o)

    pl.semaphore_wait(ready, len(NEAR))
    zr, dr = {}, {}
    send_z(side, zrs, Z_NEAR, zr)
    side_slots = dict(zr)
    for n, o in enumerate(XY_MOVES):
        dr[o] = late_rho.send(drs.at[n, 0], o)
        late_rho.send(drs.at[n, 1], o, slice(0, 2) if o[1] == 1 else slice(R - 2, R))
    zr_far = {}
    send_z(late_rho, zrs, Z_EDGE, zr_far)
    yr, yb = [], []
    for j, d in ups:
        yr.append(late.send(yrs.at[j], (0, d, 0)))
        yb.append(late.send(ybs.at[j], (0, d, 0)))

    inv0 = 1.0 / state[0]
    fields = [inv0] + [state[k] * inv0 for k in (1, 2, 3)] + [state[4]]
    own = [[[roll(v, -s, axis) for s in (1, -1)] for axis in (1, 2)] for v in fields]
    region = ((lane2 + 2) % L) // (4 * X)

    def to_speed(t):
        r = 1.0 / t[0]
        return [r] + [m * r for m in t[1:4]] + [t[4]]

    def coefficients(inv_m, inv_n):
        ws = [[inv_m + inv_n[d][s] for s in range(2)] for d in range(3)]
        scale = ALPHA / (2.0 * inv_m + ALPHA * sum(w for pair in ws for w in pair))
        return [[w * scale for w in pair] for pair in ws]

    def update(source, ws, nbr):
        acc = source
        for d in range(3):
            for s in range(2):
                acc = acc + ws[d][s] * nbr[d][s]
        return acc

    first.arrived()
    xg = [to_speed([g0[xa[j] + f] for f in range(5)]) for j in range(2)]
    zmerged = [jnp.where(lane2 % 4 < 2, g0[za[1] + v], g0[za[0] + v]) for v in range(2)]
    zinv = 1.0 / jnp.where(region == 0, zmerged[0], 1.0)
    shifted = [roll(zinv, 4 * X * k, 1) for k in (1, 2, 3)]
    zspeed = zmerged[0] * jnp.where(region == 1, shifted[0], jnp.where(region == 2, shifted[1], shifted[2]))
    zspeed = jnp.where(region == 0, zinv, zspeed)

    def xz_neighbours(f):
        v, (_, (zp, zm)) = fields[f], own[f]
        t, k = (zspeed, f * X) if f < 4 else (zmerged[1], 0)
        high = cat(*[roll(t, L - 1 - 4 * (k + p), 1)[None] for p in range(X)])
        low = cat(*[roll(t, 1 - 4 * (k + p), 1)[None] for p in range(X)])
        return [(cat(v[1:X], xg[1][f][None]), cat(xg[0][f][None], v[0:X - 1])),
                (jnp.where(lane3 == L - 1, high, zp), jnp.where(lane3 == 0, low, zm))]

    ws = [None] * 3
    ws[0], ws[2] = [[inv0 + v for v in pair] for pair in xz_neighbours(0)]
    (g00, g02), (g10, g12), (g20, g22) = [[p - m for p, m in xz_neighbours(k)] for k in (1, 2, 3)]
    squares, div = g00 * g00 + g22 * g22 + 2.0 * (g02 * g20), g00 + g22
    weight = ws[0][0] + ws[0][1] + ws[2][0] + ws[2][1]
    (xp, xm), (zp, zm) = xz_neighbours(4)
    inflow = ws[0][0] * xp + ws[0][1] * xm + ws[2][0] * zp + ws[2][1] * zm

    side.arrived()
    send_z(late_rho, zrs, Z_VERTEX, zr_far)
    first_y.arrived()
    yg = [to_speed([g5[ya[j] + f * A:ya[j] + (f + 1) * A] for f in range(5)]) for j in range(2)]

    def y_neighbours(f):
        yp, ym = own[f][0]
        after = cat(*[roll(yg[1][f], R - 1 - p, 1) for p in range(R)])
        before = cat(*[roll(yg[0][f], 1 - p, 1) for p in range(R)])
        return jnp.where(row3 == R - 1, after, yp), jnp.where(row3 == 0, before, ym)

    ws[1] = [inv0 + v for v in y_neighbours(0)]
    near_scale = ALPHA / (2.0 * inv0 + ALPHA * (weight + ws[1][0] + ws[1][1]))
    g01, g11, g21 = [p - m for p, m in (y_neighbours(k) for k in (1, 2, 3))]
    div = div + g11
    source = squares + g11 * g11 + 2.0 * (g01 * g10 + g12 * g21) + div * div
    source = source * (0.5 * near_scale)
    yp, ym = y_neighbours(4)
    sigma1 = source + near_scale * (inflow + ws[1][0] * yp + ws[1][1] * ym)
    near_w = [[w * near_scale for w in pair] for pair in ws]

    z_fold = jnp.where(lane3 == DZ - 1, near_w[2][0] * roll(sigma1, -1, 2),
                       jnp.where(lane3 == L - DZ, near_w[2][1] * roll(sigma1, 1, 2), 0.0))
    z_own = pack_lanes([sigma1, source + z_fold], wide)
    z2s[...] = z_own
    z2, d2 = {}, {}
    send_z(second, z2s, Z_VERTEX, z2)
    for n, o in enumerate(XY_MOVES):
        d2s[n, 0], d2s[n, 1] = pack_corner(sigma1, source, o)
        d2[o] = second.send(d2s.at[n], o)
    send_z(second, z2s, Z_EDGE, z2)
    y_fold = jnp.where(row3 == H - 1, near_w[1][0] * roll(sigma1, -1, 1),
                       jnp.where(row3 == H, near_w[1][1] * roll(sigma1, 1, 1), 0.0))
    for j, start in ((0, H), (1, 0)):
        y2s[j, 0:X // 2] = pack_rows(sigma1, start, H)
        y2s[j, X // 2:X] = pack_rows(source + y_fold, start, H)
    y2 = [second.send(y2s.at[j], (0, d, 0)) for j, d in ups]
    for j, d in ups:
        x2s[j, 0:D] = sigma1[planes(d, D)]
        x2s[j, D:2 * D] = source[planes(d, D)]
    x2s[0, D] = source[X - D] + near_w[0][1][X - D] * sigma1[X - D - 1]
    x2s[1, 2 * D - 1] = source[D - 1] + near_w[0][0][D - 1] * sigma1[D]
    x2 = [second.send(x2s.at[j], (d, 0, 0)) for j, d in ups]
    send_z(second, z2s, Z_NEAR, z2)

    late.arrived()
    core = state[0:4] + [energy]
    near_row = (row3 == 0) | (row3 == R - 1)

    def first_rows(f):
        return unpack_rows(g5[ya[1] + f * A:ya[1] + (f + 1) * A], g5[ya[0] + f * A:ya[0] + (f + 1) * A], 1)

    def late_rows(at, to, n):
        return unpack_rows(g1[yb[1] + at:yb[1] + to], g1[yb[0] + at:yb[0] + to], n)

    rho_before, rho_after = [cat(*[roll(g1[yr[j]:yr[j] + X // 2], -H * k, 1) for k in range(R // H)]) for j in range(2)]
    rho_y = jnp.where(near_row, first_rows(0), jnp.where(row3 < H, rho_after, rho_before))
    rho_yy = jnp.where(row3 < H, roll(rho_after, -1, 1), roll(rho_before, 1, 1))
    xn = [[g0[xa[j] + f][None] for f in range(4)] + [g1[xe[j]][None]] for j in range(2)]
    xc = [cat(g1[xb[0] + f][None], xn[0][f], core[f], xn[1][f], g1[xb[1] + f][None]) for f in range(5)]
    yc = [rho_y] + [jnp.where(near_row, first_rows(1 + f), late_rows(f * A, (f + 1) * A, 1)) for f in range(3)]
    yc.append(late_rows(3 * A, 3 * A + B, 2))
    zc = [cat(*[roll(zmerged[f // 4], -4 * (f * X + p), 1)[None] for p in range(X)]) for f in range(4)]
    zc.append(cat(*[roll(zmerged[1], -4 * (X + p), 1)[None] for p in range(X)]))

    def x_stencil(c):
        return c[0:X + 1], c[1:X + 2], c[2:X + 3], c[3:X + 4]

    def ring_stencil(c, gh, axis):
        m, p = ring(c, gh, -1, axis), ring(c, gh, 1, axis)
        return cat(*m), cat(c, gh), cat(*p), cat(*ring(p[0], p[1], 1, axis))

    def faces(st):
        m, q, p, pp = st
        sixth = 1.0 / 6.0
        return (5.0 * q + 2.0 * p - m) * sixth, (2.0 * q + 5.0 * p - pp) * sixth

    def plain_flux(s, d):
        r = 1.0 / s[0]
        v = s[1 + d] * r
        pressure = (GAMMA - 1.0) * (s[4] - 0.5 * (s[1] * s[1] + s[2] * s[2] + s[3] * s[3]) * r)
        out = [s[1 + d]]
        for k in range(3):
            out.append(s[1 + k] * v + pressure if k == d else s[1 + k] * v)
        out.append((s[4] + pressure) * v)
        return out, v

    def difference(flux, d):
        if d == 0:
            return flux[1:X + 1] - flux[0:X]
        return flux[0:X] - ring(flux[0:X], flux[X:2 * X], -1, d)[0]

    base = [None] * 5
    speed = []
    for d in range(3):
        if d == 0:
            lr = [faces(x_stencil(c)) for c in xc]
        else:
            lr = [faces(ring_stencil(c, gh, d)) for c, gh in zip(core, (None, yc, zc)[d])]
        lf, lv = plain_flux([v[0] for v in lr], d)
        rf, rv = plain_flux([v[1] for v in lr], d)
        speed.append((lv, rv))
        for k in range(5):
            flux = 0.5 * (lf[k] + rf[k]) - (0.5 * LAMBDA) * (lr[k][1] - lr[k][0])
            change = difference(flux, d)
            base[k] = change if base[k] is None else base[k] + change
    base = [core[k] - STEP_DT * base[k] for k in range(5)]
    adv_ref[0] = base[0]

    def lower(v, d):
        return v[0:X] if d == 0 else ring(v[0:X], v[X:2 * X], -1, d)[0]

    part = []
    for d, (lv, rv) in enumerate(speed):
        ll, rl = lower(lv, d), lower(rv, d)
        lv, rv = (lv[1:X + 1], rv[1:X + 1]) if d == 0 else (lv[0:X], rv[0:X])
        k = -0.5 * STEP_DT / 6.0
        part.append([k * ll, k * (-lv - 5.0 * ll - 2.0 * rl), k * (5.0 * lv + 2.0 * rv - 2.0 * ll - 5.0 * rl),
                     k * (2.0 * lv + 5.0 * rv + rl), -k * rv])
    middle = part[0][2] + part[1][2] + part[2][2]

    def pick(part, ps, step=0):
        value, reach = part
        return cat(*[value[reach + a + step:reach + b + step] for a, b in ps])

    def z_shift(value, ps, pair, step, by=1):
        at = [p for a, b in ps for p in range(a, b)]
        lane = lanes(value.shape)
        if step == 1:
            ghost, edge = [roll(pair[1], L - by - wide * p, 1) for p in at], lane >= L - by
        else:
            ghost, edge = [roll(pair[0], by - wide * p, 1) for p in at], lane < by
        return jnp.where(edge, cat(*[v[None] for v in ghost]), roll(value, -step * by, 2))

    def around_planes(c, y, pair, ps):
        m = pick(c, ps)
        cy = [ring(m, pick(y, ps), s, 1) for s in (1, -1)]
        z = [z_shift(m, ps, pair, s) for s in (1, -1)]
        return [(pick(c, ps, 1), pick(c, ps, -1)), [t[0] for t in cy], z], [t[1] for t in cy]

    def around_ghosts(y, yy, pair, e):
        ps = [(-e, X + e)]
        return [(pick(y, ps, 1), pick(y, ps, -1)), yy, [z_shift(pick(y, ps), ps, pair, s) for s in (1, -1)]]

    def around_packed(z, w):
        out = [], []
        for zt, wt in zip(z, w):
            zy = [ring(zt, wt, s, 0) for s in (1, -1)]
            for to, t, k in ((out[0], zt, 0), (out[1], wt, 1)):
                to.append([(roll(t, -wide, 1), roll(t, wide, 1)), [v[k] for v in zy], (roll(t, -1, 1), roll(t, 1, 1))])
        return out

    late_rho.arrived()
    rho_of = lambda dx, dy, dz: g2[side_slots[(0, 0, -dz)]] if dx == dy == 0 else g3[zr_far[(-dx, -dy, -dz)]]
    every = range(-D, X + D)
    outer = [p for p in every if not 0 <= p < X]
    rho_c = cat(g1[xt[0]:xt[0] + D - 1], xc[0], g1[xt[1]:xt[1] + D - 1])
    rho_ye = cat(*unpack_corner(g3, dr, -1, False), rho_y, *unpack_corner(g3, dr, 1, False))
    rho_z, rho_w = z_pairs(rho_of, 0, pack_planes(rho_own, pick((rho_c, D + 1), [(-D, 0), (X, X + D)]), outer),
                           pack_planes(rho_own, rho_ye, every))
    inv_c, inv_y = (1.0 / rho_c, D + 1), (1.0 / rho_ye, D)
    inv_z, inv_w = [1.0 / t for t in rho_z], [1.0 / t for t in rho_w]
    beyond = [1.0 / z_side(rho_of, 0, dz, 1) for dz in (-1, 1)]
    far_coef = coefficients(pick(inv_c, [(-D, 0), (X, X + D)]),
                            around_planes(inv_c, inv_y, inv_z, [(-D, 0), (X, X + D)])[0])
    coef_c = [[cat(far[0:D], mine, far[D:2 * D]) for far, mine in zip(*pair)] for pair in zip(far_coef, near_w)]
    e = D - 1
    rim = jnp.zeros((e, R, L), jnp.float32)
    yy = around_planes(inv_c, inv_y, inv_z, [(-e, X + e)])[1]
    inv_yy = cat(rim, 1.0 / rho_yy, rim)
    row = rows(inv_yy.shape)
    yy = [jnp.where(row == at, inv_yy, t) for t, at in zip(yy, (H - 1, H))]
    coef_y = coefficients(pick(inv_y, [(-e, X + e)]), around_ghosts(inv_y, yy, inv_w, e))
    coef_y[1] = [jnp.where(row == at, 0.0, t) for t, at in zip(coef_y[1], (H - 1, H))]
    zn, wn = around_packed(inv_z, inv_w)
    coef_z, coef_w = [], []
    for j, at in ((0, DZ), (1, DZ - 1)):
        last = lane2 % wide == at
        pair = list(zn[j][2])
        pair[1 - j] = jnp.where(last, beyond[j], pair[1 - j])
        coef_z.append(coefficients(inv_z[j], [*zn[j][0:2], pair]))
        coef_z[j][2][1 - j] = jnp.where(last, 0.0, coef_z[j][2][1 - j])
        coef_w.append(coefficients(inv_w[j], wn[j]))

    second.arrived()
    zero = jnp.zeros((1, R, L), jnp.float32)
    sig_of = lambda dx, dy, dz: g4[z2[(-dx, -dy, -dz)]]
    sx, qx = [cat(g4[x2[0] + t:x2[0] + t + D], g4[x2[1] + t:x2[1] + t + D]) for t in (0, D)]
    sy, qy = [unpack_rows(g4[y2[1] + t:y2[1] + t + X // 2], g4[y2[0] + t:y2[0] + t + X // 2], H) for t in (0, X // 2)]
    sy = cat(*unpack_corner(g4, d2, -1, False), sy, *unpack_corner(g4, d2, 1, False))
    qy = cat(*unpack_corner(g4, d2, -1, True), qy, *unpack_corner(g4, d2, 1, True))
    z, w = z_pairs(sig_of, 0, pack_planes(z_own, sx, outer), pack_planes(z_own, sy, every))
    q_own = roll(z_own, L // 2, 1)
    qz, qw = z_pairs(sig_of, 1, pack_planes(q_own, qx, outer), pack_planes(q_own, qy, range(-e, X + e)))
    ghosts = [(z, w)]
    for sweep in range(1, SWEEPS):
        zn, wn = around_packed(z, w)
        z = [update(qz[j], coef_z[j], zn[j]) for j in range(2)]
        if sweep < SWEEPS - 1:
            w = [update(qw[j], coef_w[j], wn[j]) for j in range(2)]
        ghosts.append((z, w))

    def lane_ghost(sweep, which, p):
        return sweep, which, p

    def one_shift(tile, ghost, step, by=1):
        sweep, which, p = ghost
        pair = ghosts[sweep][which]
        if step == 1:
            return jnp.where(lane2 >= L - by, roll(pair[1], L - by - wide * p, 1), roll(tile, -by, 1))
        return jnp.where(lane2 < by, roll(pair[0], by - wide * p, 1), roll(tile, by, 1))

    tiles = lambda value, lo: {lo + k: value[k] for k in range(value.shape[0])}
    c = {**tiles(sigma1, 0), **tiles(sx[0:D], -D), **tiles(sx[D:2 * D], X), -D - 1: zero[0], X + D: zero[0]}
    qc = {**tiles(source, 0), **tiles(qx[0:D], -D), **tiles(qx[D:2 * D], X)}
    y, qy = tiles(sy, -D), tiles(qy, -e)
    cs, ys = [c] + [{} for _ in range(1, SWEEPS)], [y] + [{} for _ in range(1, SWEEPS)]

    def sweep_plane(sweep, p):
        c, y = cs[sweep - 1], ys[sweep - 1]
        ec, ey = D + 1 - sweep, 0 if sweep == SWEEPS - 1 else D - sweep
        if not -ec <= p < X + ec:
            return
        cy = [ring(c[p], y[p], s, 0) for s in (1, -1)]
        ghost = lane_ghost(sweep - 1, 0, p)
        nbr = [(c[p + 1], c[p - 1]), [t[0] for t in cy], [one_shift(c[p], ghost, s) for s in (1, -1)]]
        cs[sweep][p] = update(qc[p], [[v[D + p] for v in pair] for pair in coef_c], nbr)
        if -ey <= p < X + ey:
            ghost = lane_ghost(sweep - 1, 1, p)
            nbr = [(y[p + 1], y[p - 1]), [t[1] for t in cy], [one_shift(y[p], ghost, s) for s in (1, -1)]]
            ys[sweep][p] = update(qy[p], [[v[e + p] for v in pair] for pair in coef_y], nbr)

    def flux_plane(p):
        if not 0 <= p < X:
            return
        c, y, ghost = cs[SWEEPS - 1], ys[SWEEPS - 1], lane_ghost(SWEEPS - 1, 0, p)
        out_sig_ref[p] = c[p]

        def y_shift(step, by):
            edge = row2 >= R - by if step == 1 else row2 < by
            return jnp.where(edge, roll(y[p], -step * by, 0), roll(c[p], -step * by, 0))

        total = base[4][p] + middle[p] * c[p]
        shifts = [lambda s, by: c[p + s * by], y_shift, lambda s, by: one_shift(c[p], ghost, s, by)]
        for d in range(3):
            (p1, p2), (m1, m2) = [[shifts[d](s, by) for by in (1, 2)] for s in (1, -1)]
            adv_ref[1 + d, p] = base[1 + d][p] + ((-4.0 * STEP_DT / 6.0) * (p1 - m1) + (0.5 * STEP_DT / 6.0) * (p2 - m2))
            a = [v[p] for v in part[d]]
            total = total + (a[0] * m2 + a[1] * m1 + a[3] * p1 + a[4] * p2)
        adv_ref[4, p] = total

    for step in range(-D, X + D + 2 * SWEEPS):
        for sweep in range(1, SWEEPS):
            sweep_plane(sweep, step - 2 * (sweep - 1))
        flux_plane(step - 2 * (SWEEPS - 1) - 1)
    assert sum(group.rows for group in groups) == sent.shape[0]
    second.copy(sent, sent, NEAR[0]).wait_send()


def write(adv, sig, adv_hbm, sig_hbm, sem):
    copies = [pltpu.make_async_copy(src, dst, sem.at[n])
              for n, (src, dst) in enumerate(((adv, adv_hbm), (sig, sig_hbm)))]
    for copy in copies:
        copy.start()
    for copy in copies:
        copy.wait()


def solution(mesh):
    sizes = tuple(mesh.shape[a] for a in AXES)

    def on_device(conserved, sigma_guess):
        X, R, L = sigma_guess.shape
        A, B, H, D = X // R, 2 * X // R, X // 2, DEPTH
        f32 = jnp.float32
        vm = lambda *shape: pltpu.VMEM((*shape, R, L), f32)
        nd = len(XY_MOVES)
        tiles = landing(X, R, sizes)
        rows = [R * n + sum(part) for n, part in tiles]
        spare = [pltpu.VMEM((n, 1, L), f32) for n in (rows[3], rows[4], sum(rows))]
        outs = pl.pallas_call(
            functools.partial(kernel, sizes),
            out_shape=(pltpu.VMEM(conserved.shape, f32), pltpu.VMEM(sigma_guess.shape, f32)),
            in_specs=[pl.BlockSpec(memory_space=pl.ANY)] * 2,
            out_specs=(pl.BlockSpec(memory_space=pltpu.VMEM),) * 2,
            scratch_shapes=[
                vm(5, X), vm(X), *[vm(n + len(part)) for n, part in tiles], *spare,
                vm(2, 5 * A), vm(2), vm(2, 3 * A + B), vm(2, H), vm(), vm(nd, 2),
                vm(2, 2 * D), vm(2, 2 * H), vm(), vm(nd, 2),
                pltpu.SemaphoreType.DMA((2,)),
                pltpu.SemaphoreType.REGULAR,
                pltpu.SemaphoreType.DMA,
                pltpu.SemaphoreType.DMA((len(tiles),)),
            ],
            compiler_params=pltpu.CompilerParams(collective_id=0, has_side_effects=True),
        )(conserved, sigma_guess)
        return pl.pallas_call(
            write,
            out_shape=tuple(jax.ShapeDtypeStruct(a.shape, f32) for a in (conserved, sigma_guess)),
            in_specs=[pl.BlockSpec(memory_space=pltpu.VMEM)] * 2,
            out_specs=(pl.BlockSpec(memory_space=pl.ANY),) * 2,
            scratch_shapes=[pltpu.SemaphoreType.DMA((2,))],
        )(*(pltpu.with_memory_space_constraint(v, pltpu.VMEM) for v in outs))

    specs = (P(None, "gx", "gy", "gz"), P("gx", "gy", "gz"))
    return jax.shard_map(on_device, mesh=mesh, in_specs=specs, out_specs=specs, check_vma=False)
```

```python
import functools
import itertools

import jax
import jax.numpy as jnp
from jax import lax
from jax.experimental import pallas as pl
from jax.experimental.pallas import tpu as pltpu
from jax.sharding import PartitionSpec as P

SWEEPS = 4
ALPHA = 10.0
GAMMA = 1.4
LAMBDA = 3.0
STEP_DT = 0.4
DEPTH = SWEEPS
MESH = pl.DeviceIdType.MESH
AXES = ("gx", "gy", "gz")

OFFSETS = [o for o in itertools.product((-1, 0, 1), repeat=3) if any(o)]
NEAR = [(0, 1, 0), (0, -1, 0), (1, 0, 0), (-1, 0, 0), (0, 0, 1), (0, 0, -1)]
XY_MOVES = [o for o in OFFSETS if o[0] != 0 and o[1] != 0 and o[2] == 0]
Z_NEAR = [(0, 0, 1), (0, 0, -1)]
Z_VERTEX = [o for o in OFFSETS if all(o)]
Z_EDGE = [o for o in OFFSETS if o[2] != 0 and o not in Z_NEAR and o not in Z_VERTEX]


def iota(shape, dim):
    return lax.broadcasted_iota(jnp.int32, shape, dim)


def roll(value, shift, axis):
    size = value.shape[axis]
    shift = shift % size
    return value if shift == 0 else pltpu.roll(value, shift, axis)


def ring(core, ghost, step, axis):
    size = core.shape[axis]
    a, b = roll(core, -step, axis), roll(ghost, -step, axis)
    edge = iota(core.shape, axis) == (size - 1 if step == 1 else 0)
    return jnp.where(edge, b, a), jnp.where(edge, a, b)


def distinct(moves, sizes):
    first = {}
    return {o: first.setdefault(tuple(v % s for v, s in zip(o, sizes)), o) for o in moves}


def z_rows(offset, R):
    n = R if offset[1] == 0 else DEPTH - 1 if offset[0] else DEPTH
    return slice(0, n) if offset[1] == -1 else slice(R - n, R)


def landing(X, R, sizes):
    sent = lambda moves: sorted(set(distinct(moves, sizes).values()))
    rows = [z_rows(o, R).stop - z_rows(o, R).start for o in sent(Z_EDGE) + sent(Z_VERTEX)]
    part = [n for n in rows if n < R]
    full = len(rows) - len(part)
    A, B, H = X // R, 2 * X // R, X // 2
    near, corner = len(sent(Z_NEAR)), 2 * len(XY_MOVES)
    return [
        (2 * (5 + 2), []),
        (2 * (H + 3 * A + B + 5 + 1 + DEPTH - 1), []),
        (near, []),
        (len(XY_MOVES) + full, part + [2] * len(XY_MOVES)),
        (corner + near + full + 2 * 2 * H + 2 * 2 * DEPTH, part),
        (2 * 5 * A, []),
    ]


def kernel(sizes, cons_hbm, sig_hbm, adv_ref, out_sig_ref, cons, sig, g0, g1, g2, g3, g4, g5, t3, t4, sent,
           yas, zas, ybs, yrs, zrs, drs, x2s, y2s, z2s, d2s, in_sem, ready, send_sem, recv_sem):
    X, R, L = sig.shape
    H, D, DZ = R // 2, DEPTH, L // (4 * X)
    wide = 2 * DZ
    me = [lax.axis_index(a) for a in AXES]

    def device(offset):
        return {a: lax.rem(me[i] + offset[i] + sizes[i], sizes[i]) for i, a in enumerate(AXES)}

    load_c = pltpu.make_async_copy(cons_hbm, cons, in_sem.at[0])
    load_s = pltpu.make_async_copy(sig_hbm, sig, in_sem.at[1])
    load_c.start()
    load_s.start()
    barrier = pltpu.get_barrier_semaphore()
    for o in NEAR:
        pl.semaphore_signal(barrier, inc=1, device_id=device(o), device_id_type=MESH)

    class Group:
        def __init__(self, n, buf, spare):
            self.n, self.buf, self.spare, self.used, self.rows = n, buf, spare, 0, 0

        def copy(self, src, dst, offset):
            return pltpu.make_async_remote_copy(
                src_ref=src, dst_ref=dst, send_sem=send_sem, recv_sem=recv_sem.at[self.n],
                device_id=device(offset), device_id_type=MESH)

        def send(self, src, offset, part=None):
            at = self.used
            if part is not None:
                self.used += 1
                self.rows += part.stop - part.start
                self.copy(src.at[part], self.buf.at[at, part], offset).start()
            elif len(src.shape) == 2:
                self.used, self.rows = at + 1, self.rows + R
                self.copy(src, self.buf.at[at], offset).start()
            else:
                self.used, self.rows = at + src.shape[0], self.rows + R * src.shape[0]
                self.copy(src, self.buf.at[at:self.used], offset).start()
            return at

        def arrived(self):
            assert self.used == self.buf.shape[0] and self.rows == self.spare.shape[0] * self.spare.shape[1]
            self.copy(self.spare, self.spare, NEAR[0]).wait_recv()

    groups = [Group(n, buf, size)
              for n, (buf, size) in enumerate(zip((g0, g1, g2, g3, g4, g5), (g0, g1, g2, t3, t4, g5)))]
    first, late, side, late_rho, second, first_y = groups

    rows = lambda shape: iota(shape, len(shape) - 2)
    lanes = lambda shape: iota(shape, len(shape) - 1)

    def pack_rows(field, first, n):
        size = X * n // R
        out = field[0:size]
        r = rows(out.shape)
        for g in range(1, R // n):
            part = roll(field[g * size:(g + 1) * size], n * g, 1)
            out = jnp.where((r + (2 * R - first - n * g)) % R < n, part, out)
        return out

    def unpack_rows(after, before, n):
        low = rows(after.shape) < H
        return jnp.concatenate(
            [jnp.where(low, roll(after, -n * g, 1), roll(before, -n * g, 1)) for g in range(R // n)],
            axis=0)

    lane2, row2 = lanes((R, L)), rows((R, L))
    low2 = row2 < H

    def pack_lanes(fields, width):
        out = jnp.zeros((R, L), jnp.float32)
        for k, tile in enumerate(f[p] for f in fields for p in range(X)):
            out = jnp.where(((lane2 + width // 2) % L) // width == k, roll(tile, width * k, 1), out)
        return out

    slot2 = ((lane2 + DZ) % L) // wide
    side2 = lane2 % wide >= DZ

    def pack_planes(out, value, ps):
        for k, p in enumerate(ps):
            out = jnp.where(slot2 == p % (2 * X), roll(value[k], wide * p, 1), out)
        return out

    def pack_corner(f, s, o):
        a1, a2, a3, a4 = (f[X - a if o[0] == 1 else a - 1] for a in range(1, 5))
        if o[1] == 1:
            one = jnp.where(row2 >= H, a1, jnp.where(row2 >= 1, roll(a2, -H, 0), roll(a4, 1, 0)))
            two = roll(a3, 2, 0)
        else:
            one = jnp.where(row2 < H, a1, jnp.where(row2 < R - 1, roll(a2, H, 0), roll(a4, -1, 0)))
            two = roll(a3, -2, 0)
        if s is not None:
            s1, s2, s3 = (s[X - a if o[0] == 1 else a - 1] for a in range(1, 4))
            if o[1] == 1:
                two = jnp.where(row2 > H, s1, jnp.where(row2 == H, roll(s3, 1 - H, 0),
                                                        jnp.where(row2 >= 2, roll(s2, -H, 0), two)))
            else:
                two = jnp.where(row2 < H - 1, s1, jnp.where(row2 == H - 1, roll(s3, H - 1, 0),
                                                            jnp.where(row2 < R - 2, roll(s2, H, 0), two)))
        return one, two

    def unpack_corner(buf, slots, dx, source):
        after, before = slots[(-dx, -1, 0)], slots[(-dx, 1, 0)]
        fa, fb, sa, sb = buf[after], buf[before], buf[after + 1], buf[before + 1]
        if source:
            out = [jnp.where(low2, sa, sb), roll(jnp.where(low2, sb, sa), H, 0),
                   jnp.where(low2, roll(sa, 1 - H, 0), roll(sb, H - 1, 0))]
        else:
            out = [jnp.where(low2, fa, fb), roll(jnp.where(low2, fb, fa), H, 0),
                   jnp.where(low2, roll(sa, 2, 0), roll(sb, -2, 0)),
                   jnp.where(low2, roll(fa, 1, 0), roll(fb, -1, 0))]
        out = [v[None] for v in out]
        return out if dx == 1 else out[::-1]

    def cat(*parts):
        return jnp.concatenate(parts, axis=0)

    ups = ((0, 1), (1, -1))

    def plane(d, back=0):
        return X - 1 - back if d == 1 else back

    def planes(d, count, back=0):
        return slice(X - count - back, X - back) if d == 1 else slice(back, back + count)

    def send_z(group, src_ref, moves, slots):
        for o, same in distinct(moves, sizes).items():
            slots[o] = group.send(src_ref, o, z_rows(o, R)) if o == same else slots[same]

    def z_side(of, dy, dz, f):
        own, after, before = (of(dx, dy, dz) for dx in (0, 1, -1))
        if f == 0:
            return jnp.where(slot2 < X, own, roll(jnp.where(slot2 < X // 2, after, before), L // 2, 1))
        return jnp.where(slot2 < X, roll(own, L // 2, 1), jnp.where(slot2 < X + X // 2, after, before))

    def sides(own, low, high):
        return jnp.where(side2, low, own), jnp.where(side2, own, high)

    def z_pairs(of, f, own_z, own_w):
        z = [z_side(of, 0, dz, f) for dz in (-1, 1)]
        w = [jnp.where(low2, z_side(of, 1, dz, f), z_side(of, -1, dz, f)) for dz in (-1, 1)]
        return sides(own_z, *z), sides(own_w, *w)

    load_c.wait()
    load_s.wait()
    state = [cons[f] for f in range(4)] + [sig[...]]
    energy = cons[4]
    A, B = X // R, 2 * X // R
    for f in range(5):
        yas[0, f * A:(f + 1) * A] = pack_rows(state[f], R - 1, 1)
        yas[1, f * A:(f + 1) * A] = pack_rows(state[f], 0, 1)
    zas[0] = pack_lanes(state[0:4], 4)
    zas[1] = pack_lanes([state[4], energy], 4)
    pl.semaphore_wait(barrier, len(NEAR))
    ya = [first_y.send(yas.at[j], (0, d, 0)) for j, d in ups]
    xa = []
    for j, d in ups:
        xa.append(first.send(cons.at[0:4, plane(d)], (d, 0, 0)))
        first.send(sig.at[plane(d)], (d, 0, 0))
    za = [first.send(zas, (0, 0, d)) for j, d in ups]
    for o in NEAR:
        pl.semaphore_signal(ready, inc=1, device_id=device(o), device_id_type=MESH)

    for j, second_row, start in ((0, R - 2, R - 1 - H), (1, 1, 1)):
        for f in range(3):
            ybs[j, f * A:(f + 1) * A] = pack_rows(state[1 + f], second_row, 1)
        ybs[j, 3 * A:3 * A + B] = pack_rows(energy, (R - 2, 0)[j], 2)
        yrs[j] = pack_rows(state[0], start, H)
    lane3 = lanes(energy.shape)
    row3 = rows(energy.shape)
    rho_zz = jnp.where(lane3 == DZ - 1, roll(state[0], -1, 2), roll(state[0], 1, 2))
    rho_own = pack_lanes([state[0], rho_zz], wide)
    zrs[...] = rho_own
    for n, o in enumerate(XY_MOVES):
        drs[n, 0], drs[n, 1] = pack_corner(state[0], None, o)

    pl.semaphore_wait(ready, len(NEAR))
    zr, dr = {}, {}
    send_z(side, zrs, Z_NEAR, zr)
    side_slots = dict(zr)
    for n, o in enumerate(XY_MOVES):
        dr[o] = late_rho.send(drs.at[n, 0], o)
        late_rho.send(drs.at[n, 1], o, slice(0, 2) if o[1] == 1 else slice(R - 2, R))
    zr_far = {}
    send_z(late_rho, zrs, Z_EDGE, zr_far)
    xb, xe, xt = [], [], []
    for j, d in ups:
        xb.append(late.send(cons.at[0:5, plane(d, 1)], (d, 0, 0)))
        xe.append(late.send(cons.at[4, plane(d)], (d, 0, 0)))
        xt.append(late.send(cons.at[0, planes(d, D - 1, 2)], (d, 0, 0)))
    yr, yb = [], []
    for j, d in ups:
        yr.append(late.send(yrs.at[j], (0, d, 0)))
        yb.append(late.send(ybs.at[j], (0, d, 0)))

    inv0 = 1.0 / state[0]
    fields = [inv0] + [state[k] * inv0 for k in (1, 2, 3)] + [state[4]]
    own = [[[roll(v, -s, axis) for s in (1, -1)] for axis in (1, 2)] for v in fields]
    region = ((lane2 + 2) % L) // (4 * X)

    def to_speed(t):
        r = 1.0 / t[0]
        return [r] + [m * r for m in t[1:4]] + [t[4]]

    def coefficients(inv_m, inv_n):
        ws = [[inv_m + inv_n[d][s] for s in range(2)] for d in range(3)]
        scale = ALPHA / (2.0 * inv_m + ALPHA * sum(w for pair in ws for w in pair))
        return [[w * scale for w in pair] for pair in ws]

    def update(source, ws, nbr):
        acc = source
        for d in range(3):
            for s in range(2):
                acc = acc + ws[d][s] * nbr[d][s]
        return acc

    first.arrived()
    xg = [to_speed([g0[xa[j] + f] for f in range(5)]) for j in range(2)]
    zmerged = [jnp.where(lane2 % 4 < 2, g0[za[1] + v], g0[za[0] + v]) for v in range(2)]
    zinv = 1.0 / jnp.where(region == 0, zmerged[0], 1.0)
    shifted = [roll(zinv, 4 * X * k, 1) for k in (1, 2, 3)]
    zspeed = zmerged[0] * jnp.where(region == 1, shifted[0], jnp.where(region == 2, shifted[1], shifted[2]))
    zspeed = jnp.where(region == 0, zinv, zspeed)

    def xz_neighbours(f):
        v, (_, (zp, zm)) = fields[f], own[f]
        t, k = (zspeed, f * X) if f < 4 else (zmerged[1], 0)
        high = cat(*[roll(t, L - 1 - 4 * (k + p), 1)[None] for p in range(X)])
        low = cat(*[roll(t, 1 - 4 * (k + p), 1)[None] for p in range(X)])
        return [(cat(v[1:X], xg[1][f][None]), cat(xg[0][f][None], v[0:X - 1])),
                (jnp.where(lane3 == L - 1, high, zp), jnp.where(lane3 == 0, low, zm))]

    ws = [None] * 3
    ws[0], ws[2] = [[inv0 + v for v in pair] for pair in xz_neighbours(0)]
    (g00, g02), (g10, g12), (g20, g22) = [[p - m for p, m in xz_neighbours(k)] for k in (1, 2, 3)]
    squares, div = g00 * g00 + g22 * g22 + 2.0 * (g02 * g20), g00 + g22
    weight = ws[0][0] + ws[0][1] + ws[2][0] + ws[2][1]
    (xp, xm), (zp, zm) = xz_neighbours(4)
    inflow = ws[0][0] * xp + ws[0][1] * xm + ws[2][0] * zp + ws[2][1] * zm

    side.arrived()
    send_z(late_rho, zrs, Z_VERTEX, zr_far)
    first_y.arrived()
    yg = [to_speed([g5[ya[j] + f * A:ya[j] + (f + 1) * A] for f in range(5)]) for j in range(2)]

    def y_neighbours(f):
        yp, ym = own[f][0]
        after = cat(*[roll(yg[1][f], R - 1 - p, 1) for p in range(R)])
        before = cat(*[roll(yg[0][f], 1 - p, 1) for p in range(R)])
        return jnp.where(row3 == R - 1, after, yp), jnp.where(row3 == 0, before, ym)

    ws[1] = [inv0 + v for v in y_neighbours(0)]
    near_scale = ALPHA / (2.0 * inv0 + ALPHA * (weight + ws[1][0] + ws[1][1]))
    g01, g11, g21 = [p - m for p, m in (y_neighbours(k) for k in (1, 2, 3))]
    div = div + g11
    source = squares + g11 * g11 + 2.0 * (g01 * g10 + g12 * g21) + div * div
    source = source * (0.5 * near_scale)
    yp, ym = y_neighbours(4)
    sigma1 = source + near_scale * (inflow + ws[1][0] * yp + ws[1][1] * ym)
    near_w = [[w * near_scale for w in pair] for pair in ws]

    z_fold = jnp.where(lane3 == DZ - 1, near_w[2][0] * roll(sigma1, -1, 2),
                       jnp.where(lane3 == L - DZ, near_w[2][1] * roll(sigma1, 1, 2), 0.0))
    z_own = pack_lanes([sigma1, source + z_fold], wide)
    z2s[...] = z_own
    z2, d2 = {}, {}
    send_z(second, z2s, Z_VERTEX, z2)
    for n, o in enumerate(XY_MOVES):
        d2s[n, 0], d2s[n, 1] = pack_corner(sigma1, source, o)
        d2[o] = second.send(d2s.at[n], o)
    send_z(second, z2s, Z_EDGE, z2)
    y_fold = jnp.where(row3 == H - 1, near_w[1][0] * roll(sigma1, -1, 1),
                       jnp.where(row3 == H, near_w[1][1] * roll(sigma1, 1, 1), 0.0))
    for j, start in ((0, H), (1, 0)):
        y2s[j, 0:X // 2] = pack_rows(sigma1, start, H)
        y2s[j, X // 2:X] = pack_rows(source + y_fold, start, H)
    y2 = [second.send(y2s.at[j], (0, d, 0)) for j, d in ups]
    for j, d in ups:
        x2s[j, 0:D] = sigma1[planes(d, D)]
        x2s[j, D:2 * D] = source[planes(d, D)]
    x2s[0, D] = source[X - D] + near_w[0][1][X - D] * sigma1[X - D - 1]
    x2s[1, 2 * D - 1] = source[D - 1] + near_w[0][0][D - 1] * sigma1[D]
    x2 = [second.send(x2s.at[j], (d, 0, 0)) for j, d in ups]
    send_z(second, z2s, Z_NEAR, z2)

    late.arrived()
    core = state[0:4] + [energy]
    near_row = (row3 == 0) | (row3 == R - 1)

    def first_rows(f):
        return unpack_rows(g5[ya[1] + f * A:ya[1] + (f + 1) * A], g5[ya[0] + f * A:ya[0] + (f + 1) * A], 1)

    def late_rows(at, to, n):
        return unpack_rows(g1[yb[1] + at:yb[1] + to], g1[yb[0] + at:yb[0] + to], n)

    rho_before, rho_after = [cat(*[roll(g1[yr[j]:yr[j] + X // 2], -H * k, 1) for k in range(R // H)]) for j in range(2)]
    rho_y = jnp.where(near_row, first_rows(0), jnp.where(row3 < H, rho_after, rho_before))
    rho_yy = jnp.where(row3 < H, roll(rho_after, -1, 1), roll(rho_before, 1, 1))
    xn = [[g0[xa[j] + f][None] for f in range(4)] + [g1[xe[j]][None]] for j in range(2)]
    xc = [cat(g1[xb[0] + f][None], xn[0][f], core[f], xn[1][f], g1[xb[1] + f][None]) for f in range(5)]
    yc = [rho_y] + [jnp.where(near_row, first_rows(1 + f), late_rows(f * A, (f + 1) * A, 1)) for f in range(3)]
    yc.append(late_rows(3 * A, 3 * A + B, 2))
    zc = [cat(*[roll(zmerged[f // 4], -4 * (f * X + p), 1)[None] for p in range(X)]) for f in range(4)]
    zc.append(cat(*[roll(zmerged[1], -4 * (X + p), 1)[None] for p in range(X)]))

    def x_stencil(c):
        return c[0:X + 1], c[1:X + 2], c[2:X + 3], c[3:X + 4]

    def ring_stencil(c, gh, axis):
        m, p = ring(c, gh, -1, axis), ring(c, gh, 1, axis)
        return cat(*m), cat(c, gh), cat(*p), cat(*ring(p[0], p[1], 1, axis))

    def faces(st):
        m, q, p, pp = st
        sixth = 1.0 / 6.0
        return (5.0 * q + 2.0 * p - m) * sixth, (2.0 * q + 5.0 * p - pp) * sixth

    def plain_flux(s, d):
        r = 1.0 / s[0]
        v = s[1 + d] * r
        pressure = (GAMMA - 1.0) * (s[4] - 0.5 * (s[1] * s[1] + s[2] * s[2] + s[3] * s[3]) * r)
        out = [s[1 + d]]
        for k in range(3):
            out.append(s[1 + k] * v + pressure if k == d else s[1 + k] * v)
        out.append((s[4] + pressure) * v)
        return out, v

    def difference(flux, d):
        if d == 0:
            return flux[1:X + 1] - flux[0:X]
        return flux[0:X] - ring(flux[0:X], flux[X:2 * X], -1, d)[0]

    base = [None] * 5
    speed = []
    for d in range(3):
        if d == 0:
            lr = [faces(x_stencil(c)) for c in xc]
        else:
            lr = [faces(ring_stencil(c, gh, d)) for c, gh in zip(core, (None, yc, zc)[d])]
        lf, lv = plain_flux([v[0] for v in lr], d)
        rf, rv = plain_flux([v[1] for v in lr], d)
        speed.append((lv, rv))
        for k in range(5):
            flux = 0.5 * (lf[k] + rf[k]) - (0.5 * LAMBDA) * (lr[k][1] - lr[k][0])
            change = difference(flux, d)
            base[k] = change if base[k] is None else base[k] + change
    base = [core[k] - STEP_DT * base[k] for k in range(5)]
    adv_ref[0] = base[0]

    def lower(v, d):
        return v[0:X] if d == 0 else ring(v[0:X], v[X:2 * X], -1, d)[0]

    part = []
    for d, (lv, rv) in enumerate(speed):
        ll, rl = lower(lv, d), lower(rv, d)
        lv, rv = (lv[1:X + 1], rv[1:X + 1]) if d == 0 else (lv[0:X], rv[0:X])
        k = -0.5 * STEP_DT / 6.0
        part.append([k * ll, k * (-lv - 5.0 * ll - 2.0 * rl), k * (5.0 * lv + 2.0 * rv - 2.0 * ll - 5.0 * rl),
                     k * (2.0 * lv + 5.0 * rv + rl), -k * rv])
    middle = part[0][2] + part[1][2] + part[2][2]

    def pick(part, ps, step=0):
        value, reach = part
        return cat(*[value[reach + a + step:reach + b + step] for a, b in ps])

    def z_shift(value, ps, pair, step, by=1):
        at = [p for a, b in ps for p in range(a, b)]
        lane = lanes(value.shape)
        if step == 1:
            ghost, edge = [roll(pair[1], L - by - wide * p, 1) for p in at], lane >= L - by
        else:
            ghost, edge = [roll(pair[0], by - wide * p, 1) for p in at], lane < by
        return jnp.where(edge, cat(*[v[None] for v in ghost]), roll(value, -step * by, 2))

    def around_planes(c, y, pair, ps):
        m = pick(c, ps)
        cy = [ring(m, pick(y, ps), s, 1) for s in (1, -1)]
        z = [z_shift(m, ps, pair, s) for s in (1, -1)]
        return [(pick(c, ps, 1), pick(c, ps, -1)), [t[0] for t in cy], z], [t[1] for t in cy]

    def around_ghosts(y, yy, pair, e):
        ps = [(-e, X + e)]
        return [(pick(y, ps, 1), pick(y, ps, -1)), yy, [z_shift(pick(y, ps), ps, pair, s) for s in (1, -1)]]

    def around_packed(z, w):
        out = [], []
        for zt, wt in zip(z, w):
            zy = [ring(zt, wt, s, 0) for s in (1, -1)]
            for to, t, k in ((out[0], zt, 0), (out[1], wt, 1)):
                to.append([(roll(t, -wide, 1), roll(t, wide, 1)), [v[k] for v in zy], (roll(t, -1, 1), roll(t, 1, 1))])
        return out

    late_rho.arrived()
    rho_of = lambda dx, dy, dz: g2[side_slots[(0, 0, -dz)]] if dx == dy == 0 else g3[zr_far[(-dx, -dy, -dz)]]
    every = range(-D, X + D)
    outer = [p for p in every if not 0 <= p < X]
    rho_c = cat(g1[xt[0]:xt[0] + D - 1], xc[0], g1[xt[1]:xt[1] + D - 1])
    rho_ye = cat(*unpack_corner(g3, dr, -1, False), rho_y, *unpack_corner(g3, dr, 1, False))
    rho_z, rho_w = z_pairs(rho_of, 0, pack_planes(rho_own, pick((rho_c, D + 1), [(-D, 0), (X, X + D)]), outer),
                           pack_planes(rho_own, rho_ye, every))
    inv_c, inv_y = (1.0 / rho_c, D + 1), (1.0 / rho_ye, D)
    inv_z, inv_w = [1.0 / t for t in rho_z], [1.0 / t for t in rho_w]
    beyond = [1.0 / z_side(rho_of, 0, dz, 1) for dz in (-1, 1)]
    far_coef = coefficients(pick(inv_c, [(-D, 0), (X, X + D)]),
                            around_planes(inv_c, inv_y, inv_z, [(-D, 0), (X, X + D)])[0])
    coef_c = [[cat(far[0:D], mine, far[D:2 * D]) for far, mine in zip(*pair)] for pair in zip(far_coef, near_w)]
    e = D - 1
    rim = jnp.zeros((e, R, L), jnp.float32)
    yy = around_planes(inv_c, inv_y, inv_z, [(-e, X + e)])[1]
    inv_yy = cat(rim, 1.0 / rho_yy, rim)
    row = rows(inv_yy.shape)
    yy = [jnp.where(row == at, inv_yy, t) for t, at in zip(yy, (H - 1, H))]
    coef_y = coefficients(pick(inv_y, [(-e, X + e)]), around_ghosts(inv_y, yy, inv_w, e))
    coef_y[1] = [jnp.where(row == at, 0.0, t) for t, at in zip(coef_y[1], (H - 1, H))]
    zn, wn = around_packed(inv_z, inv_w)
    coef_z, coef_w = [], []
    for j, at in ((0, DZ), (1, DZ - 1)):
        last = lane2 % wide == at
        pair = list(zn[j][2])
        pair[1 - j] = jnp.where(last, beyond[j], pair[1 - j])
        coef_z.append(coefficients(inv_z[j], [*zn[j][0:2], pair]))
        coef_z[j][2][1 - j] = jnp.where(last, 0.0, coef_z[j][2][1 - j])
        coef_w.append(coefficients(inv_w[j], wn[j]))

    second.arrived()
    zero = jnp.zeros((1, R, L), jnp.float32)
    sig_of = lambda dx, dy, dz: g4[z2[(-dx, -dy, -dz)]]
    sx, qx = [cat(g4[x2[0] + t:x2[0] + t + D], g4[x2[1] + t:x2[1] + t + D]) for t in (0, D)]
    sy, qy = [unpack_rows(g4[y2[1] + t:y2[1] + t + X // 2], g4[y2[0] + t:y2[0] + t + X // 2], H) for t in (0, X // 2)]
    sy = cat(*unpack_corner(g4, d2, -1, False), sy, *unpack_corner(g4, d2, 1, False))
    qy = cat(*unpack_corner(g4, d2, -1, True), qy, *unpack_corner(g4, d2, 1, True))
    z, w = z_pairs(sig_of, 0, pack_planes(z_own, sx, outer), pack_planes(z_own, sy, every))
    q_own = roll(z_own, L // 2, 1)
    qz, qw = z_pairs(sig_of, 1, pack_planes(q_own, qx, outer), pack_planes(q_own, qy, range(-e, X + e)))
    ghosts = [(z, w)]
    for sweep in range(1, SWEEPS):
        zn, wn = around_packed(z, w)
        z = [update(qz[j], coef_z[j], zn[j]) for j in range(2)]
        if sweep < SWEEPS - 1:
            w = [update(qw[j], coef_w[j], wn[j]) for j in range(2)]
        ghosts.append((z, w))

    def lane_ghost(sweep, which, p):
        return sweep, which, p

    def one_shift(tile, ghost, step, by=1):
        sweep, which, p = ghost
        pair = ghosts[sweep][which]
        if step == 1:
            return jnp.where(lane2 >= L - by, roll(pair[1], L - by - wide * p, 1), roll(tile, -by, 1))
        return jnp.where(lane2 < by, roll(pair[0], by - wide * p, 1), roll(tile, by, 1))

    tiles = lambda value, lo: {lo + k: value[k] for k in range(value.shape[0])}
    c = {**tiles(sigma1, 0), **tiles(sx[0:D], -D), **tiles(sx[D:2 * D], X), -D - 1: zero[0], X + D: zero[0]}
    qc = {**tiles(source, 0), **tiles(qx[0:D], -D), **tiles(qx[D:2 * D], X)}
    y, qy = tiles(sy, -D), tiles(qy, -e)
    cs, ys = [c] + [{} for _ in range(1, SWEEPS)], [y] + [{} for _ in range(1, SWEEPS)]

    def sweep_plane(sweep, p):
        c, y = cs[sweep - 1], ys[sweep - 1]
        ec, ey = D + 1 - sweep, 0 if sweep == SWEEPS - 1 else D - sweep
        if not -ec <= p < X + ec:
            return
        cy = [ring(c[p], y[p], s, 0) for s in (1, -1)]
        ghost = lane_ghost(sweep - 1, 0, p)
        nbr = [(c[p + 1], c[p - 1]), [t[0] for t in cy], [one_shift(c[p], ghost, s) for s in (1, -1)]]
        cs[sweep][p] = update(qc[p], [[v[D + p] for v in pair] for pair in coef_c], nbr)
        if -ey <= p < X + ey:
            ghost = lane_ghost(sweep - 1, 1, p)
            nbr = [(y[p + 1], y[p - 1]), [t[1] for t in cy], [one_shift(y[p], ghost, s) for s in (1, -1)]]
            ys[sweep][p] = update(qy[p], [[v[e + p] for v in pair] for pair in coef_y], nbr)

    def flux_plane(p):
        if not 0 <= p < X:
            return
        c, y, ghost = cs[SWEEPS - 1], ys[SWEEPS - 1], lane_ghost(SWEEPS - 1, 0, p)
        out_sig_ref[p] = c[p]

        def y_shift(step, by):
            edge = row2 >= R - by if step == 1 else row2 < by
            return jnp.where(edge, roll(y[p], -step * by, 0), roll(c[p], -step * by, 0))

        total = base[4][p] + middle[p] * c[p]
        shifts = [lambda s, by: c[p + s * by], y_shift, lambda s, by: one_shift(c[p], ghost, s, by)]
        for d in range(3):
            (p1, p2), (m1, m2) = [[shifts[d](s, by) for by in (1, 2)] for s in (1, -1)]
            adv_ref[1 + d, p] = base[1 + d][p] + ((-4.0 * STEP_DT / 6.0) * (p1 - m1) + (0.5 * STEP_DT / 6.0) * (p2 - m2))
            a = [v[p] for v in part[d]]
            total = total + (a[0] * m2 + a[1] * m1 + a[3] * p1 + a[4] * p2)
        adv_ref[4, p] = total

    for step in range(-D, X + D + 2 * SWEEPS):
        for sweep in range(1, SWEEPS):
            sweep_plane(sweep, step - 2 * (sweep - 1))
        flux_plane(step - 2 * (SWEEPS - 1) - 1)
    assert sum(group.rows for group in groups) == sent.shape[0]
    second.copy(sent, sent, NEAR[0]).wait_send()


def write(adv, sig, adv_hbm, sig_hbm, sem):
    copies = [pltpu.make_async_copy(src, dst, sem.at[n])
              for n, (src, dst) in enumerate(((adv, adv_hbm), (sig, sig_hbm)))]
    for copy in copies:
        copy.start()
    for copy in copies:
        copy.wait()


def solution(mesh):
    sizes = tuple(mesh.shape[a] for a in AXES)

    def on_device(conserved, sigma_guess):
        X, R, L = sigma_guess.shape
        A, B, H, D = X // R, 2 * X // R, X // 2, DEPTH
        f32 = jnp.float32
        vm = lambda *shape: pltpu.VMEM((*shape, R, L), f32)
        nd = len(XY_MOVES)
        tiles = landing(X, R, sizes)
        rows = [R * n + sum(part) for n, part in tiles]
        spare = [pltpu.VMEM((n, 1, L), f32) for n in (rows[3], rows[4], sum(rows))]
        outs = pl.pallas_call(
            functools.partial(kernel, sizes),
            out_shape=(pltpu.VMEM(conserved.shape, f32), pltpu.VMEM(sigma_guess.shape, f32)),
            in_specs=[pl.BlockSpec(memory_space=pl.ANY)] * 2,
            out_specs=(pl.BlockSpec(memory_space=pltpu.VMEM),) * 2,
            scratch_shapes=[
                vm(5, X), vm(X), *[vm(n + len(part)) for n, part in tiles], *spare,
                vm(2, 5 * A), vm(2), vm(2, 3 * A + B), vm(2, H), vm(), vm(nd, 2),
                vm(2, 2 * D), vm(2, 2 * H), vm(), vm(nd, 2),
                pltpu.SemaphoreType.DMA((2,)),
                pltpu.SemaphoreType.REGULAR,
                pltpu.SemaphoreType.DMA,
                pltpu.SemaphoreType.DMA((len(tiles),)),
            ],
            compiler_params=pltpu.CompilerParams(collective_id=0, has_side_effects=True),
        )(conserved, sigma_guess)
        return pl.pallas_call(
            write,
            out_shape=tuple(jax.ShapeDtypeStruct(a.shape, f32) for a in (conserved, sigma_guess)),
            in_specs=[pl.BlockSpec(memory_space=pltpu.VMEM)] * 2,
            out_specs=(pl.BlockSpec(memory_space=pl.ANY),) * 2,
            scratch_shapes=[pltpu.SemaphoreType.DMA((2,))],
        )(*(pltpu.with_memory_space_constraint(v, pltpu.VMEM) for v in outs))

    specs = (P(None, "gx", "gy", "gz"), P("gx", "gy", "gz"))
    return jax.shard_map(on_device, mesh=mesh, in_specs=specs, out_specs=specs, check_vma=False)
```
